32 devices in a mesh: dp: 2 (over y), row: 4 (over x, core), col: 4 (over z).
Axes of the slice: x: 2, y: 2, z: 4, core: 2. Of those that a mesh axis runs over, the one named last changes fastest.
Arguments:
- tokens: bfloat16 [8192, 2048], P(('dp', 'row', 'col'))
- gain_attn: float32 [2048], replicated, may hold values from 0.5 to 1.5
- w_query: bfloat16 [2048, 2048], P('row', 'col')
- w_keyval: bfloat16 [2048, 512], P('row', 'col')
- w_output: bfloat16 [2048, 2048], P('col', 'row'), may hold values from -1.5 to 1.5
- gain_mlp: float32 [2048], replicated, may hold values from 0.5 to 1.5
- w_gate: bfloat16 [2048, 5632], P('row', 'col'), may hold values from -0.125 to 0.125
- w_up: bfloat16 [2048, 5632], P('row', 'col'), may hold values from -0.125 to 0.125
- w_down: bfloat16 [5632, 2048], P('col', 'row'), may hold values from -0.078125 to 0.078125
- out_grad: bfloat16 [8192, 2048], P(('dp', 'row', 'col'))
- document_numbers: int32 [8192], P(('dp', 'row')), may hold values from 0 to 10, as said below
- positions: int32 [8192], P(('dp', 'row')), may hold values from 0 to 999, as said below
Outputs:
- block_out: bfloat16 [8192, 2048], P(('dp', 'row', 'col'))
- grad_tokens: bfloat16 [8192, 2048], P(('dp', 'row', 'col'))
- grad_gain_attn: float32 [2048], replicated
- grad_w_query: float32 [2048, 2048], P('row', 'col')
- grad_w_keyval: float32 [2048, 512], P('row', 'col')
- grad_w_output: float32 [2048, 2048], P('col', 'row')
- grad_gain_mlp: float32 [2048], replicated
- grad_w_gate: float32 [2048, 5632], P('row', 'col')
- grad_w_up: float32 [2048, 5632], P('row', 'col')
- grad_w_down: float32 [5632, 2048], P('col', 'row')
The draws below stay inside these ranges and needn't reach their ends.
Inputs may be any that keep to these rules, and one draw needn't show every extreme that they name: `document_numbers`: within each sequence of 1024 consecutive tokens the ids start at 0 and rise by one at the first token of each new document. `positions`: the index of each token within its document, 0 at the document's first token.
All inputs are finite; a program needn't handle non-finite values.
Results may differ from the reference program's by a relative error of at most 0.022.
Values may be sent and summed in bfloat16 or wider, within the bound.
A program may use at most 192 MiB of HBM per device.

```python
import math
import jax
import jax.numpy as jnp
from jax import lax

MODEL_WIDTH = 2048
QUERY_HEADS = 32
KEY_VALUE_HEADS = 4
HEAD_SIZE = 64
FF = 5632
SEQUENCE_LENGTH = 1024
TOKENS = 8192


def draw_tokens(key, part):
    base_values = jax.random.normal(jax.random.fold_in(key, 1), (TOKENS, MODEL_WIDTH), jnp.float32)
    row_scale = 0.2 * 10.0 ** jax.random.uniform(jax.random.fold_in(key, 2), (TOKENS, 1), jnp.float32)
    col_scale = 0.3 * 10.0 ** jax.random.uniform(jax.random.fold_in(key, 3), (1, MODEL_WIDTH), jnp.float32)
    return (base_values * row_scale * col_scale).astype(jnp.bfloat16)


def draw_out_grad(key, part):
    ramp = jnp.linspace(0.0, 1.0, TOKENS, dtype=jnp.float32)[:, None]
    base_values = jax.random.normal(jax.random.fold_in(key, 4), (TOKENS, MODEL_WIDTH), jnp.float32)
    return (base_values * 3.0 ** ramp).astype(jnp.bfloat16)


def draw_w_query(key, part):
    return (jax.random.normal(jax.random.fold_in(key, 11), (MODEL_WIDTH, QUERY_HEADS * HEAD_SIZE), jnp.float32) / math.sqrt(MODEL_WIDTH)).astype(jnp.bfloat16)


def draw_w_keyval(key, part):
    fresh_values = jax.random.normal(jax.random.fold_in(key, 12), (MODEL_WIDTH, 2 * KEY_VALUE_HEADS * HEAD_SIZE), jnp.float32) / math.sqrt(MODEL_WIDTH)
    return fresh_values.astype(jnp.bfloat16)


def document_layout(key):
    sequence_count = TOKENS // SEQUENCE_LENGTH
    shortest = max(SEQUENCE_LENGTH * 25 // 256, 1)
    longest = SEQUENCE_LENGTH * 125 // 128
    doc_slots = SEQUENCE_LENGTH // shortest + 1
    lengths = jax.random.randint(jax.random.fold_in(key, 21), (sequence_count, doc_slots), shortest, longest + 1)
    seq_index = jnp.arange(sequence_count, dtype=jnp.int32)[:, None]
    slot_index = jnp.arange(doc_slots, dtype=jnp.int32)[None, :]
    lengths = jnp.where(seq_index == 0, shortest, lengths)
    lengths = jnp.where((seq_index == 1) & (slot_index == 0), longest, lengths)
    doc_ends = jnp.cumsum(lengths, axis=1)
    places = jnp.arange(SEQUENCE_LENGTH, dtype=jnp.int32)
    seg_ids = jnp.sum((doc_ends[:, None, :] <= places[None, :, None]).astype(jnp.int32), axis=2)
    starts = jnp.concatenate([jnp.zeros((sequence_count, 1), jnp.int32), doc_ends[:, :-1].astype(jnp.int32)], axis=1)
    first_token = jnp.take_along_axis(starts, seg_ids, axis=1)
    return (seg_ids.reshape(-1).astype(jnp.int32), (places[None, :] - first_token).reshape(-1).astype(jnp.int32))


def draw_document_numbers(key, part):
    return document_layout(key)[0]


def draw_positions(key, part):
    return document_layout(key)[1]


def steps_of(stream_key, shape, cuts, low, high):
    loudness, own = 1.0, jax.random.fold_in(stream_key, 6)
    for dim, parts in cuts:
        draws = jnp.exp(jax.random.uniform(jax.random.fold_in(own, dim), (parts,), jnp.float32, low / len(cuts), high / len(cuts)))
        loudness = loudness * jnp.repeat(draws, shape[dim] // parts).reshape([-1 if axis == dim else 1 for axis in range(len(shape))])
    return loudness


def centred(key, dims, scale, reach, shards=(), held_as=jnp.bfloat16):
    gain = steps_of(key, dims, shards, -0.22, 0.18) if shards else 1.0
    entries = jax.random.normal(key, dims, jnp.float32) * scale * gain
    return jnp.minimum(jnp.maximum(entries, -reach), reach).astype(held_as)


def setup_inputs(seed: int = 0) -> dict:
    seeds = jax.random.split(jax.random.key(seed), 13)
    tokens = draw_tokens(jax.random.fold_in(seeds[12], 71), 0)
    gain_attn = jnp.clip(1.0 + 0.1 * jax.random.normal(seeds[1], (MODEL_WIDTH,), jnp.float32), 0.5, 1.5)
    w_query = draw_w_query(jax.random.fold_in(seeds[12], 71), 0)
    w_keyval = draw_w_keyval(jax.random.fold_in(seeds[12], 71), 0)
    w_output = centred(seeds[4], (QUERY_HEADS * HEAD_SIZE, MODEL_WIDTH), (max(QUERY_HEADS * HEAD_SIZE * 8 // SEQUENCE_LENGTH, 1)) ** -0.5, 1.5, ((0, 4), (1, 4)))
    gain_mlp = jnp.clip(1.0 + 0.1 * jax.random.normal(seeds[5], (MODEL_WIDTH,), jnp.float32), 0.5, 1.5)
    w_gate = centred(seeds[6], (MODEL_WIDTH, FF), MODEL_WIDTH ** -0.5, 0.125, ((0, 4), (1, 4)))
    w_up = centred(seeds[7], (MODEL_WIDTH, FF), MODEL_WIDTH ** -0.5, 0.125, ((0, 4), (1, 4)))
    w_down = centred(seeds[8], (FF, MODEL_WIDTH), FF ** -0.5, 0.078125, ((0, 4), (1, 4)))
    out_grad = draw_out_grad(jax.random.fold_in(seeds[12], 71), 0)
    document_numbers = draw_document_numbers(jax.random.fold_in(seeds[12], 71), 0)
    positions = draw_positions(jax.random.fold_in(seeds[12], 71), 0)
    return dict(tokens=tokens, gain_attn=gain_attn, w_query=w_query, w_keyval=w_keyval, w_output=w_output, gain_mlp=gain_mlp, w_gate=w_gate, w_up=w_up, w_down=w_down, out_grad=out_grad, document_numbers=document_numbers, positions=positions)


NORM_EPS = 1e-05
ROPE_BASE = 10000.0
MASK_FILL = -1e+30
HIGHEST = lax.Precision.HIGHEST

@jax.custom_vjp
def lower_precision(v):
    return lax.optimization_barrier(v.astype(jnp.bfloat16)).astype(jnp.float32)

@jax.custom_vjp
def low_back(v):
    return v

def low_keep(v):
    return (lower_precision(v), None)

def low_pass(kept, grad):
    return (grad,)

def back_keep(v):
    return (v, None)

def back_low(kept, grad):
    return (lower_precision(grad),)
lower_precision.defvjp(low_keep, low_pass)
low_back.defvjp(back_keep, back_low)

def rope_tables(positions, width):
    half_width = width // 2
    frequency = ROPE_BASE ** (-(jnp.arange(half_width, dtype=jnp.float32) * 2.0 / width))
    angles = positions.astype(jnp.float32)[:, None] * frequency[None, :]
    return (jnp.cos(angles)[:, None, :], jnp.sin(angles)[:, None, :])

def apply_rotation(values, cosine_table, sine_table):
    half_width = values.shape[-1] // 2
    first_half = values[..., :half_width]
    second_half = values[..., half_width:]
    return jnp.concatenate([first_half * cosine_table - second_half * sine_table, second_half * cosine_table + first_half * sine_table], axis=-1)

def rms_scale(values, gain_vec):
    mean_sq = lax.optimization_barrier(jnp.mean(values * values, axis=1, keepdims=True))
    return values * lax.rsqrt(mean_sq + NORM_EPS) * gain_vec

def attention_per_sequence(packed):
    query_rows, key_value_rows, seg_ids, places = packed
    cosine_table, sine_table = rope_tables(places, HEAD_SIZE)
    query_group_size = QUERY_HEADS // KEY_VALUE_HEADS
    query_rotated = lower_precision(apply_rotation(query_rows.reshape(SEQUENCE_LENGTH, QUERY_HEADS, HEAD_SIZE), cosine_table, sine_table)).reshape(SEQUENCE_LENGTH, KEY_VALUE_HEADS, query_group_size, HEAD_SIZE)
    key_value_split = key_value_rows.reshape(SEQUENCE_LENGTH, KEY_VALUE_HEADS, 2, HEAD_SIZE)
    k_rot = lower_precision(apply_rotation(key_value_split[:, :, 0], cosine_table, sine_table))
    v_low = lower_precision(key_value_split[:, :, 1])
    scores = low_back(jnp.einsum('qgrd,kgd->grqk', query_rotated, k_rot, precision=HIGHEST) * (1.0 / math.sqrt(HEAD_SIZE)))
    index_row = jnp.arange(SEQUENCE_LENGTH, dtype=jnp.int32)
    allowed = (seg_ids[:, None] == seg_ids[None, :]) & (index_row[None, :] <= index_row[:, None])
    probs = lower_precision(jax.nn.softmax(jnp.where(allowed, scores, MASK_FILL), axis=-1))
    mixed_output = jnp.einsum('grqk,kgd->qgrd', probs, v_low, precision=HIGHEST)
    return mixed_output.reshape(SEQUENCE_LENGTH, QUERY_HEADS * HEAD_SIZE)

def forward(tokens_f, gain_attn, w_query, w_keyval, w_output, gain_mlp, w_gate, w_up, w_down, document_numbers, positions):
    normed_one = lower_precision(rms_scale(tokens_f, gain_attn))
    query_rows = low_back(jnp.dot(normed_one, w_query, precision=HIGHEST))
    key_value_rows = low_back(jnp.dot(normed_one, w_keyval, precision=HIGHEST))
    sequence_count = query_rows.shape[0] // SEQUENCE_LENGTH
    mixed_output = lax.map(jax.checkpoint(attention_per_sequence), (query_rows.reshape(sequence_count, SEQUENCE_LENGTH, QUERY_HEADS * HEAD_SIZE), key_value_rows.reshape(sequence_count, SEQUENCE_LENGTH, 2 * KEY_VALUE_HEADS * HEAD_SIZE), document_numbers.reshape(sequence_count, SEQUENCE_LENGTH), positions.reshape(sequence_count, SEQUENCE_LENGTH)))
    attn_low = low_back(lower_precision(mixed_output.reshape(sequence_count * SEQUENCE_LENGTH, QUERY_HEADS * HEAD_SIZE)))
    resid_mid = tokens_f + low_back(jnp.dot(attn_low, w_output, precision=HIGHEST))
    normed_two = lower_precision(rms_scale(resid_mid, gain_mlp))
    gate_pre = low_back(jnp.dot(normed_two, w_gate, precision=HIGHEST))
    up_pre = low_back(jnp.dot(normed_two, w_up, precision=HIGHEST))
    hidden_act = lower_precision(jax.nn.silu(gate_pre) * up_pre)
    return resid_mid + low_back(jnp.dot(hidden_act, w_down, precision=HIGHEST))

def reference(tokens, gain_attn, w_query, w_keyval, w_output, gain_mlp, w_gate, w_up, w_down, out_grad, document_numbers, positions):

    def closed(tok_in, gain_one, wq_in, wkv_in, wo_in, gain_two, wg_in, wu_in, wd_in):
        return forward(tok_in, gain_one, wq_in, wkv_in, wo_in, gain_two, wg_in, wu_in, wd_in, document_numbers, positions)
    floats = (tokens.astype(jnp.float32), gain_attn.astype(jnp.float32), w_query.astype(jnp.float32), w_keyval.astype(jnp.float32), w_output.astype(jnp.float32), gain_mlp.astype(jnp.float32), w_gate.astype(jnp.float32), w_up.astype(jnp.float32), w_down.astype(jnp.float32))
    block_out, pullback = jax.vjp(closed, *floats)
    grads = pullback(out_grad.astype(jnp.float32))
    return (block_out.astype(jnp.bfloat16), grads[0].astype(jnp.bfloat16), grads[1], grads[2], grads[3], grads[4], grads[5], grads[6], grads[7], grads[8])
```

```python
import functools
import math

import jax
import jax.numpy as jnp
from jax import lax
from jax.experimental import pallas as pl
from jax.experimental.pallas import tpu as pltpu
from jax.sharding import PartitionSpec as P

HEAD_SIZE = 64
SEQUENCE_LENGTH = 1024
NORM_EPS = 1e-05
ROPE_BASE = 10000.0
MASK_FILL = -1e30
BF16 = jnp.bfloat16
F32 = jnp.float32


def nn(a, b):
    return lax.dot_general(a, b, (((1,), (0,)), ((), ())), preferred_element_type=F32)


def nt(a, b):
    return lax.dot_general(a, b, (((1,), (1,)), ((), ())), preferred_element_type=F32)


def tn(a, b):
    return lax.dot_general(a, b, (((0,), (0,)), ((), ())), preferred_element_type=F32)


def swap_halves(v):
    lane = lax.broadcasted_iota(jnp.int32, v.shape, 1)
    return jnp.where((lane % 64) < 32, pltpu.roll(v, 96, 1), pltpu.roll(v, 32, 1))


def kv_kernel(n_ref, w_ref, c_ref, s_ref, o_ref):
    kv = nn(n_ref[...], w_ref[...])
    for s in range(4):
        v = kv[:, 128 * s : 128 * s + 128]
        o_ref[s] = (v * c_ref[...] + swap_halves(v) * s_ref[...]).astype(BF16)


def load_kv(kv_refs):
    return jnp.concatenate([r[...].astype(F32) for r in kv_refs], axis=0)


def fwd_kernel(n_ref, w_ref, k0, k1, k2, k3, bias_ref, c_ref, s_ref, q_ref, o_ref, ot_ref, lse_ref):
    q = nn(n_ref[...], w_ref[...])
    kv = load_kv((k0, k1, k2, k3))
    k_low = kv[:, :64].astype(BF16)
    v_t = kv.T[64:].astype(BF16)
    for p in range(4):
        cols = slice(128 * p, 128 * p + 128)
        v = q[:, cols]
        rot = (v * c_ref[...] + swap_halves(v) * s_ref[...]) * 0.125
        rot = rot.astype(BF16)
        q_ref[:, cols] = rot
        q_t = rot.astype(F32).T.astype(BF16)
        outs = []
        for e in range(2):
            s_t = nn(k_low, q_t[64 * e : 64 * e + 64]) + bias_ref[...]
            top = jnp.max(s_t, axis=0, keepdims=True)
            ex = jnp.exp(s_t - top)
            tot = jnp.sum(ex, axis=0, keepdims=True)
            outs.append(nn(v_t, ex.astype(BF16)) * (1.0 / tot))
            lse_ref[pl.ds(2 * p + e, 1), :] = top + jnp.log(tot)
        o_t = jnp.concatenate(outs, axis=0)
        ot_ref[cols, :] = o_t
        o_ref[:, cols] = o_t.T.astype(BF16)


def bwd_kernel(
    b_ref, w_ref, q_ref, k0, k1, k2, k3, bias_ref, c_ref, s_ref, ot_ref, lse_ref,
    dq_ref, d0_ref, dr_ref, ds_scr, p_scr, dk_scr, dv_scr,
):
    ga = nn(b_ref[...], w_ref[...]).astype(BF16).astype(F32)
    kv = load_kv((k0, k1, k2, k3))
    k_low = kv[:, :64].astype(BF16)
    v_low = pltpu.roll(kv, 64, 1)[:, :64].astype(BF16)
    k_t = kv.T[:64].astype(BF16)
    lane = lax.broadcasted_iota(jnp.int32, (256, 128), 1)
    for p in range(4):
        cols = slice(128 * p, 128 * p + 128)
        qp = q_ref[:, cols].astype(F32)
        gp = ga[:, cols]
        q_t = qp.T.astype(BF16)
        g_tf = gp.T
        g_t = g_tf.astype(BF16)
        prod = g_tf * ot_ref[cols, :]
        dq_t = []
        for e in range(2):
            half = slice(64 * e, 64 * e + 64)
            s_t = nn(k_low, q_t[half]) + bias_ref[...]
            pr = jnp.exp(s_t - lse_ref[pl.ds(2 * p + e, 1), :])
            dp = nn(v_low, g_t[half])
            inner = jnp.sum(prod[half], axis=0, keepdims=True)
            ds = (pr * (dp - inner)).astype(BF16)
            ds_scr[:, 256 * e : 256 * e + 256] = ds
            p_scr[:, 256 * e : 256 * e + 256] = pr.astype(BF16)
            dq_t.append(nn(k_t, ds))
        qbd = jnp.concatenate(
            [jnp.where(lane < 64, qp, 0.0), jnp.where(lane < 64, 0.0, qp)], axis=0
        ).astype(BF16)
        gbd = jnp.concatenate(
            [jnp.where(lane < 64, gp, 0.0), jnp.where(lane < 64, 0.0, gp)], axis=0
        ).astype(BF16)
        dk = nn(ds_scr[...], qbd)
        dv = nn(p_scr[...], gbd)
        if p == 0:
            dk_scr[...] = dk
            dv_scr[...] = dv
        else:
            dk_scr[...] += dk
            dv_scr[...] += dv
        dqp = jnp.concatenate(dq_t, axis=0).T * 0.125
        dq_ref[:, cols] = (dqp * c_ref[...] - swap_halves(dqp) * s_ref[...]).astype(BF16)
    dk = dk_scr[...]
    dv = dv_scr[...]
    lane = lax.broadcasted_iota(jnp.int32, dk.shape, 1)
    both = jnp.where(lane < 64, dk + pltpu.roll(dk, 64, 1), dv + pltpu.roll(dv, 64, 1))
    d0_ref[...] = both[:256]
    for t in range(3):
        dr_ref[t] = both[256 * (t + 1) : 256 * (t + 2)].astype(BF16)


def dkv_kernel(a0, a1, a2, a3, r1, r2, r3, c_ref, s_ref, o_ref):
    own = (a0, a1, a2, a3)
    got = (r1, r2, r3)
    for s in range(4):
        v = own[s][...]
        for t in range(1, 4):
            v = v + got[t - 1][(s + t) % 4].astype(F32)
        o_ref[s] = (v * c_ref[...] - swap_halves(v) * s_ref[...]).astype(BF16)


def call(body, outs, args, flops, scratch=(), vmem=48 << 20):
    spec = pl.BlockSpec(memory_space=pltpu.VMEM)
    shapes = [jax.ShapeDtypeStruct(s, d) for s, d in outs]
    nbytes = sum(a.size * a.dtype.itemsize for a in args) + sum(
        math.prod(s) * jnp.dtype(d).itemsize for s, d in outs
    )
    return pl.pallas_call(
        body,
        out_shape=shapes,
        in_specs=[spec] * len(args),
        out_specs=[spec] * len(outs),
        scratch_shapes=list(scratch),
        compiler_params=pltpu.CompilerParams(vmem_limit_bytes=vmem),
        cost_estimate=pl.CostEstimate(flops=flops, bytes_accessed=nbytes, transcendentals=0),
    )(*args)


X_SWAP = [(0, 2), (1, 3), (2, 0), (3, 1)]
C_SWAP = [(0, 1), (1, 0), (2, 3), (3, 2)]
Y_SWAP = [(0, 1), (1, 0)]
PAIR = [(0, 1), (1, 0), (2, 3), (3, 2)]
MIDDLE = [(1, 2), (2, 1)]
OUTWARD = [(1, 0), (2, 3)]
INWARD = [(0, 1), (3, 2)]


def over_x(a):
    return lax.ppermute(a, "row", X_SWAP)


def over_c(a):
    return lax.ppermute(a, "row", C_SWAP)


def over_y(a):
    return lax.ppermute(a, "dp", Y_SWAP)


def over_z(a, pairs):
    return lax.ppermute(a, "col", pairs)


def from_slot(a, s):
    return over_z(a, [((i + s) % 4, i) for i in range(4)])


def to_slot(a, s):
    return over_z(a, [(i, (i + s) % 4) for i in range(4)])


def gather_col(own, inner):
    first = over_z(own, PAIR)
    mid = over_z(own, MIDDLE)
    third_in = over_z(first, MIDDLE)
    second = jnp.where(inner, mid, over_z(mid, OUTWARD))
    third = jnp.where(inner, third_in, over_z(third_in, OUTWARD))
    return own, first, second, third


def scatter_col(parts):
    own, first, second, third = parts
    t3 = (third + over_z(third.astype(BF16), INWARD)).astype(BF16)
    t2 = (second + over_z(second.astype(BF16), INWARD)).astype(BF16)
    t1 = (first + over_z(t3, MIDDLE)).astype(BF16)
    v = over_z(t2, MIDDLE)
    w = over_z(t1, PAIR)
    return own + v.astype(F32) + w.astype(F32)


def norm_forward(values, gain_vec):
    mean_sq = jnp.mean(values * values, axis=1, keepdims=True)
    inv_rms = lax.rsqrt(mean_sq + NORM_EPS)
    unit_rows = values * inv_rms
    return (unit_rows, inv_rms, (unit_rows * gain_vec).astype(BF16))


def norm_backward(grad_norm, unit_rows, inv_rms, gain_vec):
    scaled = grad_norm * gain_vec
    inner_sum = jnp.mean(scaled * unit_rows, axis=1, keepdims=True)
    return (inv_rms * (scaled - unit_rows * inner_sum), jnp.sum(grad_norm * unit_rows, axis=0))


def shards(
    tokens, gain_attn, w_query, w_keyval, w_output, gain_mlp, w_gate, w_up, w_down, out_grad,
    document_numbers, positions, *, rows,
):
    width = tokens.shape[1]
    fast = rows == 4
    z = lax.axis_index("col")
    r = lax.axis_index("row")
    y = lax.axis_index("dp")
    inner = (z == 1) | (z == 2)
    x, c = r // 2, r % 2
    blk = width // 8

    def permuted(a, abs_order):
        if not fast:
            return a
        axis = a.ndim - 1
        pieces = []
        for hi in range(2):
            for mid in range(2):
                for lo in range(2):
                    if abs_order:
                        at = 4 * (c ^ mid) + 2 * (x ^ hi) + (y ^ lo)
                    else:
                        at = 4 * (x ^ mid) + 2 * (c ^ hi) + (y ^ lo)
                    pieces.append(lax.dynamic_slice_in_dim(a, at * blk, blk, axis))
        return jnp.concatenate(pieces, axis=axis)

    to_rel = functools.partial(permuted, abs_order=False)
    to_abs = functools.partial(permuted, abs_order=True)

    def halves(block):
        half = block.shape[0] // 2
        return (
            lax.dynamic_slice_in_dim(block, y * half, half, 0),
            lax.dynamic_slice_in_dim(block, (1 - y) * half, half, 0),
        )

    def finish_rows(mine):
        return jnp.concatenate([mine, over_c(mine)], axis=0)

    def gather_rows(block):
        if not fast:
            return lax.all_gather(block, "row", axis=0, tiled=True)
        h0, h1 = halves(block)
        x0 = over_x(h0)
        x1 = over_y(x0)
        return finish_rows(jnp.concatenate([h0, h1, x0, x1], axis=0))

    def gather_slots(block):
        if not fast:
            full = lax.all_gather(block, "row", axis=0, tiled=True)
            return [full] + [from_slot(full, s) for s in (1, 2, 3)]
        h0, _ = halves(block)
        out = [gather_rows(block)]
        for s in (1, 2, 3):
            h = from_slot(h0, s)
            n = h.shape[0]
            if s % 2:
                yh = over_y(h)
                got = over_x(jnp.concatenate([h, yh], axis=0))
                mine = jnp.concatenate([h, yh, got], axis=0)
            else:
                xh = over_x(h)
                got = over_y(jnp.concatenate([h, xh], axis=0))
                mine = jnp.concatenate([h, got[:n], xh, got[n:]], axis=0)
            out.append(finish_rows(mine))
        return out

    wkv_halves = halves(w_keyval)
    if fast:
        kv_stack = jnp.concatenate(
            [wkv_halves[0]] + [from_slot(wkv_halves[0], s) for s in (1, 2, 3)], axis=1
        )
        xk = over_x(kv_stack)
        got = over_y(jnp.concatenate([kv_stack, xk], axis=0))
        n = kv_stack.shape[0]
        wkv = finish_rows(jnp.concatenate([kv_stack, got[:n], xk, got[n:]], axis=0))
    else:
        full = lax.all_gather(w_keyval, "row", axis=0, tiled=True)
        wkv = jnp.concatenate([full] + [from_slot(full, s) for s in (1, 2, 3)], axis=1)
    wq = gather_slots(w_query)
    wo = gather_slots(w_output.T)
    wg = gather_rows(w_gate)
    wu = gather_rows(w_up)
    wd = gather_rows(w_down.T)

    tok = to_rel(tokens)
    x_in = tok.astype(F32)
    gain_one = to_rel(gain_attn)
    gain_two = to_rel(gain_mlp)
    unit_one, inv_one, normed_one = norm_forward(x_in, gain_one)
    count = tokens.shape[0]
    my_pos = lax.dynamic_slice_in_dim(positions, z * count, count, 0)
    frequency = ROPE_BASE ** (-(jnp.arange(32, dtype=F32) * 2.0 / HEAD_SIZE))
    angles = my_pos.astype(F32)[:, None] * frequency[None, :]
    co, si = jnp.cos(angles), jnp.sin(angles)
    cos_q = jnp.concatenate([co, co, co, co], axis=1)
    sin_q = jnp.concatenate([-si, si, -si, si], axis=1)
    cos_k = jnp.concatenate([co, co, jnp.ones_like(co), jnp.ones_like(co)], axis=1)
    sin_k = jnp.concatenate([-si, si, jnp.zeros_like(si), jnp.zeros_like(si)], axis=1)
    my_seg = lax.dynamic_slice_in_dim(document_numbers, z * count, count, 0)
    key_seg = jnp.concatenate(
        [lax.dynamic_slice_in_dim(document_numbers, ((z + t) % 4) * count, count, 0) for t in range(4)]
    )
    lane = jnp.arange(count, dtype=jnp.int32)
    key_at = jnp.concatenate([((z + t) % 4) * count + lane for t in range(4)])
    allowed = (key_seg[:, None] == my_seg[None, :]) & (key_at[:, None] <= (z * count + lane)[None, :])
    bias = jnp.where(allowed, 0.0, MASK_FILL).astype(F32)

    kv = call(
        kv_kernel, [((4, count, 128), BF16)], (normed_one, wkv, cos_k, sin_k), 2 * count * width * 512
    )[0]
    kv_from = [kv]
    for t in (1, 2, 3):
        kv_from.append(over_z(kv, [((i + t) % 4, i) for i in range(4) if i + t >= 4]))
    kv_of = [[kv_from[t][(s - t) % 4] for t in range(4)] for s in range(4)]
    fwd = []
    for s in range(4):
        fwd.append(
            call(
                fwd_kernel,
                [((count, 512), BF16), ((count, 512), BF16), ((512, count), F32), ((8, count), F32)],
                (normed_one, wq[s], *kv_of[s], bias, cos_q, sin_q),
                2 * count * width * 512 + 8 * 4 * count * 1024 * 256,
            )
        )
    attn = [f[1] for f in fwd]
    attn_out = nt(attn[0], wo[0]) + nt(attn[1], wo[1]) + nt(attn[2], wo[2]) + nt(attn[3], wo[3])
    resid_mid = x_in + attn_out

    unit_two, inv_two, normed_two = norm_forward(resid_mid, gain_two)
    dy = to_rel(out_grad)
    dys = gather_col(dy, inner)
    n2s = gather_col(normed_two, inner)
    outs, gns, acts, ggs, gus = [], [], [], [], []
    for s in range(4):
        gate_pre = nn(n2s[s], wg)
        up_pre = nn(n2s[s], wu)
        grad_act = nn(dys[s], wd)
        sig = jax.nn.sigmoid(gate_pre)
        silu = gate_pre * sig
        act = (silu * up_pre).astype(BF16)
        gg = (grad_act * up_pre * sig * (1.0 + gate_pre * (1.0 - sig))).astype(BF16)
        gu = (grad_act * silu).astype(BF16)
        outs.append(nt(act, wd))
        gns.append(nt(gg, wg) + nt(gu, wu))
        acts.append(act)
        ggs.append(gg)
        gus.append(gu)
    grad_norm_two = scatter_col(gns)
    block_out = (resid_mid + scatter_col(outs)).astype(BF16)
    n2_all = jnp.concatenate(n2s, axis=0)
    dy_all = jnp.concatenate(dys, axis=0)
    act_all = jnp.concatenate(acts, axis=0)
    gg_all = jnp.concatenate(ggs, axis=0)
    gu_all = jnp.concatenate(gus, axis=0)

    def ordered(lo, hi):
        return jnp.where(y == 0, jnp.concatenate([lo, hi], axis=0), jnp.concatenate([hi, lo], axis=0))

    def weight_grad(act_rel, g):
        half = width // 2
        if not fast:
            full = lax.psum_scatter(tn(act_rel, g).astype(BF16), "row", scatter_dimension=0, tiled=True)
            return lax.psum(full, "dp").astype(F32)
        got = over_c(tn(act_rel[:, half:], g).astype(BF16))
        t = tn(act_rel[:, :half], g) + got.astype(F32)
        q = half // 2
        got = over_x(t[q:].astype(BF16))
        t = (t[:q] + got.astype(F32)).astype(BF16)
        got = over_y(t).astype(F32)
        t = t.astype(F32)
        return ordered(t[: q // 2] + got[q // 2 :], t[q // 2 :] + got[: q // 2])

    def weight_grad_slots(act_rel, gs):
        half = width // 2
        if not fast:
            tot = 0.0
            for s in range(4):
                full = lax.psum_scatter(
                    tn(act_rel, gs[s]).astype(BF16), "row", scatter_dimension=0, tiled=True
                )
                tot = tot + (full if s == 0 else to_slot(full, s)).astype(F32)
            return lax.psum(tot.astype(BF16), "dp").astype(F32)
        tot = 0.0
        for s in range(4):
            got = over_c(tn(act_rel[:, half:], gs[s]).astype(BF16))
            t = tn(act_rel[:, :half], gs[s]) + got.astype(F32)
            b = blk
            t00, t01, t10, t11 = t[:b], t[b : 2 * b], t[2 * b : 3 * b], t[3 * b :]
            if s % 2:
                got = over_y(jnp.concatenate([t01, t11], axis=0).astype(BF16)).astype(F32)
                u0 = t00 + got[:b]
                u1 = t10 + got[b:]
                u = u0 + over_x(u1.astype(BF16)).astype(F32)
            else:
                got = over_x(jnp.concatenate([t10, t11], axis=0).astype(BF16)).astype(F32)
                u0 = t00 + got[:b]
                u1 = t01 + got[b:]
                u = u0 + over_y(u1.astype(BF16)).astype(F32)
            u = u.astype(BF16)
            tot = tot + (u if s == 0 else to_slot(u, s)).astype(F32)
        tot = tot.astype(BF16)
        return ordered(tot.astype(F32), over_y(tot).astype(F32))

    g_down = weight_grad(dy_all, act_all)
    g_gate = weight_grad(n2_all, gg_all)
    g_up = weight_grad(n2_all, gu_all)

    mid_norm, gain_two_term = norm_backward(grad_norm_two, unit_two, inv_two, gain_two)
    grad_mid = dy.astype(F32) + mid_norm
    branch = grad_mid.astype(BF16)
    bwd = []
    for s in range(4):
        bwd.append(
            call(
                bwd_kernel,
                [((count, 512), BF16), ((count, 128), F32), ((3, count, 128), BF16)],
                (branch, wo[s], fwd[s][0], *kv_of[s], bias, cos_q, sin_q, fwd[s][2], fwd[s][3]),
                2 * count * width * 512 + 8 * 10 * count * 1024 * 256,
                scratch=(
                    pltpu.VMEM((1024, 512), BF16),
                    pltpu.VMEM((1024, 512), BF16),
                    pltpu.VMEM((1024, 128), F32),
                    pltpu.VMEM((1024, 128), F32),
                ),
            )
        )
    got = []
    for t in (1, 2, 3):
        out = jnp.stack([bwd[s][2][t - 1] for s in range(4)])
        got.append(over_z(out, [(i, (i + t) % 4) for i in range(4) if i + t >= 4]))
    dkv = call(
        dkv_kernel,
        [((4, count, 128), BF16)],
        (*[bwd[s][1] for s in range(4)], *got, cos_k, sin_k),
        count * 512 * 8,
    )[0]
    dkv = jnp.concatenate([dkv[s] for s in range(4)], axis=1)
    dq = [bwd[s][0] for s in range(4)]
    grad_norm_one = nt(dq[0], wq[0]) + nt(dq[1], wq[1]) + nt(dq[2], wq[2]) + nt(dq[3], wq[3])
    grad_norm_one = grad_norm_one + nt(dkv, wkv)
    in_norm, gain_one_term = norm_backward(grad_norm_one, unit_one, inv_one, gain_one)
    grad_tokens = (grad_mid + in_norm).astype(BF16)
    g_output = weight_grad_slots(branch, attn)
    g_query = weight_grad_slots(normed_one, dq)
    g_keyval = weight_grad_slots(normed_one, [dkv[:, 128 * s : 128 * s + 128] for s in range(4)])

    def total(v):
        if not fast:
            return lax.psum(v, ("dp", "row", "col"))
        v = v + over_c(v)
        v = v + over_x(v)
        v = v + over_y(v)
        v = v + over_z(v, PAIR)
        return v + over_z(v, [(0, 2), (1, 3), (2, 0), (3, 1)])

    return (
        to_abs(block_out),
        to_abs(grad_tokens),
        total(to_abs(gain_one_term)),
        g_query,
        g_keyval,
        g_output.T,
        total(to_abs(gain_two_term)),
        g_gate,
        g_up,
        g_down.T,
    )


def solution(mesh):
    spec = P(("dp", "row", "col"), None)
    down = P("row", "col")
    across = P("col", "row")
    seq = P(("dp", "row"))
    return jax.shard_map(
        functools.partial(shards, rows=mesh.shape["row"]),
        mesh=mesh,
        in_specs=(spec, P(), down, down, across, P(), down, down, across, spec, seq, seq),
        out_specs=(spec, spec, P(), down, down, across, P(), down, down, across),
        check_vma=False,
    )
```

```python
import functools
import math

import jax
import jax.numpy as jnp
from jax import lax
from jax.experimental import pallas as pl
from jax.experimental.pallas import tpu as pltpu
from jax.sharding import PartitionSpec as P

HEAD_SIZE = 64
SEQUENCE_LENGTH = 1024
NORM_EPS = 1e-05
ROPE_BASE = 10000.0
MASK_FILL = -1e30
BF16 = jnp.bfloat16
F32 = jnp.float32


def nn(a, b):
    return lax.dot_general(a, b, (((1,), (0,)), ((), ())), preferred_element_type=F32)


def nt(a, b):
    return lax.dot_general(a, b, (((1,), (1,)), ((), ())), preferred_element_type=F32)


def tn(a, b):
    return lax.dot_general(a, b, (((0,), (0,)), ((), ())), preferred_element_type=F32)


def swap_halves(v):
    lane = lax.broadcasted_iota(jnp.int32, v.shape, 1)
    return jnp.where((lane % 64) < 32, pltpu.roll(v, 96, 1), pltpu.roll(v, 32, 1))


def kv_kernel(n_ref, w_ref, c_ref, s_ref, o_ref):
    kv = nn(n_ref[...], w_ref[...])
    for s in range(4):
        v = kv[:, 128 * s : 128 * s + 128]
        o_ref[s] = (v * c_ref[...] + swap_halves(v) * s_ref[...]).astype(BF16)


def load_kv(kv_refs):
    return jnp.concatenate([r[...].astype(F32) for r in kv_refs], axis=0)


def fwd_kernel(n_ref, w_ref, k0, k1, k2, k3, bias_ref, c_ref, s_ref, q_ref, o_ref, ot_ref, lse_ref):
    q = nn(n_ref[...], w_ref[...])
    kv = load_kv((k0, k1, k2, k3))
    k_low = kv[:, :64].astype(BF16)
    v_t = kv.T[64:].astype(BF16)
    for p in range(4):
        cols = slice(128 * p, 128 * p + 128)
        v = q[:, cols]
        rot = (v * c_ref[...] + swap_halves(v) * s_ref[...]) * 0.125
        rot = rot.astype(BF16)
        q_ref[:, cols] = rot
        q_t = rot.astype(F32).T.astype(BF16)
        outs = []
        for e in range(2):
            s_t = nn(k_low, q_t[64 * e : 64 * e + 64]) + bias_ref[...]
            top = jnp.max(s_t, axis=0, keepdims=True)
            ex = jnp.exp(s_t - top)
            tot = jnp.sum(ex, axis=0, keepdims=True)
            outs.append(nn(v_t, ex.astype(BF16)) * (1.0 / tot))
            lse_ref[pl.ds(2 * p + e, 1), :] = top + jnp.log(tot)
        o_t = jnp.concatenate(outs, axis=0)
        ot_ref[cols, :] = o_t
        o_ref[:, cols] = o_t.T.astype(BF16)


def bwd_kernel(
    b_ref, w_ref, q_ref, k0, k1, k2, k3, bias_ref, c_ref, s_ref, ot_ref, lse_ref,
    dq_ref, d0_ref, dr_ref, ds_scr, p_scr, dk_scr, dv_scr,
):
    ga = nn(b_ref[...], w_ref[...]).astype(BF16).astype(F32)
    kv = load_kv((k0, k1, k2, k3))
    k_low = kv[:, :64].astype(BF16)
    v_low = pltpu.roll(kv, 64, 1)[:, :64].astype(BF16)
    k_t = kv.T[:64].astype(BF16)
    lane = lax.broadcasted_iota(jnp.int32, (256, 128), 1)
    for p in range(4):
        cols = slice(128 * p, 128 * p + 128)
        qp = q_ref[:, cols].astype(F32)
        gp = ga[:, cols]
        q_t = qp.T.astype(BF16)
        g_tf = gp.T
        g_t = g_tf.astype(BF16)
        prod = g_tf * ot_ref[cols, :]
        dq_t = []
        for e in range(2):
            half = slice(64 * e, 64 * e + 64)
            s_t = nn(k_low, q_t[half]) + bias_ref[...]
            pr = jnp.exp(s_t - lse_ref[pl.ds(2 * p + e, 1), :])
            dp = nn(v_low, g_t[half])
            inner = jnp.sum(prod[half], axis=0, keepdims=True)
            ds = (pr * (dp - inner)).astype(BF16)
            ds_scr[:, 256 * e : 256 * e + 256] = ds
            p_scr[:, 256 * e : 256 * e + 256] = pr.astype(BF16)
            dq_t.append(nn(k_t, ds))
        qbd = jnp.concatenate(
            [jnp.where(lane < 64, qp, 0.0), jnp.where(lane < 64, 0.0, qp)], axis=0
        ).astype(BF16)
        gbd = jnp.concatenate(
            [jnp.where(lane < 64, gp, 0.0), jnp.where(lane < 64, 0.0, gp)], axis=0
        ).astype(BF16)
        dk = nn(ds_scr[...], qbd)
        dv = nn(p_scr[...], gbd)
        if p == 0:
            dk_scr[...] = dk
            dv_scr[...] = dv
        else:
            dk_scr[...] += dk
            dv_scr[...] += dv
        dqp = jnp.concatenate(dq_t, axis=0).T * 0.125
        dq_ref[:, cols] = (dqp * c_ref[...] - swap_halves(dqp) * s_ref[...]).astype(BF16)
    dk = dk_scr[...]
    dv = dv_scr[...]
    lane = lax.broadcasted_iota(jnp.int32, dk.shape, 1)
    both = jnp.where(lane < 64, dk + pltpu.roll(dk, 64, 1), dv + pltpu.roll(dv, 64, 1))
    d0_ref[...] = both[:256]
    for t in range(3):
        dr_ref[t] = both[256 * (t + 1) : 256 * (t + 2)].astype(BF16)


def dkv_kernel(a0, a1, a2, a3, r1, r2, r3, c_ref, s_ref, o_ref):
    own = (a0, a1, a2, a3)
    got = (r1, r2, r3)
    for s in range(4):
        v = own[s][...]
        for t in range(1, 4):
            v = v + got[t - 1][(s + t) % 4].astype(F32)
        o_ref[s] = (v * c_ref[...] - swap_halves(v) * s_ref[...]).astype(BF16)


def call(body, outs, args, flops, scratch=(), vmem=48 << 20):
    spec = pl.BlockSpec(memory_space=pltpu.VMEM)
    shapes = [jax.ShapeDtypeStruct(s, d) for s, d in outs]
    nbytes = sum(a.size * a.dtype.itemsize for a in args) + sum(
        math.prod(s) * jnp.dtype(d).itemsize for s, d in outs
    )
    return pl.pallas_call(
        body,
        out_shape=shapes,
        in_specs=[spec] * len(args),
        out_specs=[spec] * len(outs),
        scratch_shapes=list(scratch),
        compiler_params=pltpu.CompilerParams(vmem_limit_bytes=vmem),
        cost_estimate=pl.CostEstimate(flops=flops, bytes_accessed=nbytes, transcendentals=0),
    )(*args)


MESH = pl.DeviceIdType.MESH


class Wire:
    def __init__(self, send_sem, recv_sem, z):
        self.send_sem, self.recv_sem, self.z = send_sem, recv_sem, z
        self.count = 0
        self.made = []

    def to(self, where):
        r = lax.axis_index("row")
        if where == "x":
            return {"row": lax.rem(r + 2, 4)}
        if where == "c":
            return {"row": r + 1 - 2 * lax.rem(r, 2)}
        if where == "y":
            return {"dp": 1 - lax.axis_index("dp")}
        return {"col": where}

    def copy(self, src, dst, where, only=None):
        k = self.count
        self.count += 1
        cp = pltpu.make_async_remote_copy(
            src_ref=src, dst_ref=dst, send_sem=self.send_sem.at[k], recv_sem=self.recv_sem.at[k],
            device_id=self.to(where), device_id_type=MESH,
        )
        self.made.append((cp, only))
        return cp

    def send(self, src, dst, where):
        cp = self.copy(src, dst, where)
        cp.start()
        return cp

    def finish(self):
        for cp, only in self.made:
            if only is None:
                cp.wait_send()
            else:
                pl.when(only)(cp.wait_send)


def greet(z):
    barrier = pltpu.get_barrier_semaphore()
    wire = Wire(None, None, z)
    for where in ("x", "c", "y"):
        pl.semaphore_signal(barrier, inc=1, device_id=wire.to(where), device_id_type=MESH)
    for d in (1, 2, 3):
        pl.semaphore_signal(barrier, inc=1, device_id={"col": lax.rem(z + d, 4)}, device_id_type=MESH)
    pl.semaphore_wait(barrier, 6)


def attend_slot(w_ref, n_ref, kv_scr, s, bias_ref, c_ref, s_ref, q_ref, o_ref, ot_ref, lse_ref, q_scr):
    q_scr[...] = nn(n_ref[...], w_ref[...])
    kv = jnp.concatenate([kv_scr[t, (s - t) % 4].astype(F32) for t in range(4)], axis=0)
    k_low = kv[:, :64].astype(BF16)
    v_t = kv.T[64:].astype(BF16)

    def pair(p, carry):
        at = pl.multiple_of(p * 128, 128)
        cols = pl.ds(at, 128)
        v = q_scr[:, cols]
        rot = ((v * c_ref[...] + swap_halves(v) * s_ref[...]) * 0.125).astype(BF16)
        q_ref[s, :, cols] = rot
        q_t = rot.astype(F32).T.astype(BF16)
        outs = []
        for e in range(2):
            s_t = nn(k_low, q_t[64 * e : 64 * e + 64]) + bias_ref[...]
            top = jnp.max(s_t, axis=0, keepdims=True)
            ex = jnp.exp(s_t - top)
            tot = jnp.sum(ex, axis=0, keepdims=True)
            outs.append(nn(v_t, ex.astype(BF16)) * (1.0 / tot))
            lse_ref[s, pl.ds(2 * p + e, 1), :] = top + jnp.log(tot)
        o_t = jnp.concatenate(outs, axis=0)
        ot_ref[s, cols, :] = o_t
        o_ref[s, :, cols] = o_t.T.astype(BF16)
        return carry

    lax.fori_loop(0, 4, pair, 0)


def start_kernel(
    tok_ref, gain1_ref, gain2_ref, wq_ref, wo_ref, wkv_ref, wg_ref, wu_ref, wd_ref, dy_ref, bias_ref,
    cq_ref, sq_ref, ck_ref, sk_ref,
    WQ, WO, WKV, WG, WU, WD, DY, n1_ref, q_ref, kv_out, o_ref, ot_ref, lse_ref, mid_ref, n2_ref,
    wbuf, wkv_scr, kv_scr, q_scr, send_sem, recv_sem, loc_sem,
):
    z = lax.axis_index("col")
    y = lax.axis_index("dp")
    inner = (z == 1) | (z == 2)
    w = Wire(send_sem, recv_sem, z)
    locs = []

    def local(src, dst):
        cp = pltpu.make_async_copy(src, dst, loc_sem.at[len(locs)])
        cp.start()
        locs.append(cp)
        return cp

    greet(z)
    blocks = {"kv": (wkv_ref, WKV), "q": (wq_ref, WQ), "o": (wo_ref, WO)}
    ev = {}

    def start_z(name):
        ref, full = blocks[name]
        for s in (1, 2, 3):
            d = 4 - s
            ev[name, s, "z"] = w.send(ref.at[y], full.at[s, 0, 0, 0], lax.rem(z + d, 4))

    def start_own(name):
        ref, full = blocks[name]
        ev[name, 0, "x"] = w.send(ref.at[y], full.at[0, 0, 1, 0], "x")
        ev[name, 0, "own"] = [local(ref.at[y], full.at[0, 0, 0, 0]), local(ref.at[1 - y], full.at[0, 0, 0, 1])]
        ev[name, 0, "c0"] = [
            w.send(ref.at[y], full.at[0, 1, 0, 0], "c"), w.send(ref.at[1 - y], full.at[0, 1, 0, 1], "c")
        ]

    def own_second(name):
        full = blocks[name][1]
        ev[name, 0, "x"].wait_recv()
        ev[name, 0, "y"] = w.send(full.at[0, 0, 1, 0], full.at[0, 0, 1, 1], "y")

    def own_core(name):
        full = blocks[name][1]
        ev[name, 0, "y"].wait_recv()
        ev[name, 0, "c"] = w.send(full.at[0, 0, 1], full.at[0, 1, 1], "c")

    def first(name, s):
        full = blocks[name][1]
        ev[name, s, "z"].wait_recv()
        if s % 2:
            ev[name, s, 1] = w.send(full.at[s, 0, 0, 0], full.at[s, 0, 0, 1], "y")
        else:
            ev[name, s, 1] = w.send(full.at[s, 0, 0, 0], full.at[s, 0, 1, 0], "x")

    def second(name, s):
        full = blocks[name][1]
        ev[name, s, 1].wait_recv()
        if s % 2:
            ev[name, s, 2] = w.send(full.at[s, 0, 0], full.at[s, 0, 1], "x")
        else:
            ev[name, s, 2] = w.send(full.at[s, 0, :, 0], full.at[s, 0, :, 1], "y")

    def core(name, s):
        full = blocks[name][1]
        ev[name, s, 2].wait_recv()
        ev[name, s, "c"] = w.send(full.at[s, 0], full.at[s, 1], "c")

    def whole(name, s):
        ev[name, s, "c"].wait_recv()
        if s == 0:
            for cp in ev[name, 0, "c0"]:
                cp.wait_recv()
            for cp in ev[name, 0, "own"]:
                cp.wait()

    def fetch(full, s, dst):
        return local(full.at[s], dst)

    start_z("kv")
    start_own("kv")
    start_z("q")
    start_own("q")

    x_in = tok_ref[...].astype(F32)
    inv = lax.rsqrt(jnp.mean(x_in * x_in, axis=1, keepdims=True) + NORM_EPS)
    n1_ref[...] = (x_in * inv * gain1_ref[...]).astype(BF16)
    for t in (1, 2, 3):

        @pl.when(z + t < 4)
        def _():
            kv_scr[t] = jnp.zeros_like(kv_scr[t])

    own_second("kv")
    for s in (1, 2, 3):
        first("kv", s)
    own_second("q")
    for s in (1, 2, 3):
        second("kv", s)
    own_core("kv")
    for s in (1, 2, 3):
        first("q", s)
    for s in (1, 2, 3):
        core("kv", s)
    own_core("q")
    start_z("o")
    start_own("o")
    got = []
    for s in range(4):
        whole("kv", s)
        got.append(fetch(WKV, s, wkv_scr.at[s]))
    for s in range(4):
        got[s].wait()
        kv = nn(n1_ref[...], wkv_scr[s].reshape(2048, 128))
        kv_scr[0, s] = (kv * ck_ref[...] + swap_halves(kv) * sk_ref[...]).astype(BF16)
    kv_cp = {}
    for d in (1, 2, 3):
        cp = w.copy(kv_scr.at[0], kv_scr.at[4 - d], lax.rem(z + d, 4), only=z + d < 4)
        kv_cp[4 - d] = cp
        pl.when(z + d < 4)(cp.start)
    for s in (1, 2, 3):
        second("q", s)
    whole("q", 0)
    cps = [fetch(WQ, 0, wbuf.at[0])]
    for s in (1, 2, 3):
        core("q", s)
    own_second("o")
    for t in (1, 2, 3):
        pl.when(z + t >= 4)(kv_cp[t].wait_recv)

    def attend(s):
        cps[s].wait()
        attend_slot(
            wbuf.at[s % 2].reshape(2048, 512), n1_ref, kv_scr, s, bias_ref, cq_ref, sq_ref, q_ref, o_ref, ot_ref,
            lse_ref, q_scr,
        )

    whole("q", 1)
    cps.append(fetch(WQ, 1, wbuf.at[1]))
    attend(0)
    for s in (1, 2, 3):
        first("o", s)
    own_core("o")
    whole("q", 2)
    cps.append(fetch(WQ, 2, wbuf.at[0]))
    attend(1)
    for s in (1, 2, 3):
        second("o", s)
    mats = {"g": (wg_ref, WG), "u": (wu_ref, WU), "d": (wd_ref, WD)}

    def mat_start(name):
        ref, full = mats[name]
        ev[name, "x"] = w.send(ref.at[y], full.at[0, 1, 0], "x")
        ev[name, "own"] = [local(ref.at[y], full.at[0, 0, 0]), local(ref.at[1 - y], full.at[0, 0, 1])]
        ev[name, "c0"] = [
            w.send(ref.at[y], full.at[1, 0, 0], "c"), w.send(ref.at[1 - y], full.at[1, 0, 1], "c")
        ]

    def mat_second(name):
        full = mats[name][1]
        ev[name, "x"].wait_recv()
        ev[name, "y"] = w.send(full.at[0, 1, 0], full.at[0, 1, 1], "y")

    def mat_core(name):
        full = mats[name][1]
        ev[name, "y"].wait_recv()
        ev[name, "c"] = w.send(full.at[0, 1], full.at[1, 1], "c")

    def mat_whole(name):
        ev[name, "c"].wait_recv()
        for cp in ev[name, "c0"]:
            cp.wait_recv()
        for cp in ev[name, "own"]:
            cp.wait()

    for name in mats:
        mat_start(name)
    buddy = z + 1 - 2 * lax.rem(z, 2)
    middle = 3 - z
    d1 = w.send(dy_ref, DY.at[1], buddy)
    d2 = w.copy(dy_ref, DY.at[2], middle, only=inner)
    pl.when(inner)(d2.start)
    dy_own = local(dy_ref, DY.at[0])
    whole("q", 3)
    cps.append(fetch(WQ, 3, wbuf.at[1]))
    attend(2)
    for s in (1, 2, 3):
        core("o", s)
    for name in mats:
        mat_second(name)
    d1.wait_recv()
    e3 = w.copy(DY.at[1], DY.at[3], middle, only=inner)
    pl.when(inner)(e3.start)
    attend(3)
    d2f = w.copy(DY.at[2], DY.at[2], buddy, only=inner)

    @pl.when(inner)
    def _():
        d2.wait_recv()
        d2f.start()

    acc = x_in
    del x_in
    mid_ref[...] = tok_ref[...].astype(F32)
    oc = []
    for s in range(4):
        whole("o", s)
        if s < 2:
            oc.append(fetch(WO, s, wbuf.at[s % 2]))
    for s in range(4):
        oc[s].wait()
        mid_ref[...] += nt(o_ref[s], wbuf[s % 2].reshape(2048, 512))
        if s < 2:
            oc.append(fetch(WO, s + 2, wbuf.at[s % 2]))
    mid = mid_ref[...]
    inv = lax.rsqrt(jnp.mean(mid * mid, axis=1, keepdims=True) + NORM_EPS)
    n2_ref[...] = (mid * inv * gain2_ref[...]).astype(BF16)
    kv_out[...] = kv_scr[...]
    for name in mats:
        mat_core(name)
    e3f = w.copy(DY.at[3], DY.at[3], buddy, only=inner)

    @pl.when(inner)
    def _():
        e3.wait_recv()
        e3f.start()

    @pl.when(jnp.logical_not(inner))
    def _():
        d2f.wait_recv()
        e3f.wait_recv()

    dy_own.wait()
    for name in mats:
        mat_whole(name)
    w.finish()


def start_call(args):
    vmem = pl.BlockSpec(memory_space=pltpu.VMEM)
    hbm = pl.BlockSpec(memory_space=pl.ANY)
    outs = [
        ((4, 2, 2, 2, 256, 512), BF16, hbm), ((4, 2, 2, 2, 256, 512), BF16, hbm),
        ((4, 2, 2, 2, 256, 128), BF16, hbm),
        ((2, 2, 2, 256, 1408), BF16, hbm), ((2, 2, 2, 256, 1408), BF16, hbm), ((2, 2, 2, 256, 1408), BF16, hbm),
        ((4, 256, 2048), BF16, hbm),
        ((256, 2048), BF16, vmem), ((4, 256, 512), BF16, vmem), ((4, 4, 256, 128), BF16, vmem),
        ((4, 256, 512), BF16, vmem), ((4, 512, 256), F32, vmem), ((4, 8, 256), F32, vmem),
        ((256, 2048), F32, vmem), ((256, 2048), BF16, vmem),
    ]
    return pl.pallas_call(
        start_kernel,
        out_shape=[jax.ShapeDtypeStruct(a, b) for a, b, _ in outs],
        in_specs=[vmem] * len(args),
        out_specs=[o[2] for o in outs],
        scratch_shapes=[
            pltpu.VMEM((2, 2, 2, 2, 256, 512), BF16),
            pltpu.VMEM((4, 2, 2, 2, 256, 128), BF16),
            pltpu.VMEM((4, 4, 256, 128), BF16),
            pltpu.VMEM((256, 512), F32),
            pltpu.SemaphoreType.DMA((96,)),
            pltpu.SemaphoreType.DMA((96,)),
            pltpu.SemaphoreType.DMA((48,)),
        ],
        compiler_params=pltpu.CompilerParams(
            collective_id=0, has_side_effects=True, vmem_limit_bytes=60 << 20
        ),
        cost_estimate=pl.CostEstimate(flops=10**10, bytes_accessed=10**8, transcendentals=0),
    )(*args)


X_SWAP = [(0, 2), (1, 3), (2, 0), (3, 1)]
C_SWAP = [(0, 1), (1, 0), (2, 3), (3, 2)]
Y_SWAP = [(0, 1), (1, 0)]
PAIR = [(0, 1), (1, 0), (2, 3), (3, 2)]
MIDDLE = [(1, 2), (2, 1)]
OUTWARD = [(1, 0), (2, 3)]
INWARD = [(0, 1), (3, 2)]


def over_x(a):
    return lax.ppermute(a, "row", X_SWAP)


def over_c(a):
    return lax.ppermute(a, "row", C_SWAP)


def over_y(a):
    return lax.ppermute(a, "dp", Y_SWAP)


def over_z(a, pairs):
    return lax.ppermute(a, "col", pairs)


def from_slot(a, s):
    return over_z(a, [((i + s) % 4, i) for i in range(4)])


def to_slot(a, s):
    return over_z(a, [(i, (i + s) % 4) for i in range(4)])


def gather_col(own, inner):
    first = over_z(own, PAIR)
    mid = over_z(own, MIDDLE)
    third_in = over_z(first, MIDDLE)
    second = jnp.where(inner, mid, over_z(mid, OUTWARD))
    third = jnp.where(inner, third_in, over_z(third_in, OUTWARD))
    return own, first, second, third


def scatter_col(parts):
    own, first, second, third = parts
    t3 = (third + over_z(third.astype(BF16), INWARD)).astype(BF16)
    t2 = (second + over_z(second.astype(BF16), INWARD)).astype(BF16)
    t1 = (first + over_z(t3, MIDDLE)).astype(BF16)
    v = over_z(t2, MIDDLE)
    w = over_z(t1, PAIR)
    return own + v.astype(F32) + w.astype(F32)


def norm_forward(values, gain_vec):
    mean_sq = jnp.mean(values * values, axis=1, keepdims=True)
    inv_rms = lax.rsqrt(mean_sq + NORM_EPS)
    unit_rows = values * inv_rms
    return (unit_rows, inv_rms, (unit_rows * gain_vec).astype(BF16))


def norm_backward(grad_norm, unit_rows, inv_rms, gain_vec):
    scaled = grad_norm * gain_vec
    inner_sum = jnp.mean(scaled * unit_rows, axis=1, keepdims=True)
    return (inv_rms * (scaled - unit_rows * inner_sum), jnp.sum(grad_norm * unit_rows, axis=0))


def shards(
    tokens, gain_attn, w_query, w_keyval, w_output, gain_mlp, w_gate, w_up, w_down, out_grad,
    document_numbers, positions, *, rows,
):
    width = tokens.shape[1]
    fast = rows == 4
    z = lax.axis_index("col")
    r = lax.axis_index("row")
    y = lax.axis_index("dp")
    inner = (z == 1) | (z == 2)
    x, c = r // 2, r % 2
    blk = width // 8

    def permuted(a, abs_order):
        if not fast:
            return a
        axis = a.ndim - 1
        pieces = []
        for hi in range(2):
            for mid in range(2):
                for lo in range(2):
                    if abs_order:
                        at = 4 * (c ^ mid) + 2 * (x ^ hi) + (y ^ lo)
                    else:
                        at = 4 * (x ^ mid) + 2 * (c ^ hi) + (y ^ lo)
                    pieces.append(lax.dynamic_slice_in_dim(a, at * blk, blk, axis))
        return jnp.concatenate(pieces, axis=axis)

    to_rel = functools.partial(permuted, abs_order=False)
    to_abs = functools.partial(permuted, abs_order=True)

    def gather_rows(block):
        return lax.all_gather(block, "row", axis=0, tiled=True)

    def gather_slots(block):
        full = gather_rows(block)
        return [full] + [from_slot(full, s) for s in (1, 2, 3)]

    tok = to_rel(tokens)
    x_in = tok.astype(F32)
    gain_one = to_rel(gain_attn)
    gain_two = to_rel(gain_mlp)
    unit_one, inv_one, normed_one = norm_forward(x_in, gain_one)
    count = tokens.shape[0]
    my_pos = lax.dynamic_slice_in_dim(positions, z * count, count, 0)
    frequency = ROPE_BASE ** (-(jnp.arange(32, dtype=F32) * 2.0 / HEAD_SIZE))
    angles = my_pos.astype(F32)[:, None] * frequency[None, :]
    co, si = jnp.cos(angles), jnp.sin(angles)
    cos_q = jnp.concatenate([co, co, co, co], axis=1)
    sin_q = jnp.concatenate([-si, si, -si, si], axis=1)
    cos_k = jnp.concatenate([co, co, jnp.ones_like(co), jnp.ones_like(co)], axis=1)
    sin_k = jnp.concatenate([-si, si, jnp.zeros_like(si), jnp.zeros_like(si)], axis=1)
    my_seg = lax.dynamic_slice_in_dim(document_numbers, z * count, count, 0)
    key_seg = jnp.concatenate(
        [lax.dynamic_slice_in_dim(document_numbers, ((z + t) % 4) * count, count, 0) for t in range(4)]
    )
    lane = jnp.arange(count, dtype=jnp.int32)
    key_at = jnp.concatenate([((z + t) % 4) * count + lane for t in range(4)])
    allowed = (key_seg[:, None] == my_seg[None, :]) & (key_at[:, None] <= (z * count + lane)[None, :])
    bias = jnp.where(allowed, 0.0, MASK_FILL).astype(F32)

    def separate():
        full = lax.all_gather(w_keyval, "row", axis=0, tiled=True)
        wkv = jnp.concatenate([full] + [from_slot(full, s) for s in (1, 2, 3)], axis=1)
        wq = gather_slots(w_query)
        wo = gather_slots(w_output.T)
        wg, wu, wd = gather_rows(w_gate), gather_rows(w_up), gather_rows(w_down.T)
        kv = call(
            kv_kernel, [((4, count, 128), BF16)], (normed_one, wkv, cos_k, sin_k), 2 * count * width * 512
        )[0]
        kv_from = [kv]
        for t in (1, 2, 3):
            kv_from.append(over_z(kv, [((i + t) % 4, i) for i in range(4) if i + t >= 4]))
        kv_of = [[kv_from[t][(s - t) % 4] for t in range(4)] for s in range(4)]
        fwd = []
        for s in range(4):
            fwd.append(
                call(
                    fwd_kernel,
                    [((count, 512), BF16), ((count, 512), BF16), ((512, count), F32), ((8, count), F32)],
                    (normed_one, wq[s], *kv_of[s], bias, cos_q, sin_q),
                    2 * count * width * 512 + 8 * 4 * count * 1024 * 256,
                )
            )
        attn = [f[1] for f in fwd]
        mid = x_in + (nt(attn[0], wo[0]) + nt(attn[1], wo[1]) + nt(attn[2], wo[2]) + nt(attn[3], wo[3]))
        n2 = norm_forward(mid, gain_two)[2]
        return wq, wo, wkv, wg, wu, wd, gather_col(dy, inner), kv_of, fwd, attn, mid, n2

    def together():
        def cut(block):
            return block.reshape(2, block.shape[0] // 2, block.shape[1])

        WQ, WO, WKV, WG, WU, WD, DY, n1, q, kv, o, ot, lse, mid, n2 = start_call(
            (
                tok, gain_one[None, :], gain_two[None, :], cut(w_query), cut(w_output.T), cut(w_keyval), cut(w_gate),
                cut(w_up), cut(w_down.T), dy, bias, cos_q, sin_q, cos_k, sin_k,
            )
        )
        wq = [WQ[s].reshape(width, 512) for s in range(4)]
        wo = [WO[s].reshape(width, 512) for s in range(4)]
        wkv = jnp.concatenate([WKV[s].reshape(width, 128) for s in range(4)], axis=1)
        kv_of = [[kv[t, (s - t) % 4] for t in range(4)] for s in range(4)]
        fwd = [(q[s], o[s], ot[s], lse[s]) for s in range(4)]
        wide = [m.reshape(width, m.shape[-1]) for m in (WG, WU, WD)]
        return wq, wo, wkv, *wide, [DY[s] for s in range(4)], kv_of, fwd, [o[s] for s in range(4)], mid, n2

    dy = to_rel(out_grad)
    wq, wo, wkv, wg, wu, wd, dys, kv_of, fwd, attn, resid_mid, normed_two = (together if fast else separate)()

    unit_two, inv_two, _ = norm_forward(resid_mid, gain_two)
    n2s = gather_col(normed_two, inner)
    outs, gns, acts, ggs, gus = [], [], [], [], []
    for s in range(4):
        gate_pre = nn(n2s[s], wg)
        up_pre = nn(n2s[s], wu)
        grad_act = nn(dys[s], wd)
        sig = jax.nn.sigmoid(gate_pre)
        silu = gate_pre * sig
        act = (silu * up_pre).astype(BF16)
        gg = (grad_act * up_pre * sig * (1.0 + gate_pre * (1.0 - sig))).astype(BF16)
        gu = (grad_act * silu).astype(BF16)
        outs.append(nt(act, wd))
        gns.append(nt(gg, wg) + nt(gu, wu))
        acts.append(act)
        ggs.append(gg)
        gus.append(gu)
    grad_norm_two = scatter_col(gns)
    block_out = (resid_mid + scatter_col(outs)).astype(BF16)
    n2_all = jnp.concatenate(n2s, axis=0)
    dy_all = jnp.concatenate(dys, axis=0)
    act_all = jnp.concatenate(acts, axis=0)
    gg_all = jnp.concatenate(ggs, axis=0)
    gu_all = jnp.concatenate(gus, axis=0)

    def ordered(lo, hi):
        return jnp.where(y == 0, jnp.concatenate([lo, hi], axis=0), jnp.concatenate([hi, lo], axis=0))

    def weight_grad(act_rel, g):
        half = width // 2
        if not fast:
            full = lax.psum_scatter(tn(act_rel, g).astype(BF16), "row", scatter_dimension=0, tiled=True)
            return lax.psum(full, "dp").astype(F32)
        got = over_c(tn(act_rel[:, half:], g).astype(BF16))
        t = tn(act_rel[:, :half], g) + got.astype(F32)
        q = half // 2
        got = over_x(t[q:].astype(BF16))
        t = (t[:q] + got.astype(F32)).astype(BF16)
        got = over_y(t).astype(F32)
        t = t.astype(F32)
        return ordered(t[: q // 2] + got[q // 2 :], t[q // 2 :] + got[: q // 2])

    def weight_grad_slots(act_rel, gs):
        half = width // 2
        if not fast:
            tot = 0.0
            for s in range(4):
                full = lax.psum_scatter(
                    tn(act_rel, gs[s]).astype(BF16), "row", scatter_dimension=0, tiled=True
                )
                tot = tot + (full if s == 0 else to_slot(full, s)).astype(F32)
            return lax.psum(tot.astype(BF16), "dp").astype(F32)
        tot = 0.0
        for s in range(4):
            got = over_c(tn(act_rel[:, half:], gs[s]).astype(BF16))
            t = tn(act_rel[:, :half], gs[s]) + got.astype(F32)
            b = blk
            t00, t01, t10, t11 = t[:b], t[b : 2 * b], t[2 * b : 3 * b], t[3 * b :]
            if s % 2:
                got = over_y(jnp.concatenate([t01, t11], axis=0).astype(BF16)).astype(F32)
                u0 = t00 + got[:b]
                u1 = t10 + got[b:]
                u = u0 + over_x(u1.astype(BF16)).astype(F32)
            else:
                got = over_x(jnp.concatenate([t10, t11], axis=0).astype(BF16)).astype(F32)
                u0 = t00 + got[:b]
                u1 = t01 + got[b:]
                u = u0 + over_y(u1.astype(BF16)).astype(F32)
            u = u.astype(BF16)
            tot = tot + (u if s == 0 else to_slot(u, s)).astype(F32)
        tot = tot.astype(BF16)
        return ordered(tot.astype(F32), over_y(tot).astype(F32))

    g_down = weight_grad(dy_all, act_all)
    g_gate = weight_grad(n2_all, gg_all)
    g_up = weight_grad(n2_all, gu_all)

    mid_norm, gain_two_term = norm_backward(grad_norm_two, unit_two, inv_two, gain_two)
    grad_mid = dy.astype(F32) + mid_norm
    branch = grad_mid.astype(BF16)
    bwd = []
    for s in range(4):
        bwd.append(
            call(
                bwd_kernel,
                [((count, 512), BF16), ((count, 128), F32), ((3, count, 128), BF16)],
                (branch, wo[s], fwd[s][0], *kv_of[s], bias, cos_q, sin_q, fwd[s][2], fwd[s][3]),
                2 * count * width * 512 + 8 * 10 * count * 1024 * 256,
                scratch=(
                    pltpu.VMEM((1024, 512), BF16),
                    pltpu.VMEM((1024, 512), BF16),
                    pltpu.VMEM((1024, 128), F32),
                    pltpu.VMEM((1024, 128), F32),
                ),
            )
        )
    got = []
    for t in (1, 2, 3):
        out = jnp.stack([bwd[s][2][t - 1] for s in range(4)])
        got.append(over_z(out, [(i, (i + t) % 4) for i in range(4) if i + t >= 4]))
    dkv = call(
        dkv_kernel,
        [((4, count, 128), BF16)],
        (*[bwd[s][1] for s in range(4)], *got, cos_k, sin_k),
        count * 512 * 8,
    )[0]
    dkv = jnp.concatenate([dkv[s] for s in range(4)], axis=1)
    dq = [bwd[s][0] for s in range(4)]
    grad_norm_one = nt(dq[0], wq[0]) + nt(dq[1], wq[1]) + nt(dq[2], wq[2]) + nt(dq[3], wq[3])
    grad_norm_one = grad_norm_one + nt(dkv, wkv)
    in_norm, gain_one_term = norm_backward(grad_norm_one, unit_one, inv_one, gain_one)
    grad_tokens = (grad_mid + in_norm).astype(BF16)
    g_output = weight_grad_slots(branch, attn)
    g_query = weight_grad_slots(normed_one, dq)
    g_keyval = weight_grad_slots(normed_one, [dkv[:, 128 * s : 128 * s + 128] for s in range(4)])

    def total(v):
        if not fast:
            return lax.psum(v, ("dp", "row", "col"))
        v = v + over_c(v)
        v = v + over_x(v)
        v = v + over_y(v)
        v = v + over_z(v, PAIR)
        return v + over_z(v, [(0, 2), (1, 3), (2, 0), (3, 1)])

    return (
        to_abs(block_out),
        to_abs(grad_tokens),
        total(to_abs(gain_one_term)),
        g_query,
        g_keyval,
        g_output.T,
        total(to_abs(gain_two_term)),
        g_gate,
        g_up,
        g_down.T,
    )


def solution(mesh):
    spec = P(("dp", "row", "col"), None)
    down = P("row", "col")
    across = P("col", "row")
    seq = P(("dp", "row"))
    return jax.shard_map(
        functools.partial(shards, rows=mesh.shape["row"]),
        mesh=mesh,
        in_specs=(spec, P(), down, down, across, P(), down, down, across, spec, seq, seq),
        out_specs=(spec, spec, P(), down, down, across, P(), down, down, across),
        check_vma=False,
    )
```

```python
import functools
import math

import jax
import jax.numpy as jnp
from jax import lax
from jax.experimental import pallas as pl
from jax.experimental.pallas import tpu as pltpu
from jax.sharding import PartitionSpec as P

HEAD_SIZE = 64
SEQUENCE_LENGTH = 1024
NORM_EPS = 1e-05
ROPE_BASE = 10000.0
MASK_FILL = -1e30
BF16 = jnp.bfloat16
F32 = jnp.float32


def nn(a, b):
    return lax.dot_general(a, b, (((1,), (0,)), ((), ())), preferred_element_type=F32)


def nt(a, b):
    return lax.dot_general(a, b, (((1,), (1,)), ((), ())), preferred_element_type=F32)


def tn(a, b):
    return lax.dot_general(a, b, (((0,), (0,)), ((), ())), preferred_element_type=F32)


def swap_halves(v):
    lane = lax.broadcasted_iota(jnp.int32, v.shape, 1)
    return jnp.where((lane % 64) < 32, pltpu.roll(v, 96, 1), pltpu.roll(v, 32, 1))


def kv_kernel(n_ref, w_ref, c_ref, s_ref, o_ref):
    kv = nn(n_ref[...], w_ref[...])
    for s in range(4):
        v = kv[:, 128 * s : 128 * s + 128]
        o_ref[s] = (v * c_ref[...] + swap_halves(v) * s_ref[...]).astype(BF16)


def load_kv(kv_refs):
    return jnp.concatenate([r[...].astype(F32) for r in kv_refs], axis=0)


def fwd_kernel(n_ref, w_ref, k0, k1, k2, k3, bias_ref, c_ref, s_ref, q_ref, o_ref, ot_ref, lse_ref):
    q = nn(n_ref[...], w_ref[...])
    kv = load_kv((k0, k1, k2, k3))
    k_low = kv[:, :64].astype(BF16)
    v_t = kv.T[64:].astype(BF16)
    for p in range(4):
        cols = slice(128 * p, 128 * p + 128)
        v = q[:, cols]
        rot = (v * c_ref[...] + swap_halves(v) * s_ref[...]) * 0.125
        rot = rot.astype(BF16)
        q_ref[:, cols] = rot
        q_t = rot.astype(F32).T.astype(BF16)
        outs = []
        for e in range(2):
            s_t = nn(k_low, q_t[64 * e : 64 * e + 64]) + bias_ref[...]
            top = jnp.max(s_t, axis=0, keepdims=True)
            ex = jnp.exp(s_t - top)
            tot = jnp.sum(ex, axis=0, keepdims=True)
            outs.append(nn(v_t, ex.astype(BF16)) * (1.0 / tot))
            lse_ref[pl.ds(2 * p + e, 1), :] = top + jnp.log(tot)
        o_t = jnp.concatenate(outs, axis=0)
        ot_ref[cols, :] = o_t
        o_ref[:, cols] = o_t.T.astype(BF16)


def bwd_kernel(
    b_ref, w_ref, q_ref, k0, k1, k2, k3, bias_ref, c_ref, s_ref, ot_ref, lse_ref,
    dq_ref, d0_ref, dr_ref, ds_scr, p_scr, dk_scr, dv_scr,
):
    ga = nn(b_ref[...], w_ref[...]).astype(BF16).astype(F32)
    kv = load_kv((k0, k1, k2, k3))
    k_low = kv[:, :64].astype(BF16)
    v_low = pltpu.roll(kv, 64, 1)[:, :64].astype(BF16)
    k_t = kv.T[:64].astype(BF16)
    lane = lax.broadcasted_iota(jnp.int32, (256, 128), 1)
    for p in range(4):
        cols = slice(128 * p, 128 * p + 128)
        qp = q_ref[:, cols].astype(F32)
        gp = ga[:, cols]
        q_t = qp.T.astype(BF16)
        g_tf = gp.T
        g_t = g_tf.astype(BF16)
        prod = g_tf * ot_ref[cols, :]
        dq_t = []
        for e in range(2):
            half = slice(64 * e, 64 * e + 64)
            s_t = nn(k_low, q_t[half]) + bias_ref[...]
            pr = jnp.exp(s_t - lse_ref[pl.ds(2 * p + e, 1), :])
            dp = nn(v_low, g_t[half])
            inner = jnp.sum(prod[half], axis=0, keepdims=True)
            ds = (pr * (dp - inner)).astype(BF16)
            ds_scr[:, 256 * e : 256 * e + 256] = ds
            p_scr[:, 256 * e : 256 * e + 256] = pr.astype(BF16)
            dq_t.append(nn(k_t, ds))
        qbd = jnp.concatenate(
            [jnp.where(lane < 64, qp, 0.0), jnp.where(lane < 64, 0.0, qp)], axis=0
        ).astype(BF16)
        gbd = jnp.concatenate(
            [jnp.where(lane < 64, gp, 0.0), jnp.where(lane < 64, 0.0, gp)], axis=0
        ).astype(BF16)
        dk = nn(ds_scr[...], qbd)
        dv = nn(p_scr[...], gbd)
        if p == 0:
            dk_scr[...] = dk
            dv_scr[...] = dv
        else:
            dk_scr[...] += dk
            dv_scr[...] += dv
        dqp = jnp.concatenate(dq_t, axis=0).T * 0.125
        dq_ref[:, cols] = (dqp * c_ref[...] - swap_halves(dqp) * s_ref[...]).astype(BF16)
    dk = dk_scr[...]
    dv = dv_scr[...]
    lane = lax.broadcasted_iota(jnp.int32, dk.shape, 1)
    both = jnp.where(lane < 64, dk + pltpu.roll(dk, 64, 1), dv + pltpu.roll(dv, 64, 1))
    d0_ref[...] = both[:256]
    for t in range(3):
        dr_ref[t] = both[256 * (t + 1) : 256 * (t + 2)].astype(BF16)


def dkv_kernel(a0, a1, a2, a3, r1, r2, r3, c_ref, s_ref, o_ref):
    own = (a0, a1, a2, a3)
    got = (r1, r2, r3)
    for s in range(4):
        v = own[s][...]
        for t in range(1, 4):
            v = v + got[t - 1][(s + t) % 4].astype(F32)
        o_ref[s] = (v * c_ref[...] - swap_halves(v) * s_ref[...]).astype(BF16)


def call(body, outs, args, flops, scratch=(), vmem=48 << 20):
    spec = pl.BlockSpec(memory_space=pltpu.VMEM)
    shapes = [jax.ShapeDtypeStruct(s, d) for s, d in outs]
    nbytes = sum(a.size * a.dtype.itemsize for a in args) + sum(
        math.prod(s) * jnp.dtype(d).itemsize for s, d in outs
    )
    return pl.pallas_call(
        body,
        out_shape=shapes,
        in_specs=[spec] * len(args),
        out_specs=[spec] * len(outs),
        scratch_shapes=list(scratch),
        compiler_params=pltpu.CompilerParams(vmem_limit_bytes=vmem),
        cost_estimate=pl.CostEstimate(flops=flops, bytes_accessed=nbytes, transcendentals=0),
    )(*args)


MESH = pl.DeviceIdType.MESH


class Wire:
    def __init__(self, send_sem, recv_sem, z):
        self.send_sem, self.recv_sem, self.z = send_sem, recv_sem, z
        self.count = 0
        self.made = []

    def to(self, where):
        r = lax.axis_index("row")
        if where == "x":
            return {"row": lax.rem(r + 2, 4)}
        if where == "c":
            return {"row": r + 1 - 2 * lax.rem(r, 2)}
        if where == "y":
            return {"dp": 1 - lax.axis_index("dp")}
        return {"col": where}

    def copy(self, src, dst, where, only=None):
        k = self.count
        self.count += 1
        cp = pltpu.make_async_remote_copy(
            src_ref=src, dst_ref=dst, send_sem=self.send_sem.at[k], recv_sem=self.recv_sem.at[k],
            device_id=self.to(where), device_id_type=MESH,
        )
        self.made.append((cp, only))
        return cp

    def sent(self, cp):
        self.made = [m for m in self.made if m[0] is not cp]
        cp.wait_send()

    def send(self, src, dst, where):
        cp = self.copy(src, dst, where)
        cp.start()
        return cp

    def finish(self):
        for cp, only in self.made:
            if only is None:
                cp.wait_send()
            else:
                pl.when(only)(cp.wait_send)


def greet(z):
    barrier = pltpu.get_barrier_semaphore()
    wire = Wire(None, None, z)
    for where in ("x", "c", "y"):
        pl.semaphore_signal(barrier, inc=1, device_id=wire.to(where), device_id_type=MESH)
    for d in (1, 2, 3):
        pl.semaphore_signal(barrier, inc=1, device_id={"col": lax.rem(z + d, 4)}, device_id_type=MESH)
    pl.semaphore_wait(barrier, 6)


def attend_slot(w_ref, n_ref, kv_scr, s, bias_ref, c_ref, s_ref, q_ref, o_ref, ot_ref, lse_ref, q_scr):
    q_scr[...] = nn(n_ref[...], w_ref[...])
    kv = jnp.concatenate([kv_scr[t, (s - t) % 4].astype(F32) for t in range(4)], axis=0)
    k_low = kv[:, :64].astype(BF16)
    v_t = kv.T[64:].astype(BF16)

    def pair(p, carry):
        at = pl.multiple_of(p * 128, 128)
        cols = pl.ds(at, 128)
        v = q_scr[:, cols]
        rot = ((v * c_ref[...] + swap_halves(v) * s_ref[...]) * 0.125).astype(BF16)
        q_ref[s, :, cols] = rot
        q_t = rot.astype(F32).T.astype(BF16)
        outs = []
        for e in range(2):
            s_t = nn(k_low, q_t[64 * e : 64 * e + 64]) + bias_ref[...]
            top = jnp.max(s_t, axis=0, keepdims=True)
            ex = jnp.exp(s_t - top)
            tot = jnp.sum(ex, axis=0, keepdims=True)
            outs.append(nn(v_t, ex.astype(BF16)) * (1.0 / tot))
            lse_ref[s, pl.ds(2 * p + e, 1), :] = top + jnp.log(tot)
        o_t = jnp.concatenate(outs, axis=0)
        ot_ref[s, cols, :] = o_t
        o_ref[s, :, cols] = o_t.T.astype(BF16)
        return carry

    lax.fori_loop(0, 4, pair, 0)


def start_kernel(
    tok_ref, gain1_ref, gain2_ref, wq_ref, wo_ref, wkv_ref, wg_ref, wu_ref, wd_ref, dy_ref, bias_ref,
    cq_ref, sq_ref, ck_ref, sk_ref,
    WQ, WO, WKV, ACT, GG, GU, OUT, n1_ref, q_ref, kv_out, o_ref, ot_ref, lse_ref, mid_ref, N2, DY, gmid_ref,
    branch_ref, gain2_out,
    wm, gn_scr, land, wbuf, wkv_scr, q_scr, gate_scr, up_scr, grad_scr, stage, out_stage, send_sem, recv_sem, loc_sem,
):
    own_scr = gmid_ref
    kv_scr = kv_out
    z = lax.axis_index("col")
    y = lax.axis_index("dp")
    inner = (z == 1) | (z == 2)
    outer = jnp.logical_not(inner)
    w = Wire(send_sem, recv_sem, z)
    locs = []

    def local(src, dst):
        cp = pltpu.make_async_copy(src, dst, loc_sem.at[len(locs)])
        cp.start()
        locs.append(cp)
        return cp

    greet(z)
    blocks = {"kv": (wkv_ref, WKV), "q": (wq_ref, WQ), "o": (wo_ref, WO)}
    ev = {}

    def start_z(name):
        ref, full = blocks[name]
        for s in (1, 2, 3):
            d = 4 - s
            ev[name, s, "z"] = w.send(ref.at[y], full.at[s, 0, 0, 0], lax.rem(z + d, 4))

    def start_own(name):
        ref, full = blocks[name]
        ev[name, 0, "x"] = w.send(ref.at[y], full.at[0, 0, 1, 0], "x")
        ev[name, 0, "own"] = [local(ref.at[y], full.at[0, 0, 0, 0]), local(ref.at[1 - y], full.at[0, 0, 0, 1])]
        ev[name, 0, "c0"] = [
            w.send(ref.at[y], full.at[0, 1, 0, 0], "c"), w.send(ref.at[1 - y], full.at[0, 1, 0, 1], "c")
        ]

    def own_second(name):
        full = blocks[name][1]
        ev[name, 0, "x"].wait_recv()
        ev[name, 0, "y"] = w.send(full.at[0, 0, 1, 0], full.at[0, 0, 1, 1], "y")

    def own_core(name):
        full = blocks[name][1]
        ev[name, 0, "y"].wait_recv()
        ev[name, 0, "c"] = w.send(full.at[0, 0, 1], full.at[0, 1, 1], "c")

    def first(name, s):
        full = blocks[name][1]
        ev[name, s, "z"].wait_recv()
        if s % 2:
            ev[name, s, 1] = w.send(full.at[s, 0, 0, 0], full.at[s, 0, 0, 1], "y")
        else:
            ev[name, s, 1] = w.send(full.at[s, 0, 0, 0], full.at[s, 0, 1, 0], "x")

    def second(name, s):
        full = blocks[name][1]
        ev[name, s, 1].wait_recv()
        if s % 2:
            ev[name, s, 2] = w.send(full.at[s, 0, 0], full.at[s, 0, 1], "x")
        else:
            ev[name, s, 2] = w.send(full.at[s, 0, :, 0], full.at[s, 0, :, 1], "y")

    def core(name, s):
        full = blocks[name][1]
        ev[name, s, 2].wait_recv()
        ev[name, s, "c"] = w.send(full.at[s, 0], full.at[s, 1], "c")

    def whole(name, s):
        ev[name, s, "c"].wait_recv()
        if s == 0:
            for cp in ev[name, 0, "c0"]:
                cp.wait_recv()
            for cp in ev[name, 0, "own"]:
                cp.wait()

    mats = {"g": (wg_ref, wm.at[0]), "u": (wu_ref, wm.at[1]), "d": (wd_ref, wm.at[2])}

    def mat_start(name):
        ref, full = mats[name]
        ev[name, "x"] = w.send(ref.at[y], full.at[0, 1, 0], "x")
        ev[name, "own"] = [local(ref.at[y], full.at[0, 0, 0]), local(ref.at[1 - y], full.at[0, 0, 1])]
        ev[name, "c0"] = [
            w.send(ref.at[y], full.at[1, 0, 0], "c"), w.send(ref.at[1 - y], full.at[1, 0, 1], "c")
        ]

    def mat_second(name):
        full = mats[name][1]
        ev[name, "x"].wait_recv()
        ev[name, "y"] = w.send(full.at[0, 1, 0], full.at[0, 1, 1], "y")

    def mat_core(name):
        full = mats[name][1]
        ev[name, "y"].wait_recv()
        ev[name, "c"] = w.send(full.at[0, 1], full.at[1, 1], "c")

    def mat_whole(name):
        ev[name, "c"].wait_recv()
        for cp in ev[name, "c0"]:
            cp.wait_recv()
        for cp in ev[name, "own"]:
            cp.wait()

    buddy = z + 1 - 2 * lax.rem(z, 2)
    middle = lax.rem(7 - z, 4)

    def some(cond, cp):
        pl.when(cond)(cp.start)
        return cp

    def rows_start(full):
        f = w.send(full.at[0], full.at[1], buddy)
        m = some(inner, w.copy(full.at[0], full.at[2], middle, only=inner))
        return [f, m]

    def rows_first(full, c):
        c[0].wait_recv()
        c.append(some(inner, w.copy(full.at[1], full.at[3], middle, only=inner)))

    def rows_second(full, c):
        pl.when(inner)(c[1].wait_recv)
        c.append(some(inner, w.copy(full.at[2], full.at[2], buddy, only=inner)))

    def rows_third(full, c):
        pl.when(inner)(c[2].wait_recv)
        c.append(some(inner, w.copy(full.at[3], full.at[3], buddy, only=inner)))

    def rows_have_second(c):
        pl.when(outer)(c[3].wait_recv)

    def rows_have_third(c):
        pl.when(outer)(c[4].wait_recv)

    start_z("kv")
    start_own("kv")
    start_z("q")
    start_own("q")
    mat_start("g")
    dy_own = local(dy_ref, DY.at[0])

    def attention(wbuf, wkv_scr, q_scr):
        def norm_one(i, carry):
            at = pl.ds(pl.multiple_of(i * 32, 32), 32)
            x_in = tok_ref[at, :].astype(F32)
            inv = lax.rsqrt(jnp.mean(x_in * x_in, axis=1, keepdims=True) + NORM_EPS)
            n1_ref[at, :] = (x_in * inv * gain1_ref[...]).astype(BF16)
            mid_ref[at, :] = x_in
            return carry

        lax.fori_loop(0, 8, norm_one, 0)
        for t in (1, 2, 3):

            @pl.when(z + t < 4)
            def _():
                kv_scr[t] = jnp.zeros_like(kv_scr[t])

        own_second("kv")
        for s in (1, 2, 3):
            first("kv", s)
        own_second("q")
        for s in (1, 2, 3):
            second("kv", s)
        own_core("kv")
        for s in (1, 2, 3):
            first("q", s)
        start_z("o")
        start_own("o")
        mat_second("g")
        for s in (1, 2, 3):
            core("kv", s)
        own_core("q")
        mat_start("u")
        got = []
        for s in range(4):
            whole("kv", s)
            if s < 2:
                got.append(local(WKV.at[s], wkv_scr.at[s]))
        for s in range(4):
            got[s].wait()
            kv = nn(n1_ref[...], wkv_scr[s % 2].reshape(2048, 128))
            if s < 2:
                got.append(local(WKV.at[s + 2], wkv_scr.at[s]))
            kv_scr[0, s] = (kv * ck_ref[...] + swap_halves(kv) * sk_ref[...]).astype(BF16)
        kv_cp = {}
        for d in (1, 2, 3):
            cp = w.copy(kv_scr.at[0], kv_scr.at[4 - d], lax.rem(z + d, 4), only=z + d < 4)
            kv_cp[4 - d] = cp
            pl.when(z + d < 4)(cp.start)
        for s in (1, 2, 3):
            second("q", s)
        whole("q", 0)
        cps = [local(WQ.at[0], wbuf.at[0])]
        dy_own.wait()
        dyc = rows_start(DY)
        for s in (1, 2, 3):
            core("q", s)
        own_second("o")
        mat_core("g")
        mat_second("u")
        for t in (1, 2, 3):
            pl.when(z + t >= 4)(kv_cp[t].wait_recv)

        def attend(s):
            cps[s].wait()
            attend_slot(
                wbuf.at[s % 2].reshape(2048, 512), n1_ref, kv_scr, s, bias_ref, cq_ref, sq_ref, q_ref, o_ref,
                ot_ref, lse_ref, q_scr,
            )

        for s in (1, 2, 3):
            first("o", s)
        whole("q", 1)
        cps.append(local(WQ.at[1], wbuf.at[1]))
        attend(0)
        own_core("o")
        for s in (1, 2, 3):
            second("o", s)
        mat_start("d")
        rows_first(DY, dyc)
        whole("q", 2)
        cps.append(local(WQ.at[2], wbuf.at[0]))
        attend(1)
        rows_second(DY, dyc)
        mat_core("u")
        for s in (1, 2, 3):
            core("o", s)
        whole("q", 3)
        cps.append(local(WQ.at[3], wbuf.at[1]))
        attend(2)
        mat_second("d")
        rows_third(DY, dyc)
        attend(3)
        oc = []
        for s in range(4):
            whole("o", s)
            if s < 2:
                oc.append(local(WO.at[s], wbuf.at[s % 2]))
        for s in range(4):
            oc[s].wait()

            def columns(c, carry):
                at = pl.ds(pl.multiple_of(c * 512, 512), 512)
                mid_ref[:, at] += nt(o_ref[s], wbuf[s % 2, c // 2, c % 2].reshape(512, 512))
                return carry

            lax.fori_loop(0, 4, columns, 0)
            if s < 2:
                oc.append(local(WO.at[s + 2], wbuf.at[s % 2]))

        def norm_two(i, carry):
            at = pl.ds(pl.multiple_of(i * 32, 32), 32)
            mid = mid_ref[at, :]
            inv = lax.rsqrt(jnp.mean(mid * mid, axis=1, keepdims=True) + NORM_EPS)
            N2[0, at, :] = (mid * inv * gain2_ref[...]).astype(BF16)
            return carry

        lax.fori_loop(0, 8, norm_two, 0)
        ev["dy"] = dyc

    attention(wbuf, wkv_scr, q_scr)

    n2c = rows_start(N2)
    dyc = ev["dy"]
    mat_core("d")
    for name in mats:
        mat_whole(name)
    t3, t2, t1, last_v, last_w = (land.at[i] for i in range(5))
    rs = {}

    def feed_forward(gate_scr, up_scr, grad_scr, stage, out_stage):
        def slot(a, stored):
            dy_a = DY[a]
            n2_a = N2[a]
            gate_scr[...] = nn(n2_a, wm[0].reshape(2048, 1408))
            up_scr[...] = nn(n2_a, wm[1].reshape(2048, 1408))
            grad_scr[...] = nn(dy_a, wm[2].reshape(2048, 1408))
            for cp in stored:
                cp.wait()

            def rows(i, carry):
                at = pl.ds(pl.multiple_of(i * 32, 32), 32)
                gate = gate_scr[at, :]
                up = up_scr[at, :]
                ga = grad_scr[at, :]
                sig = 1.0 / (1.0 + jnp.exp(-gate))
                silu = gate * sig
                stage[0, at, :] = (silu * up).astype(BF16)
                stage[1, at, :] = (ga * up * sig * (1.0 + gate * (1.0 - sig))).astype(BF16)
                stage[2, at, :] = (ga * silu).astype(BF16)
                return carry

            lax.fori_loop(0, 8, rows, 0)

            def columns(c, carry):
                at = pl.ds(pl.multiple_of(c * 512, 512), 512)
                k, i = c // 2, c % 2
                out_stage[:, at] = nt(stage[0], wm[2, k, i].reshape(512, 1408)).astype(BF16)
                gn = nt(stage[1], wm[0, k, i].reshape(512, 1408)) + nt(stage[2], wm[1, k, i].reshape(512, 1408))
                if a == 0:
                    own_scr[:, at] = gn
                else:
                    gn_scr[a - 1, :, at] = gn.astype(BF16)
                return carry

            lax.fori_loop(0, 4, columns, 0)
            return [
                local(stage.at[0], ACT.at[a]), local(stage.at[1], GG.at[a]), local(stage.at[2], GU.at[a]),
                local(out_stage, OUT.at[a]),
            ]

        stored = slot(0, [])
        rows_have_second(dyc)
        rows_have_third(dyc)
        rows_first(N2, n2c)
        rows_second(N2, n2c)
        stored = slot(1, stored)
        rs["w"] = w.copy(gn_scr.at[0], last_w, buddy)
        pl.when(outer)(rs["w"].start)
        rows_have_second(n2c)
        rows_third(N2, n2c)
        stored = slot(2, stored)
        rs["t2"] = some(outer, w.copy(gn_scr.at[1], t2, buddy, only=outer))
        rows_have_third(n2c)
        stored = slot(3, stored)
        rs["t3"] = some(outer, w.copy(gn_scr.at[2], t3, buddy, only=outer))
        for cp in stored:
            cp.wait()

    feed_forward(gate_scr, up_scr, grad_scr, stage, out_stage)

    v_cp = w.copy(gn_scr.at[1], last_v, middle, only=inner)
    t1_cp = w.copy(gn_scr.at[2], t1, middle, only=inner)

    def add_rows(into, other):
        def body(i, carry):
            at = pl.ds(pl.multiple_of(i * 32, 32), 32)
            into[at, :] = (into[at, :].astype(F32) + other[at, :].astype(F32)).astype(into.dtype)
            return carry

        lax.fori_loop(0, 8, body, 0)

    @pl.when(inner)
    def _():
        rs["t2"].wait_recv()
        add_rows(gn_scr.at[1], t2)
        v_cp.start()
        rs["t3"].wait_recv()
        add_rows(gn_scr.at[2], t3)
        t1_cp.start()
        t1_cp.wait_recv()
        add_rows(gn_scr.at[0], t1)
        rs["w"].start()
        v_cp.wait_recv()
        add_rows(own_scr, last_v)

    rs["w"].wait_recv()
    gain2_out[...] = jnp.zeros_like(gain2_out)

    def norm_back(i, carry):
        at = pl.ds(pl.multiple_of(i * 32, 32), 32)
        gn = own_scr[at, :] + last_w[at, :].astype(F32)
        mid = mid_ref[at, :]
        inv = lax.rsqrt(jnp.mean(mid * mid, axis=1, keepdims=True) + NORM_EPS)
        unit = mid * inv
        gain2_out[...] += jnp.sum(gn * unit, axis=0, keepdims=True)
        scaled = gn * gain2_ref[...]
        inside = jnp.mean(scaled * unit, axis=1, keepdims=True)
        gmid = DY[0, at, :].astype(F32) + inv * (scaled - unit * inside)
        gmid_ref[at, :] = gmid
        out_stage[at, :] = gmid.astype(BF16)
        return carry

    lax.fori_loop(0, 8, norm_back, 0)
    local(out_stage, branch_ref).wait()
    w.finish()


def start_call(args):
    vmem = pl.BlockSpec(memory_space=pltpu.VMEM)
    hbm = pl.BlockSpec(memory_space=pl.ANY)
    outs = [
        ((4, 2, 2, 2, 256, 512), BF16, hbm), ((4, 2, 2, 2, 256, 512), BF16, hbm),
        ((4, 2, 2, 2, 256, 128), BF16, hbm),
        ((4, 256, 1408), BF16, hbm), ((4, 256, 1408), BF16, hbm), ((4, 256, 1408), BF16, hbm),
        ((4, 256, 2048), BF16, hbm),
        ((256, 2048), BF16, vmem), ((4, 256, 512), BF16, vmem), ((4, 4, 256, 128), BF16, vmem),
        ((4, 256, 512), BF16, vmem), ((4, 512, 256), F32, vmem), ((4, 8, 256), F32, vmem),
        ((256, 2048), F32, vmem), ((4, 256, 2048), BF16, vmem), ((4, 256, 2048), BF16, vmem),
        ((256, 2048), F32, vmem), ((256, 2048), BF16, hbm), ((1, 2048), F32, vmem),
    ]
    return pl.pallas_call(
        start_kernel,
        out_shape=[jax.ShapeDtypeStruct(a, b) for a, b, _ in outs],
        in_specs=[vmem] * 6 + [hbm] * 4 + [vmem] * (len(args) - 10),
        out_specs=[o[2] for o in outs],
        scratch_shapes=[
            pltpu.VMEM((3, 2, 2, 2, 256, 1408), BF16),
            pltpu.VMEM((3, 256, 2048), BF16),
            pltpu.VMEM((5, 256, 2048), BF16),
            pltpu.VMEM((2, 2, 2, 2, 256, 512), BF16),
            pltpu.VMEM((2, 2, 2, 2, 256, 128), BF16),
            pltpu.VMEM((256, 512), F32),
            pltpu.VMEM((256, 1408), F32),
            pltpu.VMEM((256, 1408), F32),
            pltpu.VMEM((256, 1408), F32),
            pltpu.VMEM((3, 256, 1408), BF16),
            pltpu.VMEM((256, 2048), BF16),
            pltpu.SemaphoreType.DMA((96,)),
            pltpu.SemaphoreType.DMA((96,)),
            pltpu.SemaphoreType.DMA((64,)),
        ],
        compiler_params=pltpu.CompilerParams(
            collective_id=0, has_side_effects=True, vmem_limit_bytes=67043328
        ),
        cost_estimate=pl.CostEstimate(flops=10**10, bytes_accessed=10**8, transcendentals=0),
    )(*args)


def attend_back(s, kv_of, ga_scr, q_ref, bias_ref, c_ref, s_ref, ot_ref, lse_ref, dq_scr, d0, dr, ds_scr, p_scr, dk_scr, dv_scr):
    kv = jnp.concatenate([kv_of[t, (s - t) % 4].astype(F32) for t in range(4)], axis=0)
    k_low = kv[:, :64].astype(BF16)
    v_low = pltpu.roll(kv, 64, 1)[:, :64].astype(BF16)
    k_t = kv.T[:64].astype(BF16)
    dk_scr[...] = jnp.zeros_like(dk_scr)
    dv_scr[...] = jnp.zeros_like(dv_scr)

    def pair(p, carry):
        cols = pl.ds(pl.multiple_of(p * 128, 128), 128)
        lane = lax.broadcasted_iota(jnp.int32, (256, 128), 1)
        qp = q_ref[s, :, cols].astype(F32)
        gp = ga_scr[:, cols]
        q_t = qp.T.astype(BF16)
        g_tf = gp.T
        g_t = g_tf.astype(BF16)
        prod = g_tf * ot_ref[cols, :]
        dq_t = []
        for e in range(2):
            half = slice(64 * e, 64 * e + 64)
            s_t = nn(k_low, q_t[half]) + bias_ref[...]
            pr = jnp.exp(s_t - lse_ref[s, pl.ds(2 * p + e, 1), :])
            dp = nn(v_low, g_t[half])
            inner = jnp.sum(prod[half], axis=0, keepdims=True)
            ds = (pr * (dp - inner)).astype(BF16)
            ds_scr[:, 256 * e : 256 * e + 256] = ds
            p_scr[:, 256 * e : 256 * e + 256] = pr.astype(BF16)
            dq_t.append(nn(k_t, ds))
        qbd = jnp.concatenate(
            [jnp.where(lane < 64, qp, 0.0), jnp.where(lane < 64, 0.0, qp)], axis=0
        ).astype(BF16)
        gbd = jnp.concatenate(
            [jnp.where(lane < 64, gp, 0.0), jnp.where(lane < 64, 0.0, gp)], axis=0
        ).astype(BF16)
        dk_scr[...] += nn(ds_scr[...], qbd)
        dv_scr[...] += nn(p_scr[...], gbd)
        dqp = jnp.concatenate(dq_t, axis=0).T * 0.125
        dq_scr[s, :, cols] = (dqp * c_ref[...] - swap_halves(dqp) * s_ref[...]).astype(BF16)
        return carry

    lax.fori_loop(0, 4, pair, 0)
    dk = dk_scr[...]
    dv = dv_scr[...]
    lane = lax.broadcasted_iota(jnp.int32, dk.shape, 1)
    both = jnp.where(lane < 64, dk + pltpu.roll(dk, 64, 1), dv + pltpu.roll(dv, 64, 1))
    d0[s] = both[:256]
    for t in range(3):
        dr[t, s] = both[256 * (t + 1) : 256 * (t + 2)].astype(BF16)


def add_into(into, one, other, step=32):
    def body(i, carry):
        at = pl.ds(pl.multiple_of(i * step, step), step)
        into[at, :] = (one[at, :].astype(F32) + other[at, :].astype(F32)).astype(into.dtype)
        return carry

    lax.fori_loop(0, into.shape[0] // step, body, 0)


def end_kernel(
    PD, PG, PU, WQ, WO, WKV, OT, branch_ref, gmid_ref, tok_ref, gain1_ref, gain2t_ref, n1_ref, q_ref, kv_ref, o_ref,
    lse_ref, bias_ref, cq_ref, sq_ref, ck_ref, sk_ref,
    gtok_ref, gains_ref, GD, GGT, GUP, GQ, GO, GKV, LCM, LCO, LCQ, LCK, LYM, LX,
    TM, TO, TQ, TK, S, L1O, L1Q, L1K, L2O, L2Q, L2K, LZO, LZQ, LZK, FO, FQ, FK, YO, YQ, YK,
    wbuf, wk, act_t, ga_scr, dq_scr, dkv_scr, d0, dr, ld, ds_scr, p_scr, dk_scr, dv_scr, gn_scr, pre, ot_scr, fin, gsum, gland,
    send_sem, recv_sem, loc_sem,
):
    z = lax.axis_index("col")
    y = lax.axis_index("dp")
    r = lax.axis_index("row")
    x, c = r // 2, lax.rem(r, 2)
    w = Wire(send_sem, recv_sem, z)
    locs = []

    def local(src, dst):
        cp = pltpu.make_async_copy(src, dst, loc_sem.at[len(locs)])
        cp.start()
        locs.append(cp)
        return cp

    greet(z)
    parts = (PD, PG, PU)
    finals = (GD, GGT, GUP)
    mc = [w.send(parts[m].at[1], LCM.at[m], "c") for m in range(3)]
    wo_cp = {0: local(WO.at[0], wbuf.at[0])}
    wq_cp = {0: local(WQ.at[0], wbuf.at[1])}
    ot_cp = {0: local(OT.at[0], ot_scr)}

    def turned(src):
        for j in range(8):
            act_t[256 * j : 256 * j + 256, :] = src[:, 256 * j : 256 * j + 256].astype(F32).T.astype(BF16)

    def grad_part(g, keep, give, cols):
        for i in range(2):
            for j in range(2):
                at = 512 * i + 256 * j
                give[i, j, :, cols] = nn(act_t[1024 + at : 1024 + at + 256, :], g).astype(BF16)
        for i in range(2):
            for j in range(2):
                at = 512 * i + 256 * j
                keep[i, j, :, cols] = nn(act_t[at : at + 256, :], g).astype(BF16)

    every = slice(0, 512)
    turned(branch_ref)
    oc = []
    for s in range(4):
        if s > 1:
            w.sent(oc[s - 2])
        grad_part(o_ref[s], TO.at[s], S.at[s % 2], every)
        oc.append(w.send(S.at[s % 2], LCO.at[s], "c"))

    slots = [0]

    def wide_core(m):
        mc[m].wait_recv()
        order = [(1, 0), (1, 1), (0, 0), (0, 1)]

        def load(n):
            i, j = order[n]
            b = slots[0] % 2
            slots[0] += 1
            return b, local(parts[m].at[0, i, j], pre.at[b, 0]), local(LCM.at[m, i, j], pre.at[b, 1])

        nxt = load(0)
        for n, (i, j) in enumerate(order):
            b, c0, c1 = nxt
            if n < 3:
                nxt = load(n + 1)
            c0.wait()
            c1.wait()
            add_into(TM.at[m, i, j], pre.at[b, 0], pre.at[b, 1])

    xs, ys = {}, {}

    def wide_x(m, j):
        xs[m, j] = w.send(TM.at[m, 1, j], LX.at[m, j], "x")

    def wide_y(m, j):
        xs[m, j].wait_recv()
        b = slots[0] % 2
        slots[0] += 1
        local(LX.at[m, j], pre.at[b, 0]).wait()
        add_into(TM.at[m, 0, j], TM.at[m, 0, j], pre.at[b, 0])
        ys[m, j] = w.send(TM.at[m, 0, j], LYM.at[m, 1 - j], "y")

    outs = []

    def wide_end(m, j):
        ys[m, 1 - j].wait_recv()
        b = slots[0] % 2
        slots[0] += 1
        local(LYM.at[m, j], pre.at[b, 0]).wait()
        if len(outs) >= 1:
            outs[-1].wait()
        add_into(fin, TM.at[m, 0, j], pre.at[b, 0])
        outs.append(local(fin, finals[m].at[lax.rem(y + j, 2)]))

    class Narrow:
        def __init__(self, T, LC, L1, L2, LZ, F, Y, out, width):
            self.T, self.LC, self.L1, self.L2, self.LZ, self.F, self.Y, self.out = T, LC, L1, L2, LZ, F, Y, out
            self.cps = {}
            self.width = width

        def core(self, s, cp):
            cp.wait_recv()
            tiles = [(i, j, pre.at[i, j, :, pl.ds(0, 512)]) for i in range(2) for j in range(2)]
            loads = [local(self.LC.at[s, i, j], t) for i, j, t in tiles]
            for (i, j, t), cp in zip(tiles, loads):
                cp.wait()
                add_into(self.T.at[s, i, j], self.T.at[s, i, j], t)

        def first(self, s):
            if s % 2:
                self.cps[s, 1] = w.send(self.T.at[s, :, 1], self.L1.at[s], "y")
            else:
                self.cps[s, 1] = w.send(self.T.at[s, 1], self.L1.at[s], "x")

        def second(self, s):
            self.cps[s, 1].wait_recv()
            for b in range(2):
                mine = self.T.at[s, b, 0] if s % 2 else self.T.at[s, 0, b]
                add_into(mine, mine, self.L1.at[s, b])
            if s % 2:
                self.cps[s, 2] = w.send(self.T.at[s, 1, 0], self.L2.at[s], "x")
            else:
                self.cps[s, 2] = w.send(self.T.at[s, 0, 1], self.L2.at[s], "y")

        def third(self, s):
            self.cps[s, 2].wait_recv()
            mine = self.T.at[s, 0, 0]
            add_into(mine, mine, self.L2.at[s])
            if s:
                self.cps[s, 3] = w.send(mine, self.LZ.at[s - 1], lax.rem(z + s, 4))

        def fourth(self):
            for s in (1, 2, 3):
                self.cps[s, 3].wait_recv()

            def body(i, carry):
                at = pl.ds(pl.multiple_of(i * 32, 32), 32)
                tot = self.T[0, 0, 0, at, :].astype(F32)
                for s in range(3):
                    tot = tot + self.LZ[s, at, :].astype(F32)
                self.F[at, :] = tot.astype(BF16)
                return carry

            lax.fori_loop(0, 8, body, 0)
            self.cps["y"] = w.send(self.F, self.Y, "y")

        def last(self):
            self.cps["y"].wait_recv()
            self.out[y] = self.F[...].astype(F32)
            self.out[1 - y] = self.Y[...].astype(F32)

    wo_g = Narrow(TO, LCO, L1O, L2O, LZO, FO, YO, GO, 512)
    wq_g = Narrow(TQ, LCQ, L1Q, L2Q, LZQ, FQ, YQ, GQ, 512)
    qc = []

    def attend(s):
        wo_cp[s].wait()
        ga_scr[...] = nn(branch_ref[...], wbuf[0].reshape(2048, 512)).astype(BF16).astype(F32)
        if s < 3:
            wo_cp[s + 1] = local(WO.at[s + 1], wbuf.at[0])
        ot_cp[s].wait()
        attend_back(
            s, kv_ref, ga_scr, q_ref, bias_ref, cq_ref, sq_ref, ot_scr, lse_ref, dq_scr, d0, dr, ds_scr, p_scr,
            dk_scr, dv_scr,
        )
        if s < 3:
            ot_cp[s + 1] = local(OT.at[s + 1], ot_scr)
        wq_cp[s].wait()

        def columns(i, carry):
            at = pl.ds(pl.multiple_of(i * 512, 512), 512)
            part = nt(dq_scr[s], wbuf[1, i // 2, i % 2].reshape(512, 512))
            if s:
                gn_scr[:, at] += part
            else:
                gn_scr[:, at] = part
            return carry

        lax.fori_loop(0, 4, columns, 0)
        if s < 3:
            wq_cp[s + 1] = local(WQ.at[s + 1], wbuf.at[1])
        w.sent(oc[s + 2] if s < 2 else qc[s - 2])
        grad_part(dq_scr[s], TQ.at[s], S.at[s % 2], every)
        qc.append(w.send(S.at[s % 2], LCQ.at[s], "c"))

    wide_core(0)
    wide_x(0, 0)
    wide_x(0, 1)
    for s in (1, 3, 0, 2):
        wo_g.core(s, oc[s])
        if s % 2:
            wo_g.first(s)
    turned(n1_ref)
    attend(0)
    wide_core(1)
    wide_y(0, 0)
    wide_x(1, 0)
    attend(1)
    wide_y(0, 1)
    wide_x(1, 1)
    attend(2)
    wide_core(2)
    wide_y(1, 0)
    wide_x(2, 0)
    attend(3)
    dk_cp = {}
    for t in (1, 2, 3):
        cp = w.copy(dr.at[t - 1], ld.at[t - 1], lax.rem(z + t, 4), only=z + t >= 4)
        dk_cp[t] = cp
        pl.when(z + t >= 4)(cp.start)
    wk_cp = {0: local(WKV.at[0], wk.at[0]), 1: local(WKV.at[1], wk.at[1])}
    wide_y(1, 1)
    wide_x(2, 1)
    for s in (1, 3, 0, 2):
        wq_g.core(s, qc[s])
        if s % 2:
            wq_g.first(s)
    for s in (1, 3):
        wo_g.second(s)
    for s in (0, 2):
        wo_g.first(s)

    for s in range(4):
        dkv_scr[:, 128 * s : 128 * s + 128] = d0[s]
    for t in (1, 2, 3):

        @pl.when(z < t)
        def _():
            dk_cp[t].wait_recv()
            for s in range(4):
                dkv_scr[:, 128 * s : 128 * s + 128] += ld[t - 1, (s + t) % 4].astype(F32)

    for s in range(4):
        cols = slice(128 * s, 128 * s + 128)
        v = dkv_scr[:, cols]
        dkv = (v * ck_ref[...] - swap_halves(v) * sk_ref[...]).astype(BF16)
        wk_cp[s].wait()

        def columns(i, carry):
            at = pl.ds(pl.multiple_of(i * 512, 512), 512)
            gn_scr[:, at] += nt(dkv, wk[s % 2, i // 2, i % 2].reshape(512, 128))
            return carry

        lax.fori_loop(0, 4, columns, 0)
        if s < 2:
            wk_cp[s + 2] = local(WKV.at[s + 2], wk.at[s % 2])
        if s == 0:
            w.sent(qc[2])
        grad_part(dkv, TK.at[0], S.at[0], cols)
    kc = w.send(S.at[0], LCK.at[0], "c")
    wide_y(2, 0)

    gsum[0:1, :] = jnp.zeros((1, 2048), F32)

    def norm_back(i, carry):
        at = pl.ds(pl.multiple_of(i * 32, 32), 32)
        gn = gn_scr[at, :]
        x_in = tok_ref[at, :].astype(F32)
        inv = lax.rsqrt(jnp.mean(x_in * x_in, axis=1, keepdims=True) + NORM_EPS)
        unit = x_in * inv
        gsum[0:1, :] += jnp.sum(gn * unit, axis=0, keepdims=True)
        scaled = gn * gain1_ref[...]
        inside = jnp.mean(scaled * unit, axis=1, keepdims=True)
        gtok_ref[at, :] = (gmid_ref[at, :] + inv * (scaled - unit * inside)).astype(BF16)
        return carry

    lax.fori_loop(0, 8, norm_back, 0)
    gsum[1:2, :] = gain2t_ref[...]
    for hi in range(2):
        for mid in range(2):
            for lo in range(2):
                at = 4 * (c ^ mid) + 2 * (x ^ hi) + (y ^ lo)
                gains_ref[:, 256 * (4 * hi + 2 * mid + lo) : 256 * (4 * hi + 2 * mid + lo) + 256] = gsum[
                    :, pl.ds(pl.multiple_of(at * 256, 256), 256)
                ]
    steps = ["c", "x", "y", z + 1 - 2 * lax.rem(z, 2), lax.rem(z + 2, 4)]
    gain_cp = []

    def gain_next(n):
        gland[5 + n] = gains_ref[...]
        gain_cp.append(w.send(gland.at[5 + n], gland.at[n], steps[n]))

    def gain_add(n):
        gain_cp[n].wait_recv()
        gains_ref[...] += gland[n]

    gain_next(0)
    wide_y(2, 1)
    wide_end(0, 0)
    gain_add(0)
    gain_next(1)
    wide_end(0, 1)
    wk_g = Narrow(TK, LCK, L1K, L2K, LZK, FK, YK, GKV, 128)
    wk_g.core(0, kc)
    for s in (0, 2):
        wo_g.second(s)
    for s in (1, 3):
        wo_g.third(s)
    for s in (0, 2):
        wq_g.first(s)
    wk_g.first(0)
    gain_add(1)
    gain_next(2)
    for s in (1, 3):
        wq_g.second(s)
    wide_end(1, 0)
    wide_end(1, 1)
    gain_add(2)
    gain_next(3)
    for s in (0, 2):
        wo_g.third(s)
    wide_end(2, 0)
    gain_add(3)
    gain_next(4)
    for s in (0, 2):
        wq_g.second(s)
    wk_g.second(0)
    wo_g.fourth()
    for s in (1, 3):
        wq_g.third(s)
    wide_end(2, 1)
    gain_add(4)
    for s in (0, 2):
        wq_g.third(s)
    wk_g.cps[0, 2].wait_recv()
    add_into(TK.at[0, 0, 0], TK.at[0, 0, 0], L2K.at[0])
    for s in (1, 2, 3):
        wk_g.cps[s, 3] = w.send(TK.at[0, 0, 0, :, pl.ds(128 * s, 128)], LZK.at[s - 1], lax.rem(z + s, 4))
    wo_g.last()
    wq_g.fourth()
    for s in (1, 2, 3):
        wk_g.cps[s, 3].wait_recv()
    tot = TK[0, 0, 0, :, 0:128].astype(F32)
    for s in range(3):
        tot = tot + LZK[s].astype(F32)
    FK[...] = tot.astype(BF16)
    wk_g.cps["y"] = w.send(FK, YK, "y")
    wq_g.last()
    wk_g.last()
    outs[-1].wait()
    w.finish()


def end_call(args):
    vmem = pl.BlockSpec(memory_space=pltpu.VMEM)
    hbm = pl.BlockSpec(memory_space=pl.ANY)
    outs = [
        ((256, 2048), BF16, vmem), ((2, 2048), F32, vmem),
        ((2, 256, 1408), F32, hbm), ((2, 256, 1408), F32, hbm), ((2, 256, 1408), F32, hbm),
        ((2, 256, 512), F32, vmem), ((2, 256, 512), F32, vmem), ((2, 256, 128), F32, vmem),
        ((3, 2, 2, 256, 1408), BF16, hbm), ((4, 2, 2, 256, 512), BF16, hbm), ((4, 2, 2, 256, 512), BF16, hbm),
        ((1, 2, 2, 256, 512), BF16, hbm), ((3, 2, 256, 1408), BF16, hbm), ((3, 2, 256, 1408), BF16, hbm),
    ]
    scratch = [
        ((3, 2, 2, 256, 1408), BF16), ((4, 2, 2, 256, 512), BF16), ((4, 2, 2, 256, 512), BF16), ((1, 2, 2, 256, 512), BF16),
        ((2, 2, 2, 256, 512), BF16),
        ((4, 2, 256, 512), BF16), ((4, 2, 256, 512), BF16), ((1, 2, 256, 512), BF16),
        ((4, 256, 512), BF16), ((4, 256, 512), BF16), ((1, 256, 512), BF16),
        ((3, 256, 512), BF16), ((3, 256, 512), BF16), ((3, 256, 128), BF16),
        ((256, 512), BF16), ((256, 512), BF16), ((256, 128), BF16),
        ((256, 512), BF16), ((256, 512), BF16), ((256, 128), BF16),
        ((2, 2, 2, 2, 256, 512), BF16), ((2, 2, 2, 2, 256, 128), BF16), ((2048, 256), BF16), ((256, 512), F32),
        ((4, 256, 512), BF16), ((256, 512), F32), ((4, 256, 128), F32), ((3, 4, 256, 128), BF16), ((3, 4, 256, 128), BF16),
        ((1024, 512), BF16), ((1024, 512), BF16), ((1024, 128), F32), ((1024, 128), F32), ((256, 2048), F32),
        ((2, 2, 256, 1408), BF16), ((512, 256), F32), ((256, 1408), F32), ((2, 2048), F32), ((10, 2, 2048), F32),
    ]
    return pl.pallas_call(
        end_kernel,
        out_shape=[jax.ShapeDtypeStruct(a, b) for a, b, _ in outs],
        in_specs=[hbm] * 7 + [vmem] * (len(args) - 7),
        out_specs=[o[2] for o in outs],
        scratch_shapes=[pltpu.VMEM(a, b) for a, b in scratch]
        + [pltpu.SemaphoreType.DMA((96,)), pltpu.SemaphoreType.DMA((96,)), pltpu.SemaphoreType.DMA((96,))],
        compiler_params=pltpu.CompilerParams(
            collective_id=1, has_side_effects=True, vmem_limit_bytes=67043328
        ),
        cost_estimate=pl.CostEstimate(flops=10**11, bytes_accessed=2 * 10**8, transcendentals=0),
    )(*args)


X_SWAP = [(0, 2), (1, 3), (2, 0), (3, 1)]
C_SWAP = [(0, 1), (1, 0), (2, 3), (3, 2)]
Y_SWAP = [(0, 1), (1, 0)]
PAIR = [(0, 1), (1, 0), (2, 3), (3, 2)]
MIDDLE = [(1, 2), (2, 1)]
OUTWARD = [(1, 0), (2, 3)]
INWARD = [(0, 1), (3, 2)]


def over_x(a):
    return lax.ppermute(a, "row", X_SWAP)


def over_c(a):
    return lax.ppermute(a, "row", C_SWAP)


def over_y(a):
    return lax.ppermute(a, "dp", Y_SWAP)


def over_z(a, pairs):
    return lax.ppermute(a, "col", pairs)


def from_slot(a, s):
    return over_z(a, [((i + s) % 4, i) for i in range(4)])


def to_slot(a, s):
    return over_z(a, [(i, (i + s) % 4) for i in range(4)])


def gather_col(own, inner):
    first = over_z(own, PAIR)
    mid = over_z(own, MIDDLE)
    third_in = over_z(first, MIDDLE)
    second = jnp.where(inner, mid, over_z(mid, OUTWARD))
    third = jnp.where(inner, third_in, over_z(third_in, OUTWARD))
    return own, first, second, third


def scatter_col(parts):
    own, first, second, third = parts
    t3 = (third + over_z(third.astype(BF16), INWARD)).astype(BF16)
    t2 = (second + over_z(second.astype(BF16), INWARD)).astype(BF16)
    t1 = (first + over_z(t3, MIDDLE)).astype(BF16)
    v = over_z(t2, MIDDLE)
    w = over_z(t1, PAIR)
    return own + v.astype(F32) + w.astype(F32)


def norm_forward(values, gain_vec):
    mean_sq = jnp.mean(values * values, axis=1, keepdims=True)
    inv_rms = lax.rsqrt(mean_sq + NORM_EPS)
    unit_rows = values * inv_rms
    return (unit_rows, inv_rms, (unit_rows * gain_vec).astype(BF16))


def norm_backward(grad_norm, unit_rows, inv_rms, gain_vec):
    scaled = grad_norm * gain_vec
    inner_sum = jnp.mean(scaled * unit_rows, axis=1, keepdims=True)
    return (inv_rms * (scaled - unit_rows * inner_sum), jnp.sum(grad_norm * unit_rows, axis=0))


def shards(
    tokens, gain_attn, w_query, w_keyval, w_output, gain_mlp, w_gate, w_up, w_down, out_grad,
    document_numbers, positions, *, rows,
):
    width = tokens.shape[1]
    fast = rows == 4
    z = lax.axis_index("col")
    r = lax.axis_index("row")
    y = lax.axis_index("dp")
    inner = (z == 1) | (z == 2)
    x, c = r // 2, r % 2
    blk = width // 8

    def permuted(a, abs_order):
        if not fast:
            return a
        axis = a.ndim - 1
        pieces = []
        for hi in range(2):
            for mid in range(2):
                for lo in range(2):
                    if abs_order:
                        at = 4 * (c ^ mid) + 2 * (x ^ hi) + (y ^ lo)
                    else:
                        at = 4 * (x ^ mid) + 2 * (c ^ hi) + (y ^ lo)
                    pieces.append(lax.dynamic_slice_in_dim(a, at * blk, blk, axis))
        return jnp.concatenate(pieces, axis=axis)

    to_rel = functools.partial(permuted, abs_order=False)
    to_abs = functools.partial(permuted, abs_order=True)

    def gather_rows(block):
        return lax.all_gather(block, "row", axis=0, tiled=True)

    def gather_slots(block):
        full = gather_rows(block)
        return [full] + [from_slot(full, s) for s in (1, 2, 3)]

    tok = to_rel(tokens)
    x_in = tok.astype(F32)
    gain_one = to_rel(gain_attn)
    gain_two = to_rel(gain_mlp)
    unit_one, inv_one, normed_one = norm_forward(x_in, gain_one)
    count = tokens.shape[0]
    my_pos = lax.dynamic_slice_in_dim(positions, z * count, count, 0)
    frequency = ROPE_BASE ** (-(jnp.arange(32, dtype=F32) * 2.0 / HEAD_SIZE))
    angles = my_pos.astype(F32)[:, None] * frequency[None, :]
    co, si = jnp.cos(angles), jnp.sin(angles)
    cos_q = jnp.concatenate([co, co, co, co], axis=1)
    sin_q = jnp.concatenate([-si, si, -si, si], axis=1)
    cos_k = jnp.concatenate([co, co, jnp.ones_like(co), jnp.ones_like(co)], axis=1)
    sin_k = jnp.concatenate([-si, si, jnp.zeros_like(si), jnp.zeros_like(si)], axis=1)
    my_seg = lax.dynamic_slice_in_dim(document_numbers, z * count, count, 0)
    key_seg = jnp.concatenate(
        [lax.dynamic_slice_in_dim(document_numbers, ((z + t) % 4) * count, count, 0) for t in range(4)]
    )
    lane = jnp.arange(count, dtype=jnp.int32)
    key_at = jnp.concatenate([((z + t) % 4) * count + lane for t in range(4)])
    allowed = (key_seg[:, None] == my_seg[None, :]) & (key_at[:, None] <= (z * count + lane)[None, :])
    bias = jnp.where(allowed, 0.0, MASK_FILL).astype(F32)

    def separate():
        full = lax.all_gather(w_keyval, "row", axis=0, tiled=True)
        wkv = jnp.concatenate([full] + [from_slot(full, s) for s in (1, 2, 3)], axis=1)
        wq = gather_slots(w_query)
        wo = gather_slots(w_output.T)
        wg, wu, wd = gather_rows(w_gate), gather_rows(w_up), gather_rows(w_down.T)
        kv = call(
            kv_kernel, [((4, count, 128), BF16)], (normed_one, wkv, cos_k, sin_k), 2 * count * width * 512
        )[0]
        kv_from = [kv]
        for t in (1, 2, 3):
            kv_from.append(over_z(kv, [((i + t) % 4, i) for i in range(4) if i + t >= 4]))
        kv_of = [[kv_from[t][(s - t) % 4] for t in range(4)] for s in range(4)]
        fwd = []
        for s in range(4):
            fwd.append(
                call(
                    fwd_kernel,
                    [((count, 512), BF16), ((count, 512), BF16), ((512, count), F32), ((8, count), F32)],
                    (normed_one, wq[s], *kv_of[s], bias, cos_q, sin_q),
                    2 * count * width * 512 + 8 * 4 * count * 1024 * 256,
                )
            )
        attn = [f[1] for f in fwd]
        mid = x_in + (nt(attn[0], wo[0]) + nt(attn[1], wo[1]) + nt(attn[2], wo[2]) + nt(attn[3], wo[3]))
        unit_two, inv_two, n2 = norm_forward(mid, gain_two)
        dys = gather_col(dy, inner)
        n2s = gather_col(n2, inner)
        outs, gns, acts, ggs, gus = [], [], [], [], []
        for s in range(4):
            gate_pre = nn(n2s[s], wg)
            up_pre = nn(n2s[s], wu)
            grad_act = nn(dys[s], wd)
            sig = jax.nn.sigmoid(gate_pre)
            silu = gate_pre * sig
            act = (silu * up_pre).astype(BF16)
            gg = (grad_act * up_pre * sig * (1.0 + gate_pre * (1.0 - sig))).astype(BF16)
            gu = (grad_act * silu).astype(BF16)
            outs.append(nt(act, wd))
            gns.append(nt(gg, wg) + nt(gu, wu))
            acts.append(act)
            ggs.append(gg)
            gus.append(gu)
        grad_norm_two = scatter_col(gns)
        flat = [jnp.concatenate(v, axis=0) for v in (n2s, dys, acts, ggs, gus)]
        mid_norm, gain2 = norm_backward(grad_norm_two, unit_two, inv_two, gain_two)
        gmid = dy.astype(F32) + mid_norm
        return wq, wo, wkv, kv_of, fwd, attn, mid, outs, flat, gmid, gmid.astype(BF16), gain2

    def together():
        def cut(block):
            return block.reshape(2, block.shape[0] // 2, block.shape[1])

        WQ, WO, WKV, ACT, GG, GU, OUT, n1, q, kv, o, ot, lse, mid, N2, DY, gmid, branch, gain2 = start_call(
            (
                tok, gain_one[None, :], gain_two[None, :], cut(w_query), cut(w_output.T), cut(w_keyval), cut(w_gate),
                cut(w_up), cut(w_down.T), dy, bias, cos_q, sin_q, cos_k, sin_k,
            )
        )
        n2_all, dy_all, act_all, gg_all, gu_all = (m.reshape(4 * count, m.shape[-1]) for m in (N2, DY, ACT, GG, GU))

        def part(a, g):
            return tn(a, g).astype(BF16).reshape(2, 2, 2, blk, g.shape[-1])

        pd, pg, pu = part(dy_all, act_all), part(n2_all, gg_all), part(n2_all, gu_all)
        total_out = mid + OUT[0].astype(F32)
        near = z ^ 1
        second = jnp.where(z < 2, 2, 1)
        for s in (1, 2, 3):
            to = (z + s) % 4
            slot = jnp.where(to == near, 1, jnp.where(to == second, 2, 3))
            total_out = total_out + to_slot(lax.dynamic_index_in_dim(OUT, slot, 0, keepdims=False), s).astype(F32)
        gtok, gains, gd, gg, gu, gq, go, gkv = end_call(
            (
                pd, pg, pu, WQ, WO, WKV, ot, branch, gmid, tok, gain_one[None, :], gain2, n1, q, kv, o, lse, bias, cos_q,
                sin_q, cos_k, sin_k,
            )
        )[:8]

        def joined(g):
            return g.reshape(2 * blk, g.shape[-1])

        return (
            to_abs(total_out.astype(BF16)), to_abs(gtok), gains[0], joined(gq), joined(gkv), joined(go).T, gains[1],
            joined(gg), joined(gu), joined(gd).T,
        )

    dy = to_rel(out_grad)
    if fast:
        return together()
    wq, wo, wkv, kv_of, fwd, attn, resid_mid, outs, flat, grad_mid, branch, gain_two_term = separate()
    n2_all, dy_all, act_all, gg_all, gu_all = flat
    block_out = (resid_mid + scatter_col([o.astype(F32) for o in outs])).astype(BF16)

    def ordered(lo, hi):
        return jnp.where(y == 0, jnp.concatenate([lo, hi], axis=0), jnp.concatenate([hi, lo], axis=0))

    def weight_grad(act_rel, g):
        half = width // 2
        if not fast:
            full = lax.psum_scatter(tn(act_rel, g).astype(BF16), "row", scatter_dimension=0, tiled=True)
            return lax.psum(full, "dp").astype(F32)
        got = over_c(tn(act_rel[:, half:], g).astype(BF16))
        t = tn(act_rel[:, :half], g) + got.astype(F32)
        q = half // 2
        got = over_x(t[q:].astype(BF16))
        t = (t[:q] + got.astype(F32)).astype(BF16)
        got = over_y(t).astype(F32)
        t = t.astype(F32)
        return ordered(t[: q // 2] + got[q // 2 :], t[q // 2 :] + got[: q // 2])

    def weight_grad_slots(act_rel, gs):
        half = width // 2
        if not fast:
            tot = 0.0
            for s in range(4):
                full = lax.psum_scatter(
                    tn(act_rel, gs[s]).astype(BF16), "row", scatter_dimension=0, tiled=True
                )
                tot = tot + (full if s == 0 else to_slot(full, s)).astype(F32)
            return lax.psum(tot.astype(BF16), "dp").astype(F32)
        tot = 0.0
        for s in range(4):
            got = over_c(tn(act_rel[:, half:], gs[s]).astype(BF16))
            t = tn(act_rel[:, :half], gs[s]) + got.astype(F32)
            b = blk
            t00, t01, t10, t11 = t[:b], t[b : 2 * b], t[2 * b : 3 * b], t[3 * b :]
            if s % 2:
                got = over_y(jnp.concatenate([t01, t11], axis=0).astype(BF16)).astype(F32)
                u0 = t00 + got[:b]
                u1 = t10 + got[b:]
                u = u0 + over_x(u1.astype(BF16)).astype(F32)
            else:
                got = over_x(jnp.concatenate([t10, t11], axis=0).astype(BF16)).astype(F32)
                u0 = t00 + got[:b]
                u1 = t01 + got[b:]
                u = u0 + over_y(u1.astype(BF16)).astype(F32)
            u = u.astype(BF16)
            tot = tot + (u if s == 0 else to_slot(u, s)).astype(F32)
        tot = tot.astype(BF16)
        return ordered(tot.astype(F32), over_y(tot).astype(F32))

    g_down = weight_grad(dy_all, act_all)
    g_gate = weight_grad(n2_all, gg_all)
    g_up = weight_grad(n2_all, gu_all)

    bwd = []
    for s in range(4):
        bwd.append(
            call(
                bwd_kernel,
                [((count, 512), BF16), ((count, 128), F32), ((3, count, 128), BF16)],
                (branch, wo[s], fwd[s][0], *kv_of[s], bias, cos_q, sin_q, fwd[s][2], fwd[s][3]),
                2 * count * width * 512 + 8 * 10 * count * 1024 * 256,
                scratch=(
                    pltpu.VMEM((1024, 512), BF16),
                    pltpu.VMEM((1024, 512), BF16),
                    pltpu.VMEM((1024, 128), F32),
                    pltpu.VMEM((1024, 128), F32),
                ),
            )
        )
    got = []
    for t in (1, 2, 3):
        out = jnp.stack([bwd[s][2][t - 1] for s in range(4)])
        got.append(over_z(out, [(i, (i + t) % 4) for i in range(4) if i + t >= 4]))
    dkv = call(
        dkv_kernel,
        [((4, count, 128), BF16)],
        (*[bwd[s][1] for s in range(4)], *got, cos_k, sin_k),
        count * 512 * 8,
    )[0]
    dkv = jnp.concatenate([dkv[s] for s in range(4)], axis=1)
    dq = [bwd[s][0] for s in range(4)]
    grad_norm_one = nt(dq[0], wq[0]) + nt(dq[1], wq[1]) + nt(dq[2], wq[2]) + nt(dq[3], wq[3])
    grad_norm_one = grad_norm_one + nt(dkv, wkv)
    in_norm, gain_one_term = norm_backward(grad_norm_one, unit_one, inv_one, gain_one)
    grad_tokens = (grad_mid + in_norm).astype(BF16)
    g_output = weight_grad_slots(branch, attn)
    g_query = weight_grad_slots(normed_one, dq)
    g_keyval = weight_grad_slots(normed_one, [dkv[:, 128 * s : 128 * s + 128] for s in range(4)])

    def total(v):
        if not fast:
            return lax.psum(v, ("dp", "row", "col"))
        v = v + over_c(v)
        v = v + over_x(v)
        v = v + over_y(v)
        v = v + over_z(v, PAIR)
        return v + over_z(v, [(0, 2), (1, 3), (2, 0), (3, 1)])

    return (
        to_abs(block_out),
        to_abs(grad_tokens),
        total(to_abs(gain_one_term)),
        g_query,
        g_keyval,
        g_output.T,
        total(to_abs(gain_two_term)),
        g_gate,
        g_up,
        g_down.T,
    )


def solution(mesh):
    spec = P(("dp", "row", "col"), None)
    down = P("row", "col")
    across = P("col", "row")
    seq = P(("dp", "row"))
    return jax.shard_map(
        functools.partial(shards, rows=mesh.shape["row"]),
        mesh=mesh,
        in_specs=(spec, P(), down, down, across, P(), down, down, across, spec, seq, seq),
        out_specs=(spec, spec, P(), down, down, across, P(), down, down, across),
        check_vma=False,
    )
```

```python
import functools
import math

import jax
import jax.numpy as jnp
from jax import lax
from jax.experimental import pallas as pl
from jax.experimental.pallas import tpu as pltpu
from jax.sharding import PartitionSpec as P

HEAD_SIZE = 64
SEQUENCE_LENGTH = 1024
NORM_EPS = 1e-05
ROPE_BASE = 10000.0
MASK_FILL = -1e30
BF16 = jnp.bfloat16
F32 = jnp.float32


def nn(a, b):
    return lax.dot_general(a, b, (((1,), (0,)), ((), ())), preferred_element_type=F32)


def nt(a, b):
    return lax.dot_general(a, b, (((1,), (1,)), ((), ())), preferred_element_type=F32)


def tn(a, b):
    return lax.dot_general(a, b, (((0,), (0,)), ((), ())), preferred_element_type=F32)


def swap_halves(v):
    lane = lax.broadcasted_iota(jnp.int32, v.shape, 1)
    return jnp.where((lane % 64) < 32, pltpu.roll(v, 96, 1), pltpu.roll(v, 32, 1))


def kv_kernel(n_ref, w_ref, c_ref, s_ref, o_ref):
    kv = nn(n_ref[...], w_ref[...])
    for s in range(4):
        v = kv[:, 128 * s : 128 * s + 128]
        o_ref[s] = (v * c_ref[...] + swap_halves(v) * s_ref[...]).astype(BF16)


def load_kv(kv_refs):
    return jnp.concatenate([r[...].astype(F32) for r in kv_refs], axis=0)


def fwd_kernel(n_ref, w_ref, k0, k1, k2, k3, bias_ref, c_ref, s_ref, q_ref, o_ref, ot_ref, lse_ref):
    q = nn(n_ref[...], w_ref[...])
    kv = load_kv((k0, k1, k2, k3))
    k_low = kv[:, :64].astype(BF16)
    v_t = kv.T[64:].astype(BF16)
    for p in range(4):
        cols = slice(128 * p, 128 * p + 128)
        v = q[:, cols]
        rot = (v * c_ref[...] + swap_halves(v) * s_ref[...]) * 0.125
        rot = rot.astype(BF16)
        q_ref[:, cols] = rot
        q_t = rot.astype(F32).T.astype(BF16)
        outs = []
        for e in range(2):
            s_t = nn(k_low, q_t[64 * e : 64 * e + 64]) + bias_ref[...]
            top = jnp.max(s_t, axis=0, keepdims=True)
            ex = jnp.exp(s_t - top)
            tot = jnp.sum(ex, axis=0, keepdims=True)
            outs.append(nn(v_t, ex.astype(BF16)) * (1.0 / tot))
            lse_ref[pl.ds(2 * p + e, 1), :] = top + jnp.log(tot)
        o_t = jnp.concatenate(outs, axis=0)
        ot_ref[cols, :] = o_t
        o_ref[:, cols] = o_t.T.astype(BF16)


def bwd_kernel(
    b_ref, w_ref, q_ref, k0, k1, k2, k3, bias_ref, c_ref, s_ref, ot_ref, lse_ref,
    dq_ref, d0_ref, dr_ref, ds_scr, p_scr, dk_scr, dv_scr,
):
    ga = nn(b_ref[...], w_ref[...]).astype(BF16).astype(F32)
    kv = load_kv((k0, k1, k2, k3))
    k_low = kv[:, :64].astype(BF16)
    v_low = pltpu.roll(kv, 64, 1)[:, :64].astype(BF16)
    k_t = kv.T[:64].astype(BF16)
    lane = lax.broadcasted_iota(jnp.int32, (256, 128), 1)
    for p in range(4):
        cols = slice(128 * p, 128 * p + 128)
        qp = q_ref[:, cols].astype(F32)
        gp = ga[:, cols]
        q_t = qp.T.astype(BF16)
        g_tf = gp.T
        g_t = g_tf.astype(BF16)
        prod = g_tf * ot_ref[cols, :]
        dq_t = []
        for e in range(2):
            half = slice(64 * e, 64 * e + 64)
            s_t = nn(k_low, q_t[half]) + bias_ref[...]
            pr = jnp.exp(s_t - lse_ref[pl.ds(2 * p + e, 1), :])
            dp = nn(v_low, g_t[half])
            inner = jnp.sum(prod[half], axis=0, keepdims=True)
            ds = (pr * (dp - inner)).astype(BF16)
            ds_scr[:, 256 * e : 256 * e + 256] = ds
            p_scr[:, 256 * e : 256 * e + 256] = pr.astype(BF16)
            dq_t.append(nn(k_t, ds))
        qbd = jnp.concatenate(
            [jnp.where(lane < 64, qp, 0.0), jnp.where(lane < 64, 0.0, qp)], axis=0
        ).astype(BF16)
        gbd = jnp.concatenate(
            [jnp.where(lane < 64, gp, 0.0), jnp.where(lane < 64, 0.0, gp)], axis=0
        ).astype(BF16)
        dk = nn(ds_scr[...], qbd)
        dv = nn(p_scr[...], gbd)
        if p == 0:
            dk_scr[...] = dk
            dv_scr[...] = dv
        else:
            dk_scr[...] += dk
            dv_scr[...] += dv
        dqp = jnp.concatenate(dq_t, axis=0).T * 0.125
        dq_ref[:, cols] = (dqp * c_ref[...] - swap_halves(dqp) * s_ref[...]).astype(BF16)
    dk = dk_scr[...]
    dv = dv_scr[...]
    lane = lax.broadcasted_iota(jnp.int32, dk.shape, 1)
    both = jnp.where(lane < 64, dk + pltpu.roll(dk, 64, 1), dv + pltpu.roll(dv, 64, 1))
    d0_ref[...] = both[:256]
    for t in range(3):
        dr_ref[t] = both[256 * (t + 1) : 256 * (t + 2)].astype(BF16)


def dkv_kernel(a0, a1, a2, a3, r1, r2, r3, c_ref, s_ref, o_ref):
    own = (a0, a1, a2, a3)
    got = (r1, r2, r3)
    for s in range(4):
        v = own[s][...]
        for t in range(1, 4):
            v = v + got[t - 1][(s + t) % 4].astype(F32)
        o_ref[s] = (v * c_ref[...] - swap_halves(v) * s_ref[...]).astype(BF16)


def call(body, outs, args, flops, scratch=(), vmem=48 << 20):
    spec = pl.BlockSpec(memory_space=pltpu.VMEM)
    shapes = [jax.ShapeDtypeStruct(s, d) for s, d in outs]
    nbytes = sum(a.size * a.dtype.itemsize for a in args) + sum(
        math.prod(s) * jnp.dtype(d).itemsize for s, d in outs
    )
    return pl.pallas_call(
        body,
        out_shape=shapes,
        in_specs=[spec] * len(args),
        out_specs=[spec] * len(outs),
        scratch_shapes=list(scratch),
        compiler_params=pltpu.CompilerParams(vmem_limit_bytes=vmem),
        cost_estimate=pl.CostEstimate(flops=flops, bytes_accessed=nbytes, transcendentals=0),
    )(*args)


MESH = pl.DeviceIdType.MESH


def mark(name):
    return jax.named_scope(name)


def relative(x, c, y):
    at = []
    for k in range(2):
        for i in range(2):
            for j in range(2):
                at.append(pl.multiple_of(256 * (4 * (x ^ i) + 2 * (c ^ k) + (y ^ j)), 256))
    return at


class Wire:
    def __init__(self, send_sem, recv_sem, z):
        self.send_sem, self.recv_sem, self.z = send_sem, recv_sem, z
        self.count = 0
        self.made = []

    def to(self, where):
        r = lax.axis_index("row")
        if where == "x":
            return {"row": lax.rem(r + 2, 4)}
        if where == "c":
            return {"row": r + 1 - 2 * lax.rem(r, 2)}
        if where == "y":
            return {"dp": 1 - lax.axis_index("dp")}
        return {"col": where}

    def copy(self, src, dst, where, only=None, recv=None):
        k = self.count
        self.count += 1
        cp = pltpu.make_async_remote_copy(
            src_ref=src, dst_ref=dst, send_sem=self.send_sem.at[k], recv_sem=self.recv_sem.at[k if recv is None else recv],
            device_id=self.to(where), device_id_type=MESH,
        )
        self.made.append((cp, only))
        return cp

    def sent(self, cp):
        self.made = [m for m in self.made if m[0] is not cp]
        cp.wait_send()

    def send(self, src, dst, where):
        cp = self.copy(src, dst, where)
        cp.start()
        return cp

    def finish(self):
        for cp, only in self.made:
            if only is None:
                cp.wait_send()
            else:
                pl.when(only)(cp.wait_send)


def greet(z):
    barrier = pltpu.get_barrier_semaphore()
    wire = Wire(None, None, z)
    for where in ("x", "c", "y"):
        pl.semaphore_signal(barrier, inc=1, device_id=wire.to(where), device_id_type=MESH)
    for d in (1, 2, 3):
        pl.semaphore_signal(barrier, inc=1, device_id={"col": lax.rem(z + d, 4)}, device_id_type=MESH)
    pl.semaphore_wait(barrier, 6)


def attend_slot(w_ref, n_ref, kv_scr, s, bias_ref, c_ref, s_ref, q_ref, o_ref, ot_ref, lse_ref, q_scr):
    q_scr[...] = nn(n_ref[...], w_ref[...])
    kv = jnp.concatenate([kv_scr[t, (s - t) % 4].astype(F32) for t in range(4)], axis=0)
    k_low = kv[:, :64].astype(BF16)
    v_t = kv.T[64:].astype(BF16)

    def pair(p, carry):
        at = pl.multiple_of(p * 128, 128)
        cols = pl.ds(at, 128)
        v = q_scr[:, cols]
        rot = ((v * c_ref[...] + swap_halves(v) * s_ref[...]) * 0.125).astype(BF16)
        q_ref[:, cols] = rot
        q_t = rot.astype(F32).T.astype(BF16)
        outs = []
        for e in range(2):
            s_t = nn(k_low, q_t[64 * e : 64 * e + 64]) + bias_ref[...]
            top = jnp.max(s_t, axis=0, keepdims=True)
            ex = jnp.exp(s_t - top)
            tot = jnp.sum(ex, axis=0, keepdims=True)
            outs.append(nn(v_t, ex.astype(BF16)) * (1.0 / tot))
            lse_ref[s, pl.ds(2 * p + e, 1), :] = top + jnp.log(tot)
        o_t = jnp.concatenate(outs, axis=0)
        ot_ref[cols, :] = o_t
        o_ref[s, :, cols] = o_t.T.astype(BF16)
        return carry

    lax.fori_loop(0, 4, pair, 0)


def start_kernel(
    gain_ref, wq_ref, wo_ref, wkv_ref, bias_ref, cq_ref, sq_ref, ck_ref, sk_ref, tok_ref, wg_ref, wu_ref, wd_ref, dy_ref,
    WQ, WO, WKV, OUT, NONE, QS, OT, BRANCH, LCM, LXM, LYM, TGU, GDOWN, kv_out, o_ref, lse_ref, mid_ref, gmid_ref, gain2_out,
    wm, gn_scr, N2, DY, wbuf, wkv_scr, q_scr, q_stage, ot_stage, gate_scr, up_scr, grad_scr, hid, out_stage, pre,
    gains, send_sem, recv_sem, loc_sem,
):
    own_scr = gmid_ref
    kv_scr = kv_out
    r = lax.axis_index("row")
    x, c = r // 2, lax.rem(r, 2)
    z = lax.axis_index("col")
    y = lax.axis_index("dp")
    inner = (z == 1) | (z == 2)
    outer = jnp.logical_not(inner)
    w = Wire(send_sem, recv_sem, z)
    locs = []

    def local(src, dst):
        cp = pltpu.make_async_copy(src, dst, loc_sem.at[len(locs)])
        cp.start()
        locs.append(cp)
        return cp

    greet(z)
    blocks = {"kv": (wkv_ref, WKV), "q": (wq_ref, WQ), "o": (wo_ref, WO)}
    ev = {}

    def start_z(name):
        ref, full = blocks[name]
        for s in (1, 2, 3):
            d = 4 - s
            ev[name, s, "z"] = w.send(ref.at[y], full.at[s, 0, 0, 0], lax.rem(z + d, 4))

    def start_own(name):
        ref, full = blocks[name]
        ev[name, 0, "x"] = w.send(ref.at[y], full.at[0, 0, 1, 0], "x")
        ev[name, 0, "own"] = [local(ref.at[y], full.at[0, 0, 0, 0]), local(ref.at[1 - y], full.at[0, 0, 0, 1])]
        ev[name, 0, "c0"] = [
            w.send(ref.at[y], full.at[0, 1, 0, 0], "c"), w.send(ref.at[1 - y], full.at[0, 1, 0, 1], "c")
        ]

    def own_second(name):
        full = blocks[name][1]
        ev[name, 0, "x"].wait_recv()
        ev[name, 0, "y"] = w.send(full.at[0, 0, 1, 0], full.at[0, 0, 1, 1], "y")

    def own_core(name):
        full = blocks[name][1]
        ev[name, 0, "y"].wait_recv()
        ev[name, 0, "c"] = w.send(full.at[0, 0, 1], full.at[0, 1, 1], "c")

    def first(name, s):
        full = blocks[name][1]
        ev[name, s, "z"].wait_recv()
        if (s % 2 == 1) != (name == "o"):
            ev[name, s, 1] = w.send(full.at[s, 0, 0, 0], full.at[s, 0, 0, 1], "y")
        else:
            ev[name, s, 1] = w.send(full.at[s, 0, 0, 0], full.at[s, 0, 1, 0], "x")

    def second(name, s):
        full = blocks[name][1]
        ev[name, s, 1].wait_recv()
        if (s % 2 == 1) != (name == "o"):
            ev[name, s, 2] = w.send(full.at[s, 0, 0], full.at[s, 0, 1], "x")
        else:
            ev[name, s, 2] = w.send(full.at[s, 0, :, 0], full.at[s, 0, :, 1], "y")

    def core(name, s):
        full = blocks[name][1]
        ev[name, s, 2].wait_recv()
        ev[name, s, "c"] = w.send(full.at[s, 0], full.at[s, 1], "c")

    def whole(name, s):
        ev[name, s, "c"].wait_recv()
        if s == 0:
            for cp in ev[name, 0, "c0"]:
                cp.wait_recv()
            for cp in ev[name, 0, "own"]:
                cp.wait()

    mats = {"g": (wg_ref, wm.at[0]), "u": (wu_ref, wm.at[1]), "d": (wd_ref, wm.at[2])}

    def mat_start(name):
        ref, full = mats[name]
        ev[name, "x"] = w.send(ref.at[y], full.at[0, 1, 0], "x")
        ev[name, "own"] = [local(ref.at[y], full.at[0, 0, 0]), local(ref.at[1 - y], full.at[0, 0, 1])]
        ev[name, "c0"] = [
            w.send(ref.at[y], full.at[1, 0, 0], "c"), w.send(ref.at[1 - y], full.at[1, 0, 1], "c")
        ]

    def mat_second(name):
        full = mats[name][1]
        ev[name, "x"].wait_recv()
        ev[name, "y"] = w.send(full.at[0, 1, 0], full.at[0, 1, 1], "y")

    def mat_core(name):
        full = mats[name][1]
        ev[name, "y"].wait_recv()
        ev[name, "c"] = w.send(full.at[0, 1], full.at[1, 1], "c")

    def mat_whole(name):
        ev[name, "c"].wait_recv()
        for cp in ev[name, "c0"]:
            cp.wait_recv()
        for cp in ev[name, "own"]:
            cp.wait()

    buddy = z + 1 - 2 * lax.rem(z, 2)
    middle = lax.rem(7 - z, 4)

    def some(cond, cp):
        pl.when(cond)(cp.start)
        return cp

    def rows_start(full):
        f = w.send(full.at[0], full.at[1], buddy)
        m = some(inner, w.copy(full.at[0], full.at[2], middle, only=inner))
        return [f, m]

    def rows_first(full, c):
        c[0].wait_recv()
        c.append(some(inner, w.copy(full.at[1], full.at[3], middle, only=inner)))

    def rows_second(full, c):
        pl.when(inner)(c[1].wait_recv)
        c.append(some(inner, w.copy(full.at[2], full.at[2], buddy, only=inner)))

    def rows_third(full, c):
        pl.when(inner)(c[2].wait_recv)
        c.append(some(inner, w.copy(full.at[3], full.at[3], buddy, only=inner)))

    def rows_have_second(c):
        pl.when(outer)(c[3].wait_recv)

    def rows_have_third(c):
        pl.when(outer)(c[4].wait_recv)

    tok_rel, n1_rel = gn_scr.at[0], gn_scr.at[1]
    moved = []
    for m, at in enumerate(relative(x, c, y)):
        to = pl.ds(256 * m, 256)
        moved.append(local(tok_ref.at[:, pl.ds(at, 256)], tok_rel.at[:, to]))
        moved.append(local(dy_ref.at[:, pl.ds(at, 256)], DY.at[0, :, to]))
        gains[:, to] = gain_ref[:, pl.ds(at, 256)]
    start_z("kv")
    start_own("kv")
    start_z("q")
    start_own("q")

    def norm_one(i, carry):
        at = pl.ds(pl.multiple_of(i * 32, 32), 32)
        x_in = tok_rel[at, :].astype(F32)
        inv = lax.rsqrt(jnp.mean(x_in * x_in, axis=1, keepdims=True) + NORM_EPS)
        n1_rel[at, :] = (x_in * inv * gains[0:1, :]).astype(BF16)
        mid_ref[at, :] = x_in
        return carry

    for cp in moved:
        cp.wait()
    with mark("A_norm1"):
        lax.fori_loop(0, 8, norm_one, 0)
    n1_out = local(n1_rel, NONE)
    for t in (1, 2, 3):

        @pl.when(z + t < 4)
        def _():
            kv_scr[t] = jnp.zeros_like(kv_scr[t])

    with mark("A_kv1"):
        own_second("kv")
        for s in (1, 2, 3):
            first("kv", s)
        own_second("q")
    with mark("A_kv2"):
        for s in (2, 1, 3):
            second("kv", s)
        own_core("kv")
    with mark("A_q1"):
        for s in (1, 2, 3):
            first("q", s)
    with mark("A_kv3"):
        for s in (2, 1, 3):
            core("kv", s)
    own_core("q")
    with mark("A_q2"):
        for s in (2, 1, 3):
            second("q", s)
    start_own("o")
    mat_start("g")
    got = []
    with mark("A_kvw"):
        for s in range(4):
            whole("kv", s)
            if s < 2:
                got.append(local(WKV.at[s], wkv_scr.at[s]))
        for s in range(4):
            got[s].wait()
            kv = nn(n1_rel[...], wkv_scr[s % 2].reshape(2048, 128))
            if s < 2:
                got.append(local(WKV.at[s + 2], wkv_scr.at[s]))
            kv_scr[0, s] = (kv * ck_ref[...] + swap_halves(kv) * sk_ref[...]).astype(BF16)
    kv_cp = {}
    for s in (0, 2, 1, 3):
        for d in (1, 2, 3):
            u = (s + d) % 4
            cp = w.copy(kv_scr.at[0, u], kv_scr.at[4 - d, u], lax.rem(z + d, 4), only=z + d < 4)
            kv_cp[4 - d, s] = cp
            pl.when(z + d < 4)(cp.start)
    cps, kept = {}, []
    with mark("A_q0w"):
        whole("q", 0)
    cps[0] = local(WQ.at[0], wbuf.at[0])
    start_z("o")
    dyc = rows_start(DY)
    def attend(s, b):
        cps[s].wait()
        for cp in kept:
            cp.wait()
        kept.clear()
        with mark("A_kvr"):
            for t in (1, 2, 3):
                pl.when(z + t >= 4)(kv_cp[t, s].wait_recv)
        with mark(f"A_att{s}"):
            attend_slot(
                wbuf.at[b].reshape(2048, 512), n1_rel, kv_scr, s, bias_ref, cq_ref, sq_ref, q_stage, o_ref, ot_stage,
                lse_ref, q_scr,
            )
        kept.append(local(q_stage, QS.at[s]))
        kept.append(local(ot_stage, OT.at[s]))

    attend(0, 0)
    with mark("A_q3"):
        core("q", 2)
        whole("q", 2)
    cps[2] = local(WQ.at[2], wbuf.at[1])
    attend(2, 1)
    with mark("A_o1"):
        own_second("o")
        for s in (1, 2, 3):
            first("o", s)
    mat_start("u")
    with mark("A_q4"):
        core("q", 1)
        core("q", 3)
        whole("q", 1)
    cps[1] = local(WQ.at[1], wbuf.at[0])
    whole("q", 3)
    cps[3] = local(WQ.at[3], wbuf.at[1])
    with mark("A_m1"):
        mat_second("g")
    with mark("A_dy1"):
        rows_first(DY, dyc)
    attend(1, 0)
    with mark("A_o2"):
        own_core("o")
        for s in (2, 1, 3):
            second("o", s)
    mat_start("d")
    with mark("A_dy2"):
        rows_second(DY, dyc)
    oc = {}
    attend(3, 1)
    with mark("A_m2"):
        mat_second("u")
    with mark("A_dy3"):
        rows_third(DY, dyc)
    with mark("A_o3"):
        for s in (2, 1, 3):
            core("o", s)
    for k, s in enumerate((0, 2, 1, 3)):
        with mark("A_oproj"):
            if s == 0:
                whole("o", 0)
                oc[0] = local(WO.at[0], wbuf.at[0])
            oc[s].wait()
            if k < 3:
                nxt = (2, 1, 3)[k]
                whole("o", nxt)
                oc[nxt] = local(WO.at[nxt], wbuf.at[(k + 1) % 2])

            def columns(i, carry):
                at = pl.ds(pl.multiple_of(i * 512, 512), 512)
                mid_ref[:, at] += nt(o_ref[s], wbuf[k % 2, i // 2, i % 2].reshape(512, 512))
                return carry

            lax.fori_loop(0, 4, columns, 0)

    def norm_two(i, carry):
        at = pl.ds(pl.multiple_of(i * 32, 32), 32)
        mid = mid_ref[at, :]
        inv = lax.rsqrt(jnp.mean(mid * mid, axis=1, keepdims=True) + NORM_EPS)
        N2[0, at, :] = (mid * inv * gains[1:2, :]).astype(BF16)
        return carry

    lax.fori_loop(0, 8, norm_two, 0)
    n2c = rows_start(N2)
    with mark("A_m2"):
        mat_core("g")
    with mark("A_m3"):
        mat_second("d")
        mat_core("u")
    with mark("A_n1"):
        rows_first(N2, n2c)
        rows_second(N2, n2c)
    with mark("A_m4"):
        mat_core("d")
        for name in mats:
            mat_whole(name)
    n1_out.wait()
    for cp in kept:
        cp.wait()
    def slot(a, stored):
        dy_a = DY[a]
        n2_a = N2[a]
        gate_scr[...] = nn(n2_a, wm[0].reshape(2048, 1408))
        up_scr[...] = nn(n2_a, wm[1].reshape(2048, 1408))
        grad_scr[...] = nn(dy_a, wm[2].reshape(2048, 1408))
        for cp in stored:
            cp.wait()

        def rows(i, carry):
            at = pl.ds(pl.multiple_of(i * 32, 32), 32)
            gate = gate_scr[at, :]
            up = up_scr[at, :]
            ga = grad_scr[at, :]
            sig = 1.0 / (1.0 + jnp.exp(-gate))
            silu = gate * sig
            hid[2, a, at, :] = (silu * up).astype(BF16)
            hid[0, a, at, :] = (ga * up * sig * (1.0 + gate * (1.0 - sig))).astype(BF16)
            hid[1, a, at, :] = (ga * silu).astype(BF16)
            return carry

        lax.fori_loop(0, 8, rows, 0)

        def columns(c, carry):
            at = pl.ds(pl.multiple_of(c * 512, 512), 512)
            k, i = c // 2, c % 2
            out_stage[:, at] = nt(hid[2, a], wm[2, k, i].reshape(512, 1408)).astype(BF16)
            gn = nt(hid[0, a], wm[0, k, i].reshape(512, 1408)) + nt(hid[1, a], wm[1, k, i].reshape(512, 1408))
            if a == 0:
                own_scr[:, at] = gn
            else:
                gn_scr[a - 1, :, at] = gn.astype(BF16)
            return carry

        lax.fori_loop(0, 4, columns, 0)
        return [local(out_stage, OUT.at[a])]

    def send_sum(a, n, where):
        for i in range(2):
            for j in range(2):
                piece = gn_scr.at[a - 1, :, pl.ds(1024 * i + 512 * j, 512)]
                w.copy(piece, wbuf.at[n // 2, n % 2, i, j], where, recv=112 + 4 * n + 2 * i + j).start()

    def sum_arrived(n):
        for i in range(2):
            for j in range(2):
                pltpu.make_async_remote_copy(
                    src_ref=gn_scr.at[0, :, pl.ds(0, 512)], dst_ref=wbuf.at[n // 2, n % 2, i, j],
                    send_sem=send_sem.at[0], recv_sem=recv_sem.at[112 + 4 * n + 2 * i + j],
                    device_id=w.to("c"), device_id_type=MESH,
                ).wait_recv()

    place = 1 + jnp.where(inner, 0, 1)
    second_at = jnp.where(z < 2, 2, 1)
    third_at = jnp.where(z < 2, 3, 0)
    with mark("A_slot0"):
        stored = slot(0, [])
    with mark("A_w1"):
        rows_have_second(dyc)
        rows_have_third(dyc)
        rows_third(N2, n2c)
    with mark("A_slot1"):
        stored = slot(1, stored)
    send_sum(1, 0, buddy)
    with mark("A_w2"):
        rows_have_second(n2c)
    with mark("A_slot2"):
        stored = slot(2, stored)
    send_sum(2, place, second_at)
    with mark("A_w3"):
        rows_have_third(n2c)
    with mark("A_slot3"):
        stored = slot(3, stored)
    send_sum(3, place, third_at)

    def add_rows(into, n):
        def body(i, carry):
            at = pl.ds(pl.multiple_of(i * 32, 32), 32)
            for h in range(2):
                for j in range(2):
                    cols = slice(1024 * h + 512 * j, 1024 * h + 512 * j + 512)
                    other = wbuf[n // 2, n % 2, h, j, at, :].astype(F32)
                    into[at, cols] = (into[at, cols].astype(F32) + other).astype(into.dtype)
            return carry

        lax.fori_loop(0, 8, body, 0)

    wide = {2: DY, 0: N2, 1: N2}
    mc, xs, ys = {}, {}, {}

    def wide_part(m, k):
        def tile(n, carry):
            cols = pl.ds(pl.multiple_of(1024 * k + 256 * n, 256), 256)
            src = jnp.concatenate([wide[m][a, :, cols] for a in range(4)], axis=0)
            wm[m, k, n // 2, n % 2] = tn(src, hid[m].reshape(1024, 1408)).astype(BF16)
            return carry

        with mark("A_dw"):
            lax.fori_loop(0, 4, tile, 0)
        if k:
            mc[m] = w.send(wm.at[m, 1], LCM.at[m], "c")

    turn = [0]

    def fetch(src):
        b = turn[0] % 2
        turn[0] += 1
        return pre.at[b], local(src, pre.at[b])

    def wide_core(m):
        with mark("A_wc"):
            mc[m].wait_recv()
            order = [(1, 0), (1, 1), (0, 0), (0, 1)]
            nxt = fetch(LCM.at[m, 1, 0])
            for n, (i, j) in enumerate(order):
                buf, cp = nxt
                if n < 3:
                    nxt = fetch(LCM.at[m, order[n + 1][0], order[n + 1][1]])
                cp.wait()
                add_into(wm.at[m, 0, i, j], wm.at[m, 0, i, j], buf)

    def wide_x(m, j):
        xs[m, j] = w.send(wm.at[m, 0, 1, j], LXM.at[m, j], "x")

    def wide_y(m, j):
        with mark("A_wy"):
            xs[m, j].wait_recv()
            buf, cp = fetch(LXM.at[m, j])
            cp.wait()
            add_into(wm.at[m, 0, 0, j], wm.at[m, 0, 0, j], buf)
            ys[m, j] = w.send(wm.at[m, 0, 0, j], LYM.at[m, 1 - j], "y")

    def wide_end(m, j):
        with mark("A_we"):
            ys[m, 1 - j].wait_recv()
            buf, cp = fetch(LYM.at[m, j])
            cp.wait()
            fin = (gate_scr, up_scr)[j]
            add_into(fin, wm.at[m, 0, 0, j], buf)
            return local(fin, GDOWN.at[lax.rem(y + j, 2)])

    for cp in stored:
        cp.wait()
    for name in mats:
        w.sent(ev[name, "y"])
        w.sent(ev[name, "c"])
    wide_part(2, 1)
    wide_part(2, 0)
    wide_core(2)
    wide_x(2, 0)
    wide_x(2, 1)
    wide_part(0, 1)
    wide_part(0, 0)
    wide_core(0)
    wide_x(0, 0)
    wide_y(2, 0)
    wide_part(1, 1)
    wide_part(1, 0)
    wide_y(2, 1)
    wide_core(1)
    saved = [local(wm.at[0, 0, 0], TGU.at[0, 0]), local(wm.at[0, 0, 1, 1], TGU.at[0, 1, 1])]
    saved.append(local(wm.at[1, 0], TGU.at[1]))
    with mark("A_r0"):
        sum_arrived(0)
    add_rows(own_scr, 0)
    with mark("A_r1"):
        sum_arrived(1)
        sum_arrived(2)
    add_rows(own_scr, 1)
    add_rows(own_scr, 2)
    gain2_out[...] = jnp.zeros_like(gain2_out)

    def norm_back(i, carry):
        at = pl.ds(pl.multiple_of(i * 32, 32), 32)
        gn = own_scr[at, :]
        mid = mid_ref[at, :]
        inv = lax.rsqrt(jnp.mean(mid * mid, axis=1, keepdims=True) + NORM_EPS)
        unit = mid * inv
        gain2_out[...] += jnp.sum(gn * unit, axis=0, keepdims=True)
        scaled = gn * gains[1:2, :]
        inside = jnp.mean(scaled * unit, axis=1, keepdims=True)
        gmid = DY[0, at, :].astype(F32) + inv * (scaled - unit * inside)
        gmid_ref[at, :] = gmid
        out_stage[at, :] = gmid.astype(BF16)
        return carry

    lax.fori_loop(0, 8, norm_back, 0)
    last = [local(out_stage, BRANCH)]
    last.append(wide_end(2, 0))
    last.append(wide_end(2, 1))
    with mark("A_end"):
        xs[0, 0].wait_recv()
    for cp in last + saved:
        cp.wait()
    w.finish()


def start_call(args):
    vmem = pl.BlockSpec(memory_space=pltpu.VMEM)
    hbm = pl.BlockSpec(memory_space=pl.ANY)
    outs = [
        ((4, 2, 2, 2, 256, 512), BF16, hbm), ((4, 2, 2, 2, 256, 512), BF16, hbm),
        ((4, 2, 2, 2, 256, 128), BF16, hbm), ((4, 256, 2048), BF16, hbm),
        ((256, 2048), BF16, hbm), ((4, 256, 512), BF16, hbm), ((4, 512, 256), F32, hbm), ((256, 2048), BF16, hbm),
        ((3, 2, 2, 256, 1408), BF16, hbm), ((3, 2, 256, 1408), BF16, hbm), ((3, 2, 256, 1408), BF16, hbm),
        ((2, 2, 2, 256, 1408), BF16, hbm), ((2, 256, 1408), F32, hbm),
        ((4, 4, 256, 128), BF16, vmem), ((4, 256, 512), BF16, vmem), ((4, 8, 256), F32, vmem),
        ((256, 2048), F32, vmem), ((256, 2048), F32, vmem), ((1, 2048), F32, vmem),
    ]
    scratch = [
        ((3, 2, 2, 2, 256, 1408), BF16), ((3, 256, 2048), BF16), ((4, 256, 2048), BF16), ((4, 256, 2048), BF16),
        ((2, 2, 2, 2, 256, 512), BF16), ((2, 2, 2, 2, 256, 128), BF16), ((256, 512), F32),
        ((256, 512), BF16), ((512, 256), F32), ((256, 1408), F32), ((256, 1408), F32), ((256, 1408), F32),
        ((3, 4, 256, 1408), BF16), ((256, 2048), BF16), ((2, 256, 1408), BF16), ((2, 2048), F32),
    ]
    return pl.pallas_call(
        start_kernel,
        out_shape=[jax.ShapeDtypeStruct(a, b) for a, b, _ in outs],
        in_specs=[vmem] * 9 + [hbm] * (len(args) - 9),
        out_specs=[o[2] for o in outs],
        scratch_shapes=[pltpu.VMEM(a, b) for a, b in scratch]
        + [pltpu.SemaphoreType.DMA((128,)), pltpu.SemaphoreType.DMA((128,)), pltpu.SemaphoreType.DMA((128,))],
        compiler_params=pltpu.CompilerParams(
            collective_id=0, has_side_effects=True, vmem_limit_bytes=67043328
        ),
        cost_estimate=pl.CostEstimate(flops=10**10, bytes_accessed=10**8, transcendentals=0),
    )(*args)


def attend_back(s, kv_of, ga_scr, q_ref, bias_ref, c_ref, s_ref, ot_ref, lse_ref, dq_scr, d0, dr, ds_scr, p_scr, dk_scr, dv_scr):
    kv = jnp.concatenate([kv_of[t, (s - t) % 4].astype(F32) for t in range(4)], axis=0)
    k_low = kv[:, :64].astype(BF16)
    v_low = pltpu.roll(kv, 64, 1)[:, :64].astype(BF16)
    k_t = kv.T[:64].astype(BF16)
    dk_scr[...] = jnp.zeros_like(dk_scr)
    dv_scr[...] = jnp.zeros_like(dv_scr)

    def pair(p, carry):
        cols = pl.ds(pl.multiple_of(p * 128, 128), 128)
        lane = lax.broadcasted_iota(jnp.int32, (256, 128), 1)
        qp = q_ref[s, :, cols].astype(F32)
        gp = ga_scr[:, cols]
        q_t = qp.T.astype(BF16)
        g_tf = gp.T
        g_t = g_tf.astype(BF16)
        prod = g_tf * ot_ref[cols, :]
        dq_t = []
        for e in range(2):
            half = slice(64 * e, 64 * e + 64)
            s_t = nn(k_low, q_t[half]) + bias_ref[...]
            pr = jnp.exp(s_t - lse_ref[s, pl.ds(2 * p + e, 1), :])
            dp = nn(v_low, g_t[half])
            inner = jnp.sum(prod[half], axis=0, keepdims=True)
            ds = (pr * (dp - inner)).astype(BF16)
            ds_scr[:, 256 * e : 256 * e + 256] = ds
            p_scr[:, 256 * e : 256 * e + 256] = pr.astype(BF16)
            dq_t.append(nn(k_t, ds))
        qbd = jnp.concatenate(
            [jnp.where(lane < 64, qp, 0.0), jnp.where(lane < 64, 0.0, qp)], axis=0
        ).astype(BF16)
        gbd = jnp.concatenate(
            [jnp.where(lane < 64, gp, 0.0), jnp.where(lane < 64, 0.0, gp)], axis=0
        ).astype(BF16)
        dk_scr[...] += nn(ds_scr[...], qbd)
        dv_scr[...] += nn(p_scr[...], gbd)
        dqp = jnp.concatenate(dq_t, axis=0).T * 0.125
        dq_scr[s, :, cols] = (dqp * c_ref[...] - swap_halves(dqp) * s_ref[...]).astype(BF16)
        return carry

    lax.fori_loop(0, 4, pair, 0)
    dk = dk_scr[...]
    dv = dv_scr[...]
    lane = lax.broadcasted_iota(jnp.int32, dk.shape, 1)
    both = jnp.where(lane < 64, dk + pltpu.roll(dk, 64, 1), dv + pltpu.roll(dv, 64, 1))
    d0[s] = both[:256]
    for t in range(3):
        dr[t, s] = both[256 * (t + 1) : 256 * (t + 2)].astype(BF16)


def add_into(into, one, other, step=32):
    def body(i, carry):
        at = pl.ds(pl.multiple_of(i * step, step), step)
        into[at, :] = (one[at, :].astype(F32) + other[at, :].astype(F32)).astype(into.dtype)
        return carry

    lax.fori_loop(0, into.shape[0] // step, body, 0)


def end_kernel(
    WQ, WO, WKV, OT, TGU, LXM, OUT, MID, TOK, BRANCH, GMID, NONE, QS, KVS, OS, BIAS, gain1_ref, gain2t_ref,
    lse_ref, cq_ref, sq_ref, ck_ref, sk_ref,
    gtok_ref, gains_ref, GGT, GUP, GQ, GO, GKV, bout_ref, LCO, LCQ, LCK, LYM, LX, LOUT,
    TM, TO, TQ, TK, S, L1O, L1Q, L1K, L2O, L2Q, L2K, LZO, LZQ, LZK, FO, FQ, FK, YO, YQ, YK,
    wbuf, wk, act_t, ga_scr, dq_scr, dkv_scr, d0, dr, ld, ds_scr, p_scr, dk_scr, dv_scr, gn_scr, pre, ot_scr, fin, gsum, gland, obuf, branch_ref, gmid_ref, n1_ref, q_ref, kv_ref, o_ref, bias_ref,
    send_sem, recv_sem, loc_sem,
):
    z = lax.axis_index("col")
    y = lax.axis_index("dp")
    r = lax.axis_index("row")
    x, c = r // 2, lax.rem(r, 2)
    w = Wire(send_sem, recv_sem, z)
    locs = []

    def local(src, dst):
        cp = pltpu.make_async_copy(src, dst, loc_sem.at[len(locs)])
        cp.start()
        locs.append(cp)
        return cp

    brought = {
        "o": local(OS, o_ref), "b": local(BRANCH, branch_ref), "q": local(QS, q_ref), "kv": local(KVS, kv_ref),
        "bias": local(BIAS, bias_ref), "n": local(NONE, n1_ref), "g": local(GMID, gmid_ref),
    }
    greet(z)
    finals = (GGT, GUP)
    places = relative(x, c, y)
    tok_cp = [local(TOK.at[:, pl.ds(at, 256)], obuf.at[:, pl.ds(256 * m, 256)]) for m, at in enumerate(places)]
    kept = [local(TGU.at[0, 0], TM.at[0, 0]), local(TGU.at[1], TM.at[1])]
    xs, ys = {}, {}
    xs[0, 1] = w.send(TGU.at[0, 1, 1], LX.at[0, 1], "x")
    buddy = z + 1 - 2 * lax.rem(z, 2)
    out_cp = []
    for s in (1, 2, 3):
        to = lax.rem(z + s, 4)
        second = jnp.where(z < 2, 2, 1)
        slot = jnp.where(to == buddy, 1, jnp.where(to == second, 2, 3))
        out_cp.append((w.copy(OUT.at[slot], LOUT.at[s - 1], to), slot == 3))
        pl.when(slot != 3)(out_cp[-1][0].start)
    wo_cp = {0: local(WO.at[0], wbuf.at[0])}
    wq_cp = {0: local(WQ.at[0], wbuf.at[1])}
    ot_cp = {0: local(OT.at[0], ot_scr)}

    def turned(src):
        for j in range(8):
            act_t[256 * j : 256 * j + 256, :] = src[:, 256 * j : 256 * j + 256].astype(F32).T.astype(BF16)

    def grad_part(g, keep, give, cols):
        for i in range(2):
            for j in range(2):
                at = 512 * i + 256 * j
                give[i, j, :, cols] = nn(act_t[1024 + at : 1024 + at + 256, :], g).astype(BF16)
        for i in range(2):
            for j in range(2):
                at = 512 * i + 256 * j
                keep[i, j, :, cols] = nn(act_t[at : at + 256, :], g).astype(BF16)

    every = slice(0, 512)
    brought["b"].wait()
    brought["o"].wait()
    with mark("B_turn"):
        turned(branch_ref)
    oc = []
    for s in range(4):
        if s > 1:
            w.sent(oc[s - 2])
        with mark("B_go"):
            grad_part(o_ref[s], TO.at[s], S.at[s % 2], every)
        oc.append(w.send(S.at[s % 2], LCO.at[s], "c"))

    slots = [0]

    def wide_x(m, j):
        xs[m, j] = w.send(TM.at[m, 1, j], LX.at[m, j], "x")

    def wide_y(m, j):
        if (m, j) != (0, 0):
            xs[m, j].wait_recv()
        b = slots[0] % 2
        slots[0] += 1
        local((LXM if (m, j) == (0, 0) else LX).at[m, j], pre.at[b, 0]).wait()
        add_into(TM.at[m, 0, j], TM.at[m, 0, j], pre.at[b, 0])
        ys[m, j] = w.send(TM.at[m, 0, j], LYM.at[m, 1 - j], "y")

    outs = []

    def wide_end(m, j):
        ys[m, 1 - j].wait_recv()
        b = slots[0] % 2
        slots[0] += 1
        local(LYM.at[m, j], pre.at[b, 0]).wait()
        if len(outs) >= 1:
            outs[-1].wait()
        add_into(fin, TM.at[m, 0, j], pre.at[b, 0])
        outs.append(local(fin, finals[m].at[lax.rem(y + j, 2)]))

    class Narrow:
        def __init__(self, T, LC, L1, L2, LZ, F, Y, out, width):
            self.T, self.LC, self.L1, self.L2, self.LZ, self.F, self.Y, self.out = T, LC, L1, L2, LZ, F, Y, out
            self.cps = {}
            self.width = width

        def core(self, s, cp):
            cp.wait_recv()
            tiles = [(i, j, pre.at[i, j, :, pl.ds(0, 512)]) for i in range(2) for j in range(2)]
            loads = [local(self.LC.at[s, i, j], t) for i, j, t in tiles]
            for (i, j, t), cp in zip(tiles, loads):
                cp.wait()
                add_into(self.T.at[s, i, j], self.T.at[s, i, j], t)

        def first(self, s):
            if s % 2:
                self.cps[s, 1] = w.send(self.T.at[s, :, 1], self.L1.at[s], "y")
            else:
                self.cps[s, 1] = w.send(self.T.at[s, 1], self.L1.at[s], "x")

        def second(self, s):
            self.cps[s, 1].wait_recv()
            for b in range(2):
                mine = self.T.at[s, b, 0] if s % 2 else self.T.at[s, 0, b]
                add_into(mine, mine, self.L1.at[s, b])
            if s % 2:
                self.cps[s, 2] = w.send(self.T.at[s, 1, 0], self.L2.at[s], "x")
            else:
                self.cps[s, 2] = w.send(self.T.at[s, 0, 1], self.L2.at[s], "y")

        def third(self, s):
            self.cps[s, 2].wait_recv()
            mine = self.T.at[s, 0, 0]
            add_into(mine, mine, self.L2.at[s])
            if s:
                self.cps[s, 3] = w.send(mine, self.LZ.at[s - 1], lax.rem(z + s, 4))

        def fourth(self):
            for s in (1, 2, 3):
                self.cps[s, 3].wait_recv()

            def body(i, carry):
                at = pl.ds(pl.multiple_of(i * 32, 32), 32)
                tot = self.T[0, 0, 0, at, :].astype(F32)
                for s in range(3):
                    tot = tot + self.LZ[s, at, :].astype(F32)
                self.F[at, :] = tot.astype(BF16)
                return carry

            lax.fori_loop(0, 8, body, 0)
            self.cps["y"] = w.send(self.F, self.Y, "y")

        def last(self):
            self.cps["y"].wait_recv()
            self.out[y] = self.F[...].astype(F32)
            self.out[1 - y] = self.Y[...].astype(F32)

    wo_g = Narrow(TO, LCO, L1O, L2O, LZO, FO, YO, GO, 512)
    wq_g = Narrow(TQ, LCQ, L1Q, L2Q, LZQ, FQ, YQ, GQ, 512)
    qc = []
    dk_cp = {}

    def attend(s):
        wo_cp[s].wait()
        ga_scr[...] = nn(branch_ref[...], wbuf[0].reshape(2048, 512)).astype(BF16).astype(F32)
        if s < 3:
            wo_cp[s + 1] = local(WO.at[s + 1], wbuf.at[0])
        ot_cp[s].wait()
        attend_back(
            s, kv_ref, ga_scr, q_ref, bias_ref, cq_ref, sq_ref, ot_scr, lse_ref, dq_scr, d0, dr, ds_scr, p_scr,
            dk_scr, dv_scr,
        )
        if s < 3:
            ot_cp[s + 1] = local(OT.at[s + 1], ot_scr)
        for t in (1, 2, 3):
            cp = w.copy(dr.at[t - 1, s], ld.at[t - 1, s], lax.rem(z + t, 4), only=z + t >= 4)
            dk_cp[t, s] = cp
            pl.when(z + t >= 4)(cp.start)
        wq_cp[s].wait()

        def columns(i, carry):
            at = pl.ds(pl.multiple_of(i * 512, 512), 512)
            part = nt(dq_scr[s], wbuf[1, i // 2, i % 2].reshape(512, 512))
            if s:
                gn_scr[:, at] += part
            else:
                gn_scr[:, at] = part
            return carry

        lax.fori_loop(0, 4, columns, 0)
        if s < 3:
            wq_cp[s + 1] = local(WQ.at[s + 1], wbuf.at[1])
        w.sent(oc[s + 2] if s < 2 else qc[s - 2])
        grad_part(dq_scr[s], TQ.at[s], S.at[s % 2], every)
        qc.append(w.send(S.at[s % 2], LCQ.at[s], "c"))

    for cp in kept:
        cp.wait()
    wide_x(1, 0)
    wide_y(0, 0)
    wide_x(1, 1)
    for s in (1, 3, 0, 2):
        with mark("B_oc"):
            wo_g.core(s, oc[s])
        wo_g.first(s)
    for name in ("n", "q", "kv", "bias"):
        brought[name].wait()
    turned(n1_ref)
    with mark('B_att0'):
        attend(0)
    with mark("B_wy"):
        wide_y(0, 1)
    with mark('B_att1'):
        attend(1)
    with mark("B_o2"):
        for s in (1, 3):
            wo_g.second(s)
    with mark("B_qc"):
        wq_g.core(1, qc[1])
        wq_g.first(1)
    with mark('B_att2'):
        attend(2)
    with mark("B_wy"):
        wide_y(1, 0)
    with mark("B_qc"):
        wq_g.core(0, qc[0])
        wq_g.first(0)
    with mark('B_att3'):
        attend(3)
    wk_cp = {0: local(WKV.at[0], wk.at[0]), 1: local(WKV.at[1], wk.at[1])}
    with mark("B_qc"):
        for s in (3, 2):
            wq_g.core(s, qc[s])
            wq_g.first(s)
    with mark("B_o2"):
        for s in (0, 2):
            wo_g.second(s)
    with mark("B_o3"):
        for s in (1, 3):
            wo_g.third(s)
    for cp, late in out_cp:
        pl.when(late)(cp.start)
    with mark("B_wy"):
        wide_y(1, 1)
    with mark("B_q2"):
        for s in (1, 3):
            wq_g.second(s)
    with mark("B_o3"):
        for s in (0, 2):
            wo_g.third(s)
    for s in range(4):
        dkv_scr[:, 128 * s : 128 * s + 128] = d0[s]
    for t in (1, 2, 3):

        with mark("B_dkr"):

            @pl.when(z < t)
            def _():
                for s in range(4):
                    dk_cp[t, (s + t) % 4].wait_recv()
                    dkv_scr[:, 128 * s : 128 * s + 128] += ld[t - 1, (s + t) % 4].astype(F32)

    for s in range(4):
        cols = slice(128 * s, 128 * s + 128)
        v = dkv_scr[:, cols]
        dkv = (v * ck_ref[...] - swap_halves(v) * sk_ref[...]).astype(BF16)
        wk_cp[s].wait()

        def columns(i, carry):
            at = pl.ds(pl.multiple_of(i * 512, 512), 512)
            gn_scr[:, at] += nt(dkv, wk[s % 2, i // 2, i % 2].reshape(512, 128))
            return carry

        lax.fori_loop(0, 4, columns, 0)
        if s < 2:
            wk_cp[s + 2] = local(WKV.at[s + 2], wk.at[s % 2])
        if s == 0:
            w.sent(qc[2])
        with mark("B_gk"):
            grad_part(dkv, TK.at[0], S.at[0], cols)
    kc = w.send(S.at[0], LCK.at[0], "c")

    gsum[0:1, :] = jnp.zeros((1, 2048), F32)
    for cp in tok_cp:
        cp.wait()

    def norm_back(i, carry):
        at = pl.ds(pl.multiple_of(i * 32, 32), 32)
        gn = gn_scr[at, :]
        x_in = obuf[at, :].astype(F32)
        inv = lax.rsqrt(jnp.mean(x_in * x_in, axis=1, keepdims=True) + NORM_EPS)
        unit = x_in * inv
        gsum[0:1, :] += jnp.sum(gn * unit, axis=0, keepdims=True)
        scaled = gn * gain1_ref[...]
        inside = jnp.mean(scaled * unit, axis=1, keepdims=True)
        back = (gmid_ref[at, :] + inv * (scaled - unit * inside)).astype(BF16)
        for m, to in enumerate(places):
            gtok_ref[at, pl.ds(to, 256)] = back[:, 256 * m : 256 * m + 256]
        return carry

    brought["g"].wait()
    with mark("B_nb"):
        lax.fori_loop(0, 8, norm_back, 0)
    gsum[1:2, :] = gain2t_ref[...]
    for hi in range(2):
        for mid in range(2):
            for lo in range(2):
                at = 4 * (c ^ mid) + 2 * (x ^ hi) + (y ^ lo)
                gains_ref[:, 256 * (4 * hi + 2 * mid + lo) : 256 * (4 * hi + 2 * mid + lo) + 256] = gsum[
                    :, pl.ds(pl.multiple_of(at * 256, 256), 256)
                ]
    steps = ["c", "x", "y", z + 1 - 2 * lax.rem(z, 2), lax.rem(z + 2, 4)]
    gain_cp = []

    def gain_next(n):
        gland[5 + n] = gains_ref[...]
        gain_cp.append(w.send(gland.at[5 + n], gland.at[n], steps[n]))

    def gain_add(n):
        gain_cp[n].wait_recv()
        gains_ref[...] += gland[n]

    gain_next(0)
    mid_cp = local(MID, gn_scr)
    wk_g = Narrow(TK, LCK, L1K, L2K, LZK, FK, YK, GKV, 128)
    with mark("B_kc"):
        wk_g.core(0, kc)
    with mark("B_kf"):
        wk_g.first(0)
    with mark('B_g0'):
        gain_add(0)
    gain_next(1)
    with mark("B_q2"):
        for s in (0, 2):
            wq_g.second(s)
    with mark("B_we"):
        wide_end(0, 0)
    with mark("B_k2"):
        wk_g.second(0)
    with mark("B_q3"):
        for s in (1, 3, 0, 2):
            wq_g.third(s)
    with mark('B_g1'):
        gain_add(1)
    gain_next(2)
    with mark("B_we"):
        wide_end(0, 1)
    with mark("B_k3"):
        wk_g.cps[0, 2].wait_recv()
    add_into(TK.at[0, 0, 0], TK.at[0, 0, 0], L2K.at[0])
    for s in (1, 2, 3):
        wk_g.cps[s, 3] = w.send(TK.at[0, 0, 0, :, pl.ds(128 * s, 128)], LZK.at[s - 1], lax.rem(z + s, 4))
    with mark('B_g2'):
        gain_add(2)
    gain_next(3)
    with mark("B_of"):
        wo_g.fourth()
    with mark("B_we"):
        wide_end(1, 0)
        wide_end(1, 1)
    with mark('B_g3'):
        gain_add(3)
    gain_next(4)
    with mark("B_ol"):
        wo_g.last()
    with mark("B_qf"):
        wq_g.fourth()
    with mark("B_k4"):
        for s in (1, 2, 3):
            wk_g.cps[s, 3].wait_recv()
    tot = TK[0, 0, 0, :, 0:128].astype(F32)
    for s in range(3):
        tot = tot + LZK[s].astype(F32)
    FK[...] = tot.astype(BF16)
    wk_g.cps["y"] = w.send(FK, YK, "y")
    with mark("B_out"):
        mid_cp.wait()
        for n in range(4):
            if n:
                out_cp[n - 1][0].wait_recv()
            local(OUT.at[0] if n == 0 else LOUT.at[n - 1], obuf).wait()
            add_into(gn_scr, gn_scr, obuf)

        def to_own(i, carry):
            at = pl.ds(pl.multiple_of(i * 32, 32), 32)
            for m, to in enumerate(places):
                bout_ref[at, pl.ds(to, 256)] = gn_scr[at, 256 * m : 256 * m + 256].astype(BF16)
            return carry

        lax.fori_loop(0, 8, to_own, 0)
    with mark('B_g4'):
        gain_add(4)
    with mark("B_last"):
        wq_g.last()
        wk_g.last()
    outs[-1].wait()
    w.finish()


def end_call(args):
    vmem = pl.BlockSpec(memory_space=pltpu.VMEM)
    hbm = pl.BlockSpec(memory_space=pl.ANY)
    outs = [
        ((256, 2048), BF16, vmem), ((2, 2048), F32, vmem),
        ((2, 256, 1408), F32, hbm), ((2, 256, 1408), F32, hbm),
        ((2, 256, 512), F32, vmem), ((2, 256, 512), F32, vmem), ((2, 256, 128), F32, vmem), ((256, 2048), BF16, vmem),
        ((4, 2, 2, 256, 512), BF16, hbm), ((4, 2, 2, 256, 512), BF16, hbm), ((1, 2, 2, 256, 512), BF16, hbm),
        ((2, 2, 256, 1408), BF16, hbm), ((2, 2, 256, 1408), BF16, hbm), ((3, 256, 2048), BF16, hbm),
    ]
    scratch = [
        ((2, 2, 2, 256, 1408), BF16), ((4, 2, 2, 256, 512), BF16), ((4, 2, 2, 256, 512), BF16), ((1, 2, 2, 256, 512), BF16),
        ((2, 2, 2, 256, 512), BF16),
        ((4, 2, 256, 512), BF16), ((4, 2, 256, 512), BF16), ((1, 2, 256, 512), BF16),
        ((4, 256, 512), BF16), ((4, 256, 512), BF16), ((1, 256, 512), BF16),
        ((3, 256, 512), BF16), ((3, 256, 512), BF16), ((3, 256, 128), BF16),
        ((256, 512), BF16), ((256, 512), BF16), ((256, 128), BF16),
        ((256, 512), BF16), ((256, 512), BF16), ((256, 128), BF16),
        ((2, 2, 2, 2, 256, 512), BF16), ((2, 2, 2, 2, 256, 128), BF16), ((2048, 256), BF16), ((256, 512), F32),
        ((4, 256, 512), BF16), ((256, 512), F32), ((4, 256, 128), F32), ((3, 4, 256, 128), BF16), ((3, 4, 256, 128), BF16),
        ((1024, 512), BF16), ((1024, 512), BF16), ((1024, 128), F32), ((1024, 128), F32), ((256, 2048), F32),
        ((2, 2, 256, 1408), BF16), ((512, 256), F32), ((256, 1408), F32), ((2, 2048), F32), ((10, 2, 2048), F32), ((256, 2048), BF16),
        ((256, 2048), BF16), ((256, 2048), F32), ((256, 2048), BF16), ((4, 256, 512), BF16), ((4, 4, 256, 128), BF16),
        ((4, 256, 512), BF16), ((1024, 256), F32),
    ]
    return pl.pallas_call(
        end_kernel,
        out_shape=[jax.ShapeDtypeStruct(a, b) for a, b, _ in outs],
        in_specs=[hbm] * 16 + [vmem] * (len(args) - 16),
        out_specs=[o[2] for o in outs],
        scratch_shapes=[pltpu.VMEM(a, b) for a, b in scratch]
        + [pltpu.SemaphoreType.DMA((96,)), pltpu.SemaphoreType.DMA((96,)), pltpu.SemaphoreType.DMA((96,))],
        compiler_params=pltpu.CompilerParams(
            collective_id=1, has_side_effects=True, vmem_limit_bytes=67043328
        ),
        cost_estimate=pl.CostEstimate(flops=10**11, bytes_accessed=2 * 10**8, transcendentals=0),
    )(*args)


X_SWAP = [(0, 2), (1, 3), (2, 0), (3, 1)]
C_SWAP = [(0, 1), (1, 0), (2, 3), (3, 2)]
Y_SWAP = [(0, 1), (1, 0)]
PAIR = [(0, 1), (1, 0), (2, 3), (3, 2)]
MIDDLE = [(1, 2), (2, 1)]
OUTWARD = [(1, 0), (2, 3)]
INWARD = [(0, 1), (3, 2)]


def over_x(a):
    return lax.ppermute(a, "row", X_SWAP)


def over_c(a):
    return lax.ppermute(a, "row", C_SWAP)


def over_y(a):
    return lax.ppermute(a, "dp", Y_SWAP)


def over_z(a, pairs):
    return lax.ppermute(a, "col", pairs)


def from_slot(a, s):
    return over_z(a, [((i + s) % 4, i) for i in range(4)])


def to_slot(a, s):
    return over_z(a, [(i, (i + s) % 4) for i in range(4)])


def gather_col(own, inner):
    first = over_z(own, PAIR)
    mid = over_z(own, MIDDLE)
    third_in = over_z(first, MIDDLE)
    second = jnp.where(inner, mid, over_z(mid, OUTWARD))
    third = jnp.where(inner, third_in, over_z(third_in, OUTWARD))
    return own, first, second, third


def scatter_col(parts):
    own, first, second, third = parts
    t3 = (third + over_z(third.astype(BF16), INWARD)).astype(BF16)
    t2 = (second + over_z(second.astype(BF16), INWARD)).astype(BF16)
    t1 = (first + over_z(t3, MIDDLE)).astype(BF16)
    v = over_z(t2, MIDDLE)
    w = over_z(t1, PAIR)
    return own + v.astype(F32) + w.astype(F32)


def norm_forward(values, gain_vec):
    mean_sq = jnp.mean(values * values, axis=1, keepdims=True)
    inv_rms = lax.rsqrt(mean_sq + NORM_EPS)
    unit_rows = values * inv_rms
    return (unit_rows, inv_rms, (unit_rows * gain_vec).astype(BF16))


def norm_backward(grad_norm, unit_rows, inv_rms, gain_vec):
    scaled = grad_norm * gain_vec
    inner_sum = jnp.mean(scaled * unit_rows, axis=1, keepdims=True)
    return (inv_rms * (scaled - unit_rows * inner_sum), jnp.sum(grad_norm * unit_rows, axis=0))


def shards(
    tokens, gain_attn, w_query, w_keyval, w_output, gain_mlp, w_gate, w_up, w_down, out_grad,
    document_numbers, positions, *, rows,
):
    width = tokens.shape[1]
    fast = rows == 4
    z = lax.axis_index("col")
    r = lax.axis_index("row")
    y = lax.axis_index("dp")
    inner = (z == 1) | (z == 2)
    x, c = r // 2, r % 2
    blk = width // 8

    def permuted(a, abs_order):
        if not fast:
            return a
        axis = a.ndim - 1
        pieces = []
        for hi in range(2):
            for mid in range(2):
                for lo in range(2):
                    if abs_order:
                        at = 4 * (c ^ mid) + 2 * (x ^ hi) + (y ^ lo)
                    else:
                        at = 4 * (x ^ mid) + 2 * (c ^ hi) + (y ^ lo)
                    pieces.append(lax.dynamic_slice_in_dim(a, at * blk, blk, axis))
        return jnp.concatenate(pieces, axis=axis)

    to_rel = functools.partial(permuted, abs_order=False)
    to_abs = functools.partial(permuted, abs_order=True)

    def gather_rows(block):
        return lax.all_gather(block, "row", axis=0, tiled=True)

    def gather_slots(block):
        full = gather_rows(block)
        return [full] + [from_slot(full, s) for s in (1, 2, 3)]

    tok = to_rel(tokens)
    x_in = tok.astype(F32)
    gain_one = to_rel(gain_attn)
    gain_two = to_rel(gain_mlp)
    unit_one, inv_one, normed_one = norm_forward(x_in, gain_one)
    count = tokens.shape[0]
    my_pos = lax.dynamic_slice_in_dim(positions, z * count, count, 0)
    frequency = ROPE_BASE ** (-(jnp.arange(32, dtype=F32) * 2.0 / HEAD_SIZE))
    angles = my_pos.astype(F32)[:, None] * frequency[None, :]
    co, si = jnp.cos(angles), jnp.sin(angles)
    cos_q = jnp.concatenate([co, co, co, co], axis=1)
    sin_q = jnp.concatenate([-si, si, -si, si], axis=1)
    cos_k = jnp.concatenate([co, co, jnp.ones_like(co), jnp.ones_like(co)], axis=1)
    sin_k = jnp.concatenate([-si, si, jnp.zeros_like(si), jnp.zeros_like(si)], axis=1)
    my_seg = lax.dynamic_slice_in_dim(document_numbers, z * count, count, 0)
    key_seg = jnp.concatenate(
        [lax.dynamic_slice_in_dim(document_numbers, ((z + t) % 4) * count, count, 0) for t in range(4)]
    )
    lane = jnp.arange(count, dtype=jnp.int32)
    key_at = jnp.concatenate([((z + t) % 4) * count + lane for t in range(4)])
    allowed = (key_seg[:, None] == my_seg[None, :]) & (key_at[:, None] <= (z * count + lane)[None, :])
    bias = jnp.where(allowed, 0.0, MASK_FILL).astype(F32)

    def separate():
        full = lax.all_gather(w_keyval, "row", axis=0, tiled=True)
        wkv = jnp.concatenate([full] + [from_slot(full, s) for s in (1, 2, 3)], axis=1)
        wq = gather_slots(w_query)
        wo = gather_slots(w_output.T)
        wg, wu, wd = gather_rows(w_gate), gather_rows(w_up), gather_rows(w_down.T)
        kv = call(
            kv_kernel, [((4, count, 128), BF16)], (normed_one, wkv, cos_k, sin_k), 2 * count * width * 512
        )[0]
        kv_from = [kv]
        for t in (1, 2, 3):
            kv_from.append(over_z(kv, [((i + t) % 4, i) for i in range(4) if i + t >= 4]))
        kv_of = [[kv_from[t][(s - t) % 4] for t in range(4)] for s in range(4)]
        fwd = []
        for s in range(4):
            fwd.append(
                call(
                    fwd_kernel,
                    [((count, 512), BF16), ((count, 512), BF16), ((512, count), F32), ((8, count), F32)],
                    (normed_one, wq[s], *kv_of[s], bias, cos_q, sin_q),
                    2 * count * width * 512 + 8 * 4 * count * 1024 * 256,
                )
            )
        attn = [f[1] for f in fwd]
        mid = x_in + (nt(attn[0], wo[0]) + nt(attn[1], wo[1]) + nt(attn[2], wo[2]) + nt(attn[3], wo[3]))
        unit_two, inv_two, n2 = norm_forward(mid, gain_two)
        dys = gather_col(dy, inner)
        n2s = gather_col(n2, inner)
        outs, gns, acts, ggs, gus = [], [], [], [], []
        for s in range(4):
            gate_pre = nn(n2s[s], wg)
            up_pre = nn(n2s[s], wu)
            grad_act = nn(dys[s], wd)
            sig = jax.nn.sigmoid(gate_pre)
            silu = gate_pre * sig
            act = (silu * up_pre).astype(BF16)
            gg = (grad_act * up_pre * sig * (1.0 + gate_pre * (1.0 - sig))).astype(BF16)
            gu = (grad_act * silu).astype(BF16)
            outs.append(nt(act, wd))
            gns.append(nt(gg, wg) + nt(gu, wu))
            acts.append(act)
            ggs.append(gg)
            gus.append(gu)
        grad_norm_two = scatter_col(gns)
        flat = [jnp.concatenate(v, axis=0) for v in (n2s, dys, acts, ggs, gus)]
        mid_norm, gain2 = norm_backward(grad_norm_two, unit_two, inv_two, gain_two)
        gmid = dy.astype(F32) + mid_norm
        return wq, wo, wkv, kv_of, fwd, attn, mid, outs, flat, gmid, gmid.astype(BF16), gain2

    def together():
        def cut(block):
            return block.reshape(2, block.shape[0] // 2, block.shape[1])

        gain = jnp.stack([gain_attn, gain_mlp])
        WQ, WO, WKV, OUT, n1, q, ot, branch, _, LXM, _, TGU, gd, kv, o, lse, mid, gmid, gain2 = start_call(
            (
                gain, cut(w_query), cut(w_output.T), cut(w_keyval), bias, cos_q, sin_q, cos_k, sin_k, tokens, cut(w_gate),
                cut(w_up), cut(w_down.T), out_grad,
            )
        )
        gtok, gains, gg, gu, gq, go, gkv, bout = end_call(
            (
                WQ, WO, WKV, ot, TGU, LXM, OUT, mid, tokens, branch, gmid, n1, q, kv, o, bias, gain_one[None, :], gain2, lse,
                cos_q, sin_q, cos_k, sin_k,
            )
        )[:8]

        def joined(g):
            return g.reshape(2 * blk, g.shape[-1])

        return (
            bout, gtok, gains[0], joined(gq), joined(gkv), joined(go).T, gains[1],
            joined(gg), joined(gu), joined(gd).T,
        )

    dy = to_rel(out_grad)
    if fast:
        return together()
    wq, wo, wkv, kv_of, fwd, attn, resid_mid, outs, flat, grad_mid, branch, gain_two_term = separate()
    n2_all, dy_all, act_all, gg_all, gu_all = flat
    block_out = (resid_mid + scatter_col([o.astype(F32) for o in outs])).astype(BF16)

    def ordered(lo, hi):
        return jnp.where(y == 0, jnp.concatenate([lo, hi], axis=0), jnp.concatenate([hi, lo], axis=0))

    def weight_grad(act_rel, g):
        half = width // 2
        if not fast:
            full = lax.psum_scatter(tn(act_rel, g).astype(BF16), "row", scatter_dimension=0, tiled=True)
            return lax.psum(full, "dp").astype(F32)
        got = over_c(tn(act_rel[:, half:], g).astype(BF16))
        t = tn(act_rel[:, :half], g) + got.astype(F32)
        q = half // 2
        got = over_x(t[q:].astype(BF16))
        t = (t[:q] + got.astype(F32)).astype(BF16)
        got = over_y(t).astype(F32)
        t = t.astype(F32)
        return ordered(t[: q // 2] + got[q // 2 :], t[q // 2 :] + got[: q // 2])

    def weight_grad_slots(act_rel, gs):
        half = width // 2
        if not fast:
            tot = 0.0
            for s in range(4):
                full = lax.psum_scatter(
                    tn(act_rel, gs[s]).astype(BF16), "row", scatter_dimension=0, tiled=True
                )
                tot = tot + (full if s == 0 else to_slot(full, s)).astype(F32)
            return lax.psum(tot.astype(BF16), "dp").astype(F32)
        tot = 0.0
        for s in range(4):
            got = over_c(tn(act_rel[:, half:], gs[s]).astype(BF16))
            t = tn(act_rel[:, :half], gs[s]) + got.astype(F32)
            b = blk
            t00, t01, t10, t11 = t[:b], t[b : 2 * b], t[2 * b : 3 * b], t[3 * b :]
            if s % 2:
                got = over_y(jnp.concatenate([t01, t11], axis=0).astype(BF16)).astype(F32)
                u0 = t00 + got[:b]
                u1 = t10 + got[b:]
                u = u0 + over_x(u1.astype(BF16)).astype(F32)
            else:
                got = over_x(jnp.concatenate([t10, t11], axis=0).astype(BF16)).astype(F32)
                u0 = t00 + got[:b]
                u1 = t01 + got[b:]
                u = u0 + over_y(u1.astype(BF16)).astype(F32)
            u = u.astype(BF16)
            tot = tot + (u if s == 0 else to_slot(u, s)).astype(F32)
        tot = tot.astype(BF16)
        return ordered(tot.astype(F32), over_y(tot).astype(F32))

    g_down = weight_grad(dy_all, act_all)
    g_gate = weight_grad(n2_all, gg_all)
    g_up = weight_grad(n2_all, gu_all)

    bwd = []
    for s in range(4):
        bwd.append(
            call(
                bwd_kernel,
                [((count, 512), BF16), ((count, 128), F32), ((3, count, 128), BF16)],
                (branch, wo[s], fwd[s][0], *kv_of[s], bias, cos_q, sin_q, fwd[s][2], fwd[s][3]),
                2 * count * width * 512 + 8 * 10 * count * 1024 * 256,
                scratch=(
                    pltpu.VMEM((1024, 512), BF16),
                    pltpu.VMEM((1024, 512), BF16),
                    pltpu.VMEM((1024, 128), F32),
                    pltpu.VMEM((1024, 128), F32),
                ),
            )
        )
    got = []
    for t in (1, 2, 3):
        out = jnp.stack([bwd[s][2][t - 1] for s in range(4)])
        got.append(over_z(out, [(i, (i + t) % 4) for i in range(4) if i + t >= 4]))
    dkv = call(
        dkv_kernel,
        [((4, count, 128), BF16)],
        (*[bwd[s][1] for s in range(4)], *got, cos_k, sin_k),
        count * 512 * 8,
    )[0]
    dkv = jnp.concatenate([dkv[s] for s in range(4)], axis=1)
    dq = [bwd[s][0] for s in range(4)]
    grad_norm_one = nt(dq[0], wq[0]) + nt(dq[1], wq[1]) + nt(dq[2], wq[2]) + nt(dq[3], wq[3])
    grad_norm_one = grad_norm_one + nt(dkv, wkv)
    in_norm, gain_one_term = norm_backward(grad_norm_one, unit_one, inv_one, gain_one)
    grad_tokens = (grad_mid + in_norm).astype(BF16)
    g_output = weight_grad_slots(branch, attn)
    g_query = weight_grad_slots(normed_one, dq)
    g_keyval = weight_grad_slots(normed_one, [dkv[:, 128 * s : 128 * s + 128] for s in range(4)])

    def total(v):
        if not fast:
            return lax.psum(v, ("dp", "row", "col"))
        v = v + over_c(v)
        v = v + over_x(v)
        v = v + over_y(v)
        v = v + over_z(v, PAIR)
        return v + over_z(v, [(0, 2), (1, 3), (2, 0), (3, 1)])

    return (
        to_abs(block_out),
        to_abs(grad_tokens),
        total(to_abs(gain_one_term)),
        g_query,
        g_keyval,
        g_output.T,
        total(to_abs(gain_two_term)),
        g_gate,
        g_up,
        g_down.T,
    )


def solution(mesh):
    spec = P(("dp", "row", "col"), None)
    down = P("row", "col")
    across = P("col", "row")
    seq = P(("dp", "row"))
    return jax.shard_map(
        functools.partial(shards, rows=mesh.shape["row"]),
        mesh=mesh,
        in_specs=(spec, P(), down, down, across, P(), down, down, across, spec, seq, seq),
        out_specs=(spec, spec, P(), down, down, across, P(), down, down, across),
        check_vma=False,
    )
```

```python
import functools
import math

import jax
import jax.numpy as jnp
from jax import lax
from jax.experimental import pallas as pl
from jax.experimental.pallas import tpu as pltpu
from jax.sharding import PartitionSpec as P

HEAD_SIZE = 64
SEQUENCE_LENGTH = 1024
NORM_EPS = 1e-05
ROPE_BASE = 10000.0
MASK_FILL = -1e30
BF16 = jnp.bfloat16
F32 = jnp.float32


def nn(a, b):
    return lax.dot_general(a, b, (((1,), (0,)), ((), ())), preferred_element_type=F32)


def nt(a, b):
    return lax.dot_general(a, b, (((1,), (1,)), ((), ())), preferred_element_type=F32)


def tn(a, b):
    return lax.dot_general(a, b, (((0,), (0,)), ((), ())), preferred_element_type=F32)


def swap_halves(v):
    lane = lax.broadcasted_iota(jnp.int32, v.shape, 1)
    return jnp.where((lane % 64) < 32, pltpu.roll(v, 96, 1), pltpu.roll(v, 32, 1))


def kv_kernel(n_ref, w_ref, c_ref, s_ref, o_ref):
    kv = nn(n_ref[...], w_ref[...])
    for s in range(4):
        v = kv[:, 128 * s : 128 * s + 128]
        o_ref[s] = (v * c_ref[...] + swap_halves(v) * s_ref[...]).astype(BF16)


def load_kv(kv_refs):
    return jnp.concatenate([r[...].astype(F32) for r in kv_refs], axis=0)


def fwd_kernel(n_ref, w_ref, k0, k1, k2, k3, bias_ref, c_ref, s_ref, q_ref, o_ref, ot_ref, lse_ref):
    q = nn(n_ref[...], w_ref[...])
    kv = load_kv((k0, k1, k2, k3))
    k_low = kv[:, :64].astype(BF16)
    v_t = kv.T[64:].astype(BF16)
    for p in range(4):
        cols = slice(128 * p, 128 * p + 128)
        v = q[:, cols]
        rot = (v * c_ref[...] + swap_halves(v) * s_ref[...]) * 0.125
        rot = rot.astype(BF16)
        q_ref[:, cols] = rot
        q_t = rot.astype(F32).T.astype(BF16)
        outs = []
        for e in range(2):
            s_t = nn(k_low, q_t[64 * e : 64 * e + 64]) + bias_ref[...]
            top = jnp.max(s_t, axis=0, keepdims=True)
            ex = jnp.exp(s_t - top)
            tot = jnp.sum(ex, axis=0, keepdims=True)
            outs.append(nn(v_t, ex.astype(BF16)) * (1.0 / tot))
            lse_ref[pl.ds(2 * p + e, 1), :] = top + jnp.log(tot)
        o_t = jnp.concatenate(outs, axis=0)
        ot_ref[cols, :] = o_t
        o_ref[:, cols] = o_t.T.astype(BF16)


def bwd_kernel(
    b_ref, w_ref, q_ref, k0, k1, k2, k3, bias_ref, c_ref, s_ref, ot_ref, lse_ref,
    dq_ref, d0_ref, dr_ref, ds_scr, p_scr, dk_scr, dv_scr,
):
    ga = nn(b_ref[...], w_ref[...]).astype(BF16).astype(F32)
    kv = load_kv((k0, k1, k2, k3))
    k_low = kv[:, :64].astype(BF16)
    v_low = pltpu.roll(kv, 64, 1)[:, :64].astype(BF16)
    k_t = kv.T[:64].astype(BF16)
    lane = lax.broadcasted_iota(jnp.int32, (256, 128), 1)
    for p in range(4):
        cols = slice(128 * p, 128 * p + 128)
        qp = q_ref[:, cols].astype(F32)
        gp = ga[:, cols]
        q_t = qp.T.astype(BF16)
        g_tf = gp.T
        g_t = g_tf.astype(BF16)
        prod = g_tf * ot_ref[cols, :]
        dq_t = []
        for e in range(2):
            half = slice(64 * e, 64 * e + 64)
            s_t = nn(k_low, q_t[half]) + bias_ref[...]
            pr = jnp.exp(s_t - lse_ref[pl.ds(2 * p + e, 1), :])
            dp = nn(v_low, g_t[half])
            inner = jnp.sum(prod[half], axis=0, keepdims=True)
            ds = (pr * (dp - inner)).astype(BF16)
            ds_scr[:, 256 * e : 256 * e + 256] = ds
            p_scr[:, 256 * e : 256 * e + 256] = pr.astype(BF16)
            dq_t.append(nn(k_t, ds))
        qbd = jnp.concatenate(
            [jnp.where(lane < 64, qp, 0.0), jnp.where(lane < 64, 0.0, qp)], axis=0
        ).astype(BF16)
        gbd = jnp.concatenate(
            [jnp.where(lane < 64, gp, 0.0), jnp.where(lane < 64, 0.0, gp)], axis=0
        ).astype(BF16)
        dk = nn(ds_scr[...], qbd)
        dv = nn(p_scr[...], gbd)
        if p == 0:
            dk_scr[...] = dk
            dv_scr[...] = dv
        else:
            dk_scr[...] += dk
            dv_scr[...] += dv
        dqp = jnp.concatenate(dq_t, axis=0).T * 0.125
        dq_ref[:, cols] = (dqp * c_ref[...] - swap_halves(dqp) * s_ref[...]).astype(BF16)
    dk = dk_scr[...]
    dv = dv_scr[...]
    lane = lax.broadcasted_iota(jnp.int32, dk.shape, 1)
    both = jnp.where(lane < 64, dk + pltpu.roll(dk, 64, 1), dv + pltpu.roll(dv, 64, 1))
    d0_ref[...] = both[:256]
    for t in range(3):
        dr_ref[t] = both[256 * (t + 1) : 256 * (t + 2)].astype(BF16)


def dkv_kernel(a0, a1, a2, a3, r1, r2, r3, c_ref, s_ref, o_ref):
    own = (a0, a1, a2, a3)
    got = (r1, r2, r3)
    for s in range(4):
        v = own[s][...]
        for t in range(1, 4):
            v = v + got[t - 1][(s + t) % 4].astype(F32)
        o_ref[s] = (v * c_ref[...] - swap_halves(v) * s_ref[...]).astype(BF16)


def call(body, outs, args, flops, scratch=(), vmem=48 << 20):
    spec = pl.BlockSpec(memory_space=pltpu.VMEM)
    shapes = [jax.ShapeDtypeStruct(s, d) for s, d in outs]
    nbytes = sum(a.size * a.dtype.itemsize for a in args) + sum(
        math.prod(s) * jnp.dtype(d).itemsize for s, d in outs
    )
    return pl.pallas_call(
        body,
        out_shape=shapes,
        in_specs=[spec] * len(args),
        out_specs=[spec] * len(outs),
        scratch_shapes=list(scratch),
        compiler_params=pltpu.CompilerParams(vmem_limit_bytes=vmem),
        cost_estimate=pl.CostEstimate(flops=flops, bytes_accessed=nbytes, transcendentals=0),
    )(*args)


MESH = pl.DeviceIdType.MESH


def mark(name):
    return jax.named_scope(name)


def relative(x, c, y):
    at = []
    for k in range(2):
        for i in range(2):
            for j in range(2):
                at.append(pl.multiple_of(256 * (4 * (x ^ i) + 2 * (c ^ k) + (y ^ j)), 256))
    return at


class Wire:
    def __init__(self, send_sem, recv_sem, z):
        self.send_sem, self.recv_sem, self.z = send_sem, recv_sem, z
        self.count = 0
        self.made = []

    def to(self, where):
        r = lax.axis_index("row")
        if where == "x":
            return {"row": lax.rem(r + 2, 4)}
        if where == "c":
            return {"row": r + 1 - 2 * lax.rem(r, 2)}
        if where == "y":
            return {"dp": 1 - lax.axis_index("dp")}
        return {"col": where}

    def copy(self, src, dst, where, only=None, recv=None):
        k = self.count
        self.count += 1
        cp = pltpu.make_async_remote_copy(
            src_ref=src, dst_ref=dst, send_sem=self.send_sem.at[k], recv_sem=self.recv_sem.at[k if recv is None else recv],
            device_id=self.to(where), device_id_type=MESH,
        )
        self.made.append((cp, only))
        return cp

    def sent(self, cp):
        self.made = [m for m in self.made if m[0] is not cp]
        cp.wait_send()

    def send(self, src, dst, where):
        cp = self.copy(src, dst, where)
        cp.start()
        return cp

    def finish(self):
        for cp, only in self.made:
            if only is None:
                cp.wait_send()
            else:
                pl.when(only)(cp.wait_send)


def greet(z):
    barrier = pltpu.get_barrier_semaphore()
    wire = Wire(None, None, z)
    for where in ("x", "c", "y"):
        pl.semaphore_signal(barrier, inc=1, device_id=wire.to(where), device_id_type=MESH)
    for d in (1, 2, 3):
        pl.semaphore_signal(barrier, inc=1, device_id={"col": lax.rem(z + d, 4)}, device_id_type=MESH)
    pl.semaphore_wait(barrier, 6)


def attend_slot(w_ref, n_ref, kv_scr, s, bias_ref, c_ref, s_ref, q_ref, o_ref, ot_ref, lse_ref, q_scr):
    q_scr[...] = nn(n_ref[...], w_ref[...])
    kv = jnp.concatenate([kv_scr[t, (s - t) % 4].astype(F32) for t in range(4)], axis=0)
    k_low = kv[:, :64].astype(BF16)
    v_t = kv.T[64:].astype(BF16)

    def pair(p, carry):
        at = pl.multiple_of(p * 128, 128)
        cols = pl.ds(at, 128)
        v = q_scr[:, cols]
        rot = ((v * c_ref[...] + swap_halves(v) * s_ref[...]) * 0.125).astype(BF16)
        q_ref[:, cols] = rot
        q_t = rot.astype(F32).T.astype(BF16)
        outs = []
        for e in range(2):
            s_t = nn(k_low, q_t[64 * e : 64 * e + 64]) + bias_ref[...]
            top = jnp.max(s_t, axis=0, keepdims=True)
            ex = jnp.exp(s_t - top)
            tot = jnp.sum(ex, axis=0, keepdims=True)
            outs.append(nn(v_t, ex.astype(BF16)) * (1.0 / tot))
            lse_ref[s, pl.ds(2 * p + e, 1), :] = top + jnp.log(tot)
        o_t = jnp.concatenate(outs, axis=0)
        ot_ref[cols, :] = o_t
        o_ref[s, :, cols] = o_t.T.astype(BF16)
        return carry

    lax.fori_loop(0, 4, pair, 0)


def start_kernel(
    gain_ref, wq_ref, wo_ref, wkv_ref, bias_ref, cq_ref, sq_ref, ck_ref, sk_ref, tok_ref, wg_ref, wu_ref, wd_ref, dy_ref,
    WQ, WO, WKV, OUT, NONE, QS, OT, BRANCH, LCM, LXM, LYM, TGU, GDOWN, kv_out, o_ref, lse_ref, mid_ref, gmid_ref, gain2_out,
    wm, gn_scr, N2, DY, wbuf, wkv_scr, q_scr, q_stage, ot_stage, gate_scr, up_scr, grad_scr, hid, out_stage, pre,
    gains, send_sem, recv_sem, loc_sem,
):
    own_scr = gmid_ref
    kv_scr = kv_out
    r = lax.axis_index("row")
    x, c = r // 2, lax.rem(r, 2)
    z = lax.axis_index("col")
    y = lax.axis_index("dp")
    inner = (z == 1) | (z == 2)
    outer = jnp.logical_not(inner)
    w = Wire(send_sem, recv_sem, z)
    locs = []

    def local(src, dst):
        cp = pltpu.make_async_copy(src, dst, loc_sem.at[len(locs)])
        cp.start()
        locs.append(cp)
        return cp

    greet(z)
    blocks = {"kv": (wkv_ref, WKV), "q": (wq_ref, WQ), "o": (wo_ref, WO)}
    ev = {}

    def start_z(name):
        ref, full = blocks[name]
        for s in (1, 2, 3):
            d = 4 - s
            ev[name, s, "z"] = w.send(ref.at[y], full.at[s, 0, 0, 0], lax.rem(z + d, 4))

    def start_own(name):
        ref, full = blocks[name]
        ev[name, 0, "x"] = w.send(ref.at[y], full.at[0, 0, 1, 0], "x")
        ev[name, 0, "own"] = [local(ref.at[y], full.at[0, 0, 0, 0]), local(ref.at[1 - y], full.at[0, 0, 0, 1])]
        ev[name, 0, "c0"] = [
            w.send(ref.at[y], full.at[0, 1, 0, 0], "c"), w.send(ref.at[1 - y], full.at[0, 1, 0, 1], "c")
        ]

    def own_second(name):
        full = blocks[name][1]
        ev[name, 0, "x"].wait_recv()
        ev[name, 0, "y"] = w.send(full.at[0, 0, 1, 0], full.at[0, 0, 1, 1], "y")

    def own_core(name):
        full = blocks[name][1]
        ev[name, 0, "y"].wait_recv()
        ev[name, 0, "c"] = w.send(full.at[0, 0, 1], full.at[0, 1, 1], "c")

    def first(name, s):
        full = blocks[name][1]
        ev[name, s, "z"].wait_recv()
        if (s % 2 == 1) != (name == "o"):
            ev[name, s, 1] = w.send(full.at[s, 0, 0, 0], full.at[s, 0, 0, 1], "y")
        else:
            ev[name, s, 1] = w.send(full.at[s, 0, 0, 0], full.at[s, 0, 1, 0], "x")

    def second(name, s):
        full = blocks[name][1]
        ev[name, s, 1].wait_recv()
        if (s % 2 == 1) != (name == "o"):
            ev[name, s, 2] = w.send(full.at[s, 0, 0], full.at[s, 0, 1], "x")
        else:
            ev[name, s, 2] = w.send(full.at[s, 0, :, 0], full.at[s, 0, :, 1], "y")

    def core(name, s):
        full = blocks[name][1]
        ev[name, s, 2].wait_recv()
        ev[name, s, "c"] = w.send(full.at[s, 0], full.at[s, 1], "c")

    def whole(name, s):
        ev[name, s, "c"].wait_recv()
        if s == 0:
            for cp in ev[name, 0, "c0"]:
                cp.wait_recv()
            for cp in ev[name, 0, "own"]:
                cp.wait()

    mats = {"g": (wg_ref, wm.at[0]), "u": (wu_ref, wm.at[1]), "d": (wd_ref, wm.at[2])}

    def mat_start(name):
        ref, full = mats[name]
        ev[name, "x"] = w.send(ref.at[y], full.at[0, 1, 0], "x")
        ev[name, "own"] = [local(ref.at[y], full.at[0, 0, 0]), local(ref.at[1 - y], full.at[0, 0, 1])]
        ev[name, "c0"] = [
            w.send(ref.at[y], full.at[1, 0, 0], "c"), w.send(ref.at[1 - y], full.at[1, 0, 1], "c")
        ]

    def mat_second(name):
        full = mats[name][1]
        ev[name, "x"].wait_recv()
        ev[name, "y"] = w.send(full.at[0, 1, 0], full.at[0, 1, 1], "y")

    def mat_core(name):
        full = mats[name][1]
        ev[name, "y"].wait_recv()
        ev[name, "c"] = w.send(full.at[0, 1], full.at[1, 1], "c")

    def mat_whole(name):
        ev[name, "c"].wait_recv()
        for cp in ev[name, "c0"]:
            cp.wait_recv()
        for cp in ev[name, "own"]:
            cp.wait()

    buddy = z + 1 - 2 * lax.rem(z, 2)
    middle = lax.rem(7 - z, 4)

    def some(cond, cp):
        pl.when(cond)(cp.start)
        return cp

    def rows_start(full):
        f = w.send(full.at[0], full.at[1], buddy)
        m = some(inner, w.copy(full.at[0], full.at[2], middle, only=inner))
        return [f, m]

    def rows_first(full, c):
        c[0].wait_recv()
        c.append(some(inner, w.copy(full.at[1], full.at[3], middle, only=inner)))

    def rows_second(full, c):
        pl.when(inner)(c[1].wait_recv)
        c.append(some(inner, w.copy(full.at[2], full.at[2], buddy, only=inner)))

    def rows_third(full, c):
        pl.when(inner)(c[2].wait_recv)
        c.append(some(inner, w.copy(full.at[3], full.at[3], buddy, only=inner)))

    def rows_have_second(c):
        pl.when(outer)(c[3].wait_recv)

    def rows_have_third(c):
        pl.when(outer)(c[4].wait_recv)

    tok_rel, n1_rel = gn_scr.at[0], gn_scr.at[1]
    moved = []
    for m, at in enumerate(relative(x, c, y)):
        to = pl.ds(256 * m, 256)
        moved.append(local(tok_ref.at[:, pl.ds(at, 256)], tok_rel.at[:, to]))
        moved.append(local(dy_ref.at[:, pl.ds(at, 256)], DY.at[0, :, to]))
        gains[:, to] = gain_ref[:, pl.ds(at, 256)]
    start_z("kv")
    start_own("kv")
    start_z("q")
    start_own("q")

    def norm_one(i, carry):
        at = pl.ds(pl.multiple_of(i * 32, 32), 32)
        x_in = tok_rel[at, :].astype(F32)
        inv = lax.rsqrt(jnp.mean(x_in * x_in, axis=1, keepdims=True) + NORM_EPS)
        n1_rel[at, :] = (x_in * inv * gains[0:1, :]).astype(BF16)
        mid_ref[at, :] = x_in
        return carry

    for cp in moved:
        cp.wait()
    with mark("A_norm1"):
        lax.fori_loop(0, 8, norm_one, 0)
    n1_out = local(n1_rel, NONE)
    for t in (1, 2, 3):

        @pl.when(z + t < 4)
        def _():
            kv_scr[t] = jnp.zeros_like(kv_scr[t])

    with mark("A_kv1"):
        own_second("kv")
        for s in (1, 2, 3):
            first("kv", s)
        own_second("q")
    with mark("A_kv2"):
        for s in (2, 1, 3):
            second("kv", s)
        own_core("kv")
    with mark("A_q1"):
        for s in (1, 2, 3):
            first("q", s)
    with mark("A_kv3"):
        for s in (2, 1, 3):
            core("kv", s)
    own_core("q")
    with mark("A_q2"):
        for s in (2, 1, 3):
            second("q", s)
    start_own("o")
    mat_start("g")
    got = []
    with mark("A_kvw"):
        for s in range(4):
            whole("kv", s)
            if s < 2:
                got.append(local(WKV.at[s], wkv_scr.at[s]))
        for s in range(4):
            got[s].wait()
            kv = nn(n1_rel[...], wkv_scr[s % 2].reshape(2048, 128))
            if s < 2:
                got.append(local(WKV.at[s + 2], wkv_scr.at[s]))
            kv_scr[0, s] = (kv * ck_ref[...] + swap_halves(kv) * sk_ref[...]).astype(BF16)
    kv_cp = {}
    for s in (0, 2, 1, 3):
        for d in (1, 2, 3):
            u = (s + d) % 4
            cp = w.copy(kv_scr.at[0, u], kv_scr.at[4 - d, u], lax.rem(z + d, 4), only=z + d < 4)
            kv_cp[4 - d, s] = cp
            pl.when(z + d < 4)(cp.start)
    cps, kept = {}, []
    with mark("A_q0w"):
        whole("q", 0)
    cps[0] = local(WQ.at[0], wbuf.at[0])
    start_z("o")
    dyc = rows_start(DY)
    def attend(s, b):
        cps[s].wait()
        for cp in kept:
            cp.wait()
        kept.clear()
        with mark("A_kvr"):
            for t in (1, 2, 3):
                pl.when(z + t >= 4)(kv_cp[t, s].wait_recv)
        with mark(f"A_att{s}"):
            attend_slot(
                wbuf.at[b].reshape(2048, 512), n1_rel, kv_scr, s, bias_ref, cq_ref, sq_ref, q_stage, o_ref, ot_stage,
                lse_ref, q_scr,
            )
        kept.append(local(q_stage, QS.at[s]))
        kept.append(local(ot_stage, OT.at[s]))

    attend(0, 0)
    with mark("A_q3"):
        core("q", 2)
        whole("q", 2)
    cps[2] = local(WQ.at[2], wbuf.at[1])
    attend(2, 1)
    with mark("A_o1"):
        own_second("o")
        for s in (1, 2, 3):
            first("o", s)
    mat_start("u")
    with mark("A_q4"):
        core("q", 1)
        core("q", 3)
        whole("q", 1)
    cps[1] = local(WQ.at[1], wbuf.at[0])
    whole("q", 3)
    cps[3] = local(WQ.at[3], wbuf.at[1])
    with mark("A_m1"):
        mat_second("g")
    with mark("A_dy1"):
        rows_first(DY, dyc)
    attend(1, 0)
    with mark("A_o2"):
        own_core("o")
        for s in (2, 1, 3):
            second("o", s)
    mat_start("d")
    with mark("A_dy2"):
        rows_second(DY, dyc)
    oc = {}
    attend(3, 1)
    with mark("A_m2"):
        mat_second("u")
    with mark("A_dy3"):
        rows_third(DY, dyc)
    with mark("A_o3"):
        for s in (2, 1, 3):
            core("o", s)
    for k, s in enumerate((0, 2, 1, 3)):
        with mark("A_oproj"):
            if s == 0:
                whole("o", 0)
                oc[0] = local(WO.at[0], wbuf.at[0])
            oc[s].wait()
            if k < 3:
                nxt = (2, 1, 3)[k]
                whole("o", nxt)
                oc[nxt] = local(WO.at[nxt], wbuf.at[(k + 1) % 2])

            def columns(i, carry):
                at = pl.ds(pl.multiple_of(i * 512, 512), 512)
                mid_ref[:, at] += nt(o_ref[s], wbuf[k % 2, i // 2, i % 2].reshape(512, 512))
                return carry

            lax.fori_loop(0, 4, columns, 0)

    def norm_two(i, carry):
        at = pl.ds(pl.multiple_of(i * 32, 32), 32)
        mid = mid_ref[at, :]
        inv = lax.rsqrt(jnp.mean(mid * mid, axis=1, keepdims=True) + NORM_EPS)
        N2[0, at, :] = (mid * inv * gains[1:2, :]).astype(BF16)
        return carry

    lax.fori_loop(0, 8, norm_two, 0)
    n2c = rows_start(N2)
    with mark("A_m2"):
        mat_core("g")
    with mark("A_m3"):
        mat_second("d")
        mat_core("u")
    with mark("A_n1"):
        rows_first(N2, n2c)
        rows_second(N2, n2c)
    with mark("A_m4"):
        mat_core("d")
        for name in mats:
            mat_whole(name)
    n1_out.wait()
    for cp in kept:
        cp.wait()
    def slot(a, stored):
        dy_a = DY[a]
        n2_a = N2[a]
        gate_scr[...] = nn(n2_a, wm[0].reshape(2048, 1408))
        up_scr[...] = nn(n2_a, wm[1].reshape(2048, 1408))
        grad_scr[...] = nn(dy_a, wm[2].reshape(2048, 1408))
        for cp in stored:
            cp.wait()

        def rows(i, carry):
            at = pl.ds(pl.multiple_of(i * 32, 32), 32)
            gate = gate_scr[at, :]
            up = up_scr[at, :]
            ga = grad_scr[at, :]
            sig = 1.0 / (1.0 + jnp.exp(-gate))
            silu = gate * sig
            hid[2, a, at, :] = (silu * up).astype(BF16)
            hid[0, a, at, :] = (ga * up * sig * (1.0 + gate * (1.0 - sig))).astype(BF16)
            hid[1, a, at, :] = (ga * silu).astype(BF16)
            return carry

        lax.fori_loop(0, 8, rows, 0)

        def columns(c, carry):
            at = pl.ds(pl.multiple_of(c * 512, 512), 512)
            k, i = c // 2, c % 2
            out_stage[:, at] = nt(hid[2, a], wm[2, k, i].reshape(512, 1408)).astype(BF16)
            gn = nt(hid[0, a], wm[0, k, i].reshape(512, 1408)) + nt(hid[1, a], wm[1, k, i].reshape(512, 1408))
            if a == 0:
                own_scr[:, at] = gn
            else:
                gn_scr[a - 1, :, at] = gn.astype(BF16)
            return carry

        lax.fori_loop(0, 4, columns, 0)
        return [local(out_stage, OUT.at[a])]

    def send_sum(a, n, where):
        for i in range(2):
            for j in range(2):
                piece = gn_scr.at[a - 1, :, pl.ds(1024 * i + 512 * j, 512)]
                w.copy(piece, wbuf.at[n // 2, n % 2, i, j], where, recv=112 + 4 * n + 2 * i + j).start()

    def sum_arrived(n):
        for i in range(2):
            for j in range(2):
                pltpu.make_async_remote_copy(
                    src_ref=gn_scr.at[0, :, pl.ds(0, 512)], dst_ref=wbuf.at[n // 2, n % 2, i, j],
                    send_sem=send_sem.at[0], recv_sem=recv_sem.at[112 + 4 * n + 2 * i + j],
                    device_id=w.to("c"), device_id_type=MESH,
                ).wait_recv()

    place = 1 + jnp.where(inner, 0, 1)
    second_at = jnp.where(z < 2, 2, 1)
    third_at = jnp.where(z < 2, 3, 0)
    with mark("A_slot0"):
        stored = slot(0, [])
    with mark("A_w1"):
        rows_have_second(dyc)
        rows_have_third(dyc)
        rows_third(N2, n2c)
    with mark("A_slot1"):
        stored = slot(1, stored)
    send_sum(1, 0, buddy)
    with mark("A_w2"):
        rows_have_second(n2c)
    with mark("A_slot2"):
        stored = slot(2, stored)
    send_sum(2, place, second_at)
    with mark("A_w3"):
        rows_have_third(n2c)
    with mark("A_slot3"):
        stored = slot(3, stored)
    send_sum(3, place, third_at)

    def add_rows(into, n):
        def body(i, carry):
            at = pl.ds(pl.multiple_of(i * 32, 32), 32)
            for h in range(2):
                for j in range(2):
                    cols = slice(1024 * h + 512 * j, 1024 * h + 512 * j + 512)
                    other = wbuf[n // 2, n % 2, h, j, at, :].astype(F32)
                    into[at, cols] = (into[at, cols].astype(F32) + other).astype(into.dtype)
            return carry

        lax.fori_loop(0, 8, body, 0)

    wide = {2: DY, 0: N2, 1: N2}
    mc, xs, ys = {}, {}, {}

    def wide_part(m, k):
        def tile(n, carry):
            cols = pl.ds(pl.multiple_of(1024 * k + 256 * n, 256), 256)
            src = jnp.concatenate([wide[m][a, :, cols] for a in range(4)], axis=0)
            wm[m, k, n // 2, n % 2] = tn(src, hid[m].reshape(1024, 1408)).astype(BF16)
            return carry

        with mark("A_dw"):
            lax.fori_loop(0, 4, tile, 0)
        if k:
            mc[m] = w.send(wm.at[m, 1], LCM.at[m], "c")

    turn = [0]

    def fetch(src):
        b = turn[0] % 2
        turn[0] += 1
        return pre.at[b], local(src, pre.at[b])

    def wide_core(m):
        with mark("A_wc"):
            mc[m].wait_recv()
            order = [(1, 0), (1, 1), (0, 0), (0, 1)]
            nxt = fetch(LCM.at[m, 1, 0])
            for n, (i, j) in enumerate(order):
                buf, cp = nxt
                if n < 3:
                    nxt = fetch(LCM.at[m, order[n + 1][0], order[n + 1][1]])
                cp.wait()
                add_into(wm.at[m, 0, i, j], wm.at[m, 0, i, j], buf)

    def wide_x(m, j):
        xs[m, j] = w.send(wm.at[m, 0, 1, j], LXM.at[m, j], "x")

    def wide_y(m, j):
        with mark("A_wy"):
            xs[m, j].wait_recv()
            buf, cp = fetch(LXM.at[m, j])
            cp.wait()
            add_into(wm.at[m, 0, 0, j], wm.at[m, 0, 0, j], buf)
            ys[m, j] = w.send(wm.at[m, 0, 0, j], LYM.at[m, 1 - j], "y")

    def wide_end(m, j):
        with mark("A_we"):
            ys[m, 1 - j].wait_recv()
            buf, cp = fetch(LYM.at[m, j])
            cp.wait()
            fin = (gate_scr, up_scr)[j]
            add_into(fin, wm.at[m, 0, 0, j], buf)
            return local(fin, GDOWN.at[lax.rem(y + j, 2)])

    for cp in stored:
        cp.wait()
    for name in mats:
        w.sent(ev[name, "y"])
        w.sent(ev[name, "c"])
    wide_part(2, 1)
    wide_part(2, 0)
    wide_core(2)
    wide_x(2, 0)
    wide_x(2, 1)
    wide_part(0, 1)
    wide_part(0, 0)
    wide_core(0)
    wide_x(0, 0)
    wide_y(2, 0)
    wide_part(1, 1)
    wide_part(1, 0)
    wide_y(2, 1)
    wide_core(1)
    saved = [local(wm.at[0, 0, 0], TGU.at[0, 0]), local(wm.at[0, 0, 1, 1], TGU.at[0, 1, 1])]
    saved.append(local(wm.at[1, 0], TGU.at[1]))
    with mark("A_r0"):
        sum_arrived(0)
    add_rows(own_scr, 0)
    with mark("A_r1"):
        sum_arrived(1)
        sum_arrived(2)
    add_rows(own_scr, 1)
    add_rows(own_scr, 2)
    gain2_out[...] = jnp.zeros_like(gain2_out)

    def norm_back(i, carry):
        at = pl.ds(pl.multiple_of(i * 32, 32), 32)
        gn = own_scr[at, :]
        mid = mid_ref[at, :]
        inv = lax.rsqrt(jnp.mean(mid * mid, axis=1, keepdims=True) + NORM_EPS)
        unit = mid * inv
        gain2_out[...] += jnp.sum(gn * unit, axis=0, keepdims=True)
        scaled = gn * gains[1:2, :]
        inside = jnp.mean(scaled * unit, axis=1, keepdims=True)
        gmid = DY[0, at, :].astype(F32) + inv * (scaled - unit * inside)
        gmid_ref[at, :] = gmid
        out_stage[at, :] = gmid.astype(BF16)
        return carry

    lax.fori_loop(0, 8, norm_back, 0)
    last = [local(out_stage, BRANCH)]
    last.append(wide_end(2, 0))
    last.append(wide_end(2, 1))
    with mark("A_end"):
        xs[0, 0].wait_recv()
    for cp in last + saved:
        cp.wait()
    assert w.count <= 112
    w.finish()


def start_call(args):
    vmem = pl.BlockSpec(memory_space=pltpu.VMEM)
    hbm = pl.BlockSpec(memory_space=pl.ANY)
    outs = [
        ((4, 2, 2, 2, 256, 512), BF16, hbm), ((4, 2, 2, 2, 256, 512), BF16, hbm),
        ((4, 2, 2, 2, 256, 128), BF16, hbm), ((4, 256, 2048), BF16, hbm),
        ((256, 2048), BF16, hbm), ((4, 256, 512), BF16, hbm), ((4, 512, 256), F32, hbm), ((256, 2048), BF16, hbm),
        ((3, 2, 2, 256, 1408), BF16, hbm), ((3, 2, 256, 1408), BF16, hbm), ((3, 2, 256, 1408), BF16, hbm),
        ((2, 2, 2, 256, 1408), BF16, hbm), ((2, 256, 1408), F32, hbm),
        ((4, 4, 256, 128), BF16, vmem), ((4, 256, 512), BF16, vmem), ((4, 8, 256), F32, vmem),
        ((256, 2048), F32, vmem), ((256, 2048), F32, vmem), ((1, 2048), F32, vmem),
    ]
    scratch = [
        ((3, 2, 2, 2, 256, 1408), BF16), ((3, 256, 2048), BF16), ((4, 256, 2048), BF16), ((4, 256, 2048), BF16),
        ((2, 2, 2, 2, 256, 512), BF16), ((2, 2, 2, 2, 256, 128), BF16), ((256, 512), F32),
        ((256, 512), BF16), ((512, 256), F32), ((256, 1408), F32), ((256, 1408), F32), ((256, 1408), F32),
        ((3, 4, 256, 1408), BF16), ((256, 2048), BF16), ((2, 256, 1408), BF16), ((2, 2048), F32),
    ]
    return pl.pallas_call(
        start_kernel,
        out_shape=[jax.ShapeDtypeStruct(a, b) for a, b, _ in outs],
        in_specs=[vmem] * 9 + [hbm] * (len(args) - 9),
        out_specs=[o[2] for o in outs],
        scratch_shapes=[pltpu.VMEM(a, b) for a, b in scratch]
        + [pltpu.SemaphoreType.DMA((128,)), pltpu.SemaphoreType.DMA((128,)), pltpu.SemaphoreType.DMA((128,))],
        compiler_params=pltpu.CompilerParams(
            collective_id=0, has_side_effects=True, vmem_limit_bytes=67043328
        ),
        cost_estimate=pl.CostEstimate(flops=10**10, bytes_accessed=10**8, transcendentals=0),
    )(*args)


def attend_back(s, kv_of, ga_scr, q_ref, bias_ref, c_ref, s_ref, ot_ref, lse_ref, dq_scr, d0, dr, ds_scr, p_scr, dk_scr, dv_scr):
    kv = jnp.concatenate([kv_of[t, (s - t) % 4].astype(F32) for t in range(4)], axis=0)
    k_low = kv[:, :64].astype(BF16)
    v_low = pltpu.roll(kv, 64, 1)[:, :64].astype(BF16)
    k_t = kv.T[:64].astype(BF16)
    dk_scr[...] = jnp.zeros_like(dk_scr)
    dv_scr[...] = jnp.zeros_like(dv_scr)

    def pair(p, carry):
        cols = pl.ds(pl.multiple_of(p * 128, 128), 128)
        lane = lax.broadcasted_iota(jnp.int32, (256, 128), 1)
        qp = q_ref[s, :, cols].astype(F32)
        gp = ga_scr[:, cols]
        q_t = qp.T.astype(BF16)
        g_tf = gp.T
        g_t = g_tf.astype(BF16)
        prod = g_tf * ot_ref[cols, :]
        dq_t = []
        for e in range(2):
            half = slice(64 * e, 64 * e + 64)
            s_t = nn(k_low, q_t[half]) + bias_ref[...]
            pr = jnp.exp(s_t - lse_ref[s, pl.ds(2 * p + e, 1), :])
            dp = nn(v_low, g_t[half])
            inner = jnp.sum(prod[half], axis=0, keepdims=True)
            ds = (pr * (dp - inner)).astype(BF16)
            ds_scr[:, 256 * e : 256 * e + 256] = ds
            p_scr[:, 256 * e : 256 * e + 256] = pr.astype(BF16)
            dq_t.append(nn(k_t, ds))
        qbd = jnp.concatenate(
            [jnp.where(lane < 64, qp, 0.0), jnp.where(lane < 64, 0.0, qp)], axis=0
        ).astype(BF16)
        gbd = jnp.concatenate(
            [jnp.where(lane < 64, gp, 0.0), jnp.where(lane < 64, 0.0, gp)], axis=0
        ).astype(BF16)
        dk_scr[...] += nn(ds_scr[...], qbd)
        dv_scr[...] += nn(p_scr[...], gbd)
        dqp = jnp.concatenate(dq_t, axis=0).T * 0.125
        dq_scr[s, :, cols] = (dqp * c_ref[...] - swap_halves(dqp) * s_ref[...]).astype(BF16)
        return carry

    lax.fori_loop(0, 4, pair, 0)
    dk = dk_scr[...]
    dv = dv_scr[...]
    lane = lax.broadcasted_iota(jnp.int32, dk.shape, 1)
    both = jnp.where(lane < 64, dk + pltpu.roll(dk, 64, 1), dv + pltpu.roll(dv, 64, 1))
    d0[s] = both[:256]
    for t in range(3):
        dr[t, s] = both[256 * (t + 1) : 256 * (t + 2)].astype(BF16)


def add_into(into, one, other, step=32):
    def body(i, carry):
        at = pl.ds(pl.multiple_of(i * step, step), step)
        into[at, :] = (one[at, :].astype(F32) + other[at, :].astype(F32)).astype(into.dtype)
        return carry

    lax.fori_loop(0, into.shape[0] // step, body, 0)


def end_kernel(
    WQ, WO, WKV, OT, TGU, LXM, OUT, MID, TOK, BRANCH, GMID, NONE, QS, KVS, OS, BIAS, gain1_ref, gain2t_ref,
    lse_ref, cq_ref, sq_ref, ck_ref, sk_ref,
    gtok_ref, gains_ref, GGT, GUP, GQ, GO, GKV, bout_ref, LCO, LCQ, LCK, LYM, LX, LOUT,
    TM, TO, TQ, TK, S, L1O, L1Q, L1K, L2O, L2Q, L2K, LZO, LZQ, LZK, FO, FQ, FK, YO, YQ, YK,
    wbuf, wk, act_t, ga_scr, dq_scr, dkv_scr, d0, dr, ld, ds_scr, p_scr, dk_scr, dv_scr, gn_scr, pre, ot_scr, fin, gsum, gland, obuf, branch_ref, gmid_ref, n1_ref, q_ref, kv_ref, o_ref, bias_ref,
    send_sem, recv_sem, loc_sem,
):
    z = lax.axis_index("col")
    y = lax.axis_index("dp")
    r = lax.axis_index("row")
    x, c = r // 2, lax.rem(r, 2)
    w = Wire(send_sem, recv_sem, z)
    locs = []

    def local(src, dst):
        cp = pltpu.make_async_copy(src, dst, loc_sem.at[len(locs)])
        cp.start()
        locs.append(cp)
        return cp

    brought = {
        "o": local(OS, o_ref), "b": local(BRANCH, branch_ref), "q": local(QS, q_ref), "kv": local(KVS, kv_ref),
        "bias": local(BIAS, bias_ref), "n": local(NONE, n1_ref), "g": local(GMID, gmid_ref),
    }
    greet(z)
    finals = (GGT, GUP)
    places = relative(x, c, y)
    tok_cp = [local(TOK.at[:, pl.ds(at, 256)], obuf.at[:, pl.ds(256 * m, 256)]) for m, at in enumerate(places)]
    kept = [local(TGU.at[0, 0], TM.at[0, 0]), local(TGU.at[1], TM.at[1])]
    xs, ys = {}, {}
    xs[0, 1] = w.send(TGU.at[0, 1, 1], LX.at[0, 1], "x")
    buddy = z + 1 - 2 * lax.rem(z, 2)
    out_cp = []
    for s in (1, 2, 3):
        to = lax.rem(z + s, 4)
        second = jnp.where(z < 2, 2, 1)
        slot = jnp.where(to == buddy, 1, jnp.where(to == second, 2, 3))
        late = (slot == 3) & (z >= 2)
        out_cp.append((w.copy(OUT.at[slot], LOUT.at[s - 1], to), late))
        pl.when(jnp.logical_not(late))(out_cp[-1][0].start)
    wo_cp = {0: local(WO.at[0], wbuf.at[0])}
    wq_cp = {0: local(WQ.at[0], wbuf.at[1])}
    ot_cp = {0: local(OT.at[0], ot_scr)}

    def turned(src):
        for j in range(8):
            act_t[256 * j : 256 * j + 256, :] = src[:, 256 * j : 256 * j + 256].astype(F32).T.astype(BF16)

    def grad_part(g, keep, give, cols):
        for i in range(2):
            for j in range(2):
                at = 512 * i + 256 * j
                give[i, j, :, cols] = nn(act_t[1024 + at : 1024 + at + 256, :], g).astype(BF16)
        for i in range(2):
            for j in range(2):
                at = 512 * i + 256 * j
                keep[i, j, :, cols] = nn(act_t[at : at + 256, :], g).astype(BF16)

    every = slice(0, 512)
    brought["b"].wait()
    brought["o"].wait()
    with mark("B_turn"):
        turned(branch_ref)
    oc = []
    for s in range(4):
        if s > 1:
            w.sent(oc[s - 2])
        with mark("B_go"):
            grad_part(o_ref[s], TO.at[s], S.at[s % 2], every)
        oc.append(w.send(S.at[s % 2], LCO.at[s], "c"))

    slots = [0]

    def wide_x(m, j):
        xs[m, j] = w.send(TM.at[m, 1, j], LX.at[m, j], "x")

    def wide_y(m, j):
        if (m, j) != (0, 0):
            xs[m, j].wait_recv()
        b = slots[0] % 2
        slots[0] += 1
        local((LXM if (m, j) == (0, 0) else LX).at[m, j], pre.at[b, 0]).wait()
        add_into(TM.at[m, 0, j], TM.at[m, 0, j], pre.at[b, 0])
        ys[m, j] = w.send(TM.at[m, 0, j], LYM.at[m, 1 - j], "y")

    outs = []

    def wide_end(m, j):
        ys[m, 1 - j].wait_recv()
        b = slots[0] % 2
        slots[0] += 1
        local(LYM.at[m, j], pre.at[b, 0]).wait()
        if len(outs) >= 1:
            outs[-1].wait()
        add_into(fin, TM.at[m, 0, j], pre.at[b, 0])
        outs.append(local(fin, finals[m].at[lax.rem(y + j, 2)]))

    class Narrow:
        def __init__(self, T, LC, L1, L2, LZ, F, Y, out, y_first, turn=False):
            self.T, self.LC, self.L1, self.L2, self.LZ, self.F, self.Y, self.out = T, LC, L1, L2, LZ, F, Y, out
            self.cps = {}
            self.y_first, self.turn = y_first, turn

        def core(self, s, cp):
            cp.wait_recv()
            tiles = [(i, j, pre.at[i, j, :, pl.ds(0, 512)]) for i in range(2) for j in range(2)]
            loads = [local(self.LC.at[s, i, j], t) for i, j, t in tiles]
            for (i, j, t), cp in zip(tiles, loads):
                cp.wait()
                add_into(self.T.at[s, i, j], self.T.at[s, i, j], t)

        def first(self, s):
            if s in self.y_first:
                self.cps[s, 1] = w.send(self.T.at[s, :, 1], self.L1.at[s], "y")
            else:
                self.cps[s, 1] = w.send(self.T.at[s, 1], self.L1.at[s], "x")

        def second(self, s):
            self.cps[s, 1].wait_recv()
            for b in range(2):
                mine = self.T.at[s, b, 0] if s in self.y_first else self.T.at[s, 0, b]
                add_into(mine, mine, self.L1.at[s, b])
            if s in self.y_first:
                self.cps[s, 2] = w.send(self.T.at[s, 1, 0], self.L2.at[s], "x")
            else:
                self.cps[s, 2] = w.send(self.T.at[s, 0, 1], self.L2.at[s], "y")

        def third(self, s):
            self.cps[s, 2].wait_recv()
            mine = self.T.at[s, 0, 0]
            add_into(mine, mine, self.L2.at[s])
            if s:
                self.cps[s, 3] = w.send(mine, self.LZ.at[s - 1], lax.rem(z + s, 4))

        def fourth(self):
            for s in (1, 2, 3):
                self.cps[s, 3].wait_recv()

            def body(i, carry):
                at = pl.ds(pl.multiple_of(i * 32, 32), 32)
                tot = self.T[0, 0, 0, at, :].astype(F32)
                for s in range(3):
                    tot = tot + self.LZ[s, at, :].astype(F32)
                self.F[at, :] = tot.astype(BF16)
                return carry

            lax.fori_loop(0, 8, body, 0)
            self.cps["y"] = w.send(self.F, self.Y, "y")

        def last(self):
            self.cps["y"].wait_recv()
            if self.turn:
                for half, src in ((y, self.F), (1 - y, self.Y)):
                    self.out[:, pl.ds(pl.multiple_of(256 * half, 256), 256)] = src[...].astype(F32).T
            else:
                self.out[y] = self.F[...].astype(F32)
                self.out[1 - y] = self.Y[...].astype(F32)

    wo_g = Narrow(TO, LCO, L1O, L2O, LZO, FO, YO, GO, (1, 3), turn=True)
    wq_g = Narrow(TQ, LCQ, L1Q, L2Q, LZQ, FQ, YQ, GQ, (1,))
    qc = []
    dk_cp = {}

    def attend(s):
        wo_cp[s].wait()
        ga_scr[...] = nn(branch_ref[...], wbuf[0].reshape(2048, 512)).astype(BF16).astype(F32)
        if s < 3:
            wo_cp[s + 1] = local(WO.at[s + 1], wbuf.at[0])
        ot_cp[s].wait()
        attend_back(
            s, kv_ref, ga_scr, q_ref, bias_ref, cq_ref, sq_ref, ot_scr, lse_ref, dq_scr, d0, dr, ds_scr, p_scr,
            dk_scr, dv_scr,
        )
        if s < 3:
            ot_cp[s + 1] = local(OT.at[s + 1], ot_scr)
        for t in (1, 2, 3):
            cp = w.copy(dr.at[t - 1, s], ld.at[t - 1, s], lax.rem(z + t, 4), only=z + t >= 4)
            dk_cp[t, s] = cp
            pl.when(z + t >= 4)(cp.start)
        wq_cp[s].wait()

        def columns(i, carry):
            at = pl.ds(pl.multiple_of(i * 512, 512), 512)
            part = nt(dq_scr[s], wbuf[1, i // 2, i % 2].reshape(512, 512))
            if s:
                gn_scr[:, at] += part
            else:
                gn_scr[:, at] = part
            return carry

        lax.fori_loop(0, 4, columns, 0)
        if s < 3:
            wq_cp[s + 1] = local(WQ.at[s + 1], wbuf.at[1])
        w.sent(oc[s + 2] if s < 2 else qc[s - 2])
        grad_part(dq_scr[s], TQ.at[s], S.at[s % 2], every)
        qc.append(w.send(S.at[s % 2], LCQ.at[s], "c"))

    for cp in kept:
        cp.wait()
    wide_x(1, 0)
    wide_y(0, 0)
    wide_x(1, 1)
    for s in (1, 3, 0, 2):
        with mark("B_oc"):
            wo_g.core(s, oc[s])
        wo_g.first(s)
    for name in ("n", "q", "kv", "bias"):
        brought[name].wait()
    turned(n1_ref)
    with mark('B_att0'):
        attend(0)
    with mark("B_wy"):
        wide_y(0, 1)
    with mark('B_att1'):
        attend(1)
    with mark("B_qc"):
        wq_g.core(1, qc[1])
        wq_g.first(1)
    with mark('B_att2'):
        attend(2)
    with mark("B_o2"):
        for s in (1, 3):
            wo_g.second(s)
    with mark("B_wy"):
        wide_y(1, 0)
    with mark("B_qc"):
        wq_g.core(0, qc[0])
        wq_g.first(0)
    with mark('B_att3'):
        attend(3)
    wk_cp = {0: local(WKV.at[0], wk.at[0]), 1: local(WKV.at[1], wk.at[1])}
    with mark("B_qc"):
        for s in (3, 2):
            wq_g.core(s, qc[s])
            wq_g.first(s)
    with mark("B_o2"):
        for s in (0, 2):
            wo_g.second(s)
    with mark("B_o3"):
        for s in (1, 3):
            wo_g.third(s)
    for cp, late in out_cp:
        pl.when(late)(cp.start)
    with mark("B_wy"):
        wide_y(1, 1)
    with mark("B_q2"):
        wq_g.second(1)
    with mark("B_o3"):
        for s in (0, 2):
            wo_g.third(s)
    for s in range(4):
        dkv_scr[:, 128 * s : 128 * s + 128] = d0[s]
    for t in (1, 2, 3):

        with mark("B_dkr"):

            @pl.when(z < t)
            def _():
                for s in range(4):
                    dk_cp[t, (s + t) % 4].wait_recv()
                    dkv_scr[:, 128 * s : 128 * s + 128] += ld[t - 1, (s + t) % 4].astype(F32)

    for s in range(4):
        cols = slice(128 * s, 128 * s + 128)
        v = dkv_scr[:, cols]
        dkv = (v * ck_ref[...] - swap_halves(v) * sk_ref[...]).astype(BF16)
        wk_cp[s].wait()

        def columns(i, carry):
            at = pl.ds(pl.multiple_of(i * 512, 512), 512)
            gn_scr[:, at] += nt(dkv, wk[s % 2, i // 2, i % 2].reshape(512, 128))
            return carry

        lax.fori_loop(0, 4, columns, 0)
        if s < 2:
            wk_cp[s + 2] = local(WKV.at[s + 2], wk.at[s % 2])
        if s == 0:
            w.sent(qc[2])
        with mark("B_gk"):
            grad_part(dkv, TK.at[0], S.at[0], cols)
    kc = w.send(S.at[0], LCK.at[0], "c")

    gsum[0:1, :] = jnp.zeros((1, 2048), F32)
    for cp in tok_cp:
        cp.wait()

    def norm_back(i, carry):
        at = pl.ds(pl.multiple_of(i * 32, 32), 32)
        gn = gn_scr[at, :]
        x_in = obuf[at, :].astype(F32)
        inv = lax.rsqrt(jnp.mean(x_in * x_in, axis=1, keepdims=True) + NORM_EPS)
        unit = x_in * inv
        gsum[0:1, :] += jnp.sum(gn * unit, axis=0, keepdims=True)
        scaled = gn * gain1_ref[...]
        inside = jnp.mean(scaled * unit, axis=1, keepdims=True)
        back = (gmid_ref[at, :] + inv * (scaled - unit * inside)).astype(BF16)
        for m, to in enumerate(places):
            gtok_ref[at, pl.ds(to, 256)] = back[:, 256 * m : 256 * m + 256]
        return carry

    brought["g"].wait()
    with mark("B_nb"):
        lax.fori_loop(0, 8, norm_back, 0)
    gsum[1:2, :] = gain2t_ref[...]
    for hi in range(2):
        for mid in range(2):
            for lo in range(2):
                at = 4 * (c ^ mid) + 2 * (x ^ hi) + (y ^ lo)
                gains_ref[:, 256 * (4 * hi + 2 * mid + lo) : 256 * (4 * hi + 2 * mid + lo) + 256] = gsum[
                    :, pl.ds(pl.multiple_of(at * 256, 256), 256)
                ]
    steps = ["c", "x", "y", z + 1 - 2 * lax.rem(z, 2), lax.rem(z + 2, 4)]
    gain_cp = []

    def gain_next(n):
        gland[5 + n] = gains_ref[...]
        gain_cp.append(w.send(gland.at[5 + n], gland.at[n], steps[n]))

    def gain_add(n):
        gain_cp[n].wait_recv()
        gains_ref[...] += gland[n]

    gain_next(0)
    mid_cp = local(MID, gn_scr)
    wk_g = Narrow(TK, LCK, L1K, L2K, LZK, FK, YK, GKV, ())
    with mark("B_kc"):
        wk_g.core(0, kc)
    with mark("B_kf"):
        wk_g.first(0)
    with mark('B_g0'):
        gain_add(0)
    gain_next(1)
    with mark("B_q2"):
        for s in (0, 3, 2):
            wq_g.second(s)
    with mark("B_we"):
        wide_end(0, 0)
    with mark("B_k2"):
        wk_g.second(0)
    with mark("B_q3"):
        for s in (1, 0, 3, 2):
            wq_g.third(s)
    with mark('B_g1'):
        gain_add(1)
    gain_next(2)
    with mark("B_we"):
        wide_end(0, 1)
    with mark("B_k3"):
        wk_g.cps[0, 2].wait_recv()
    add_into(TK.at[0, 0, 0], TK.at[0, 0, 0], L2K.at[0])
    for s in (1, 2, 3):
        wk_g.cps[s, 3] = w.send(TK.at[0, 0, 0, :, pl.ds(128 * s, 128)], LZK.at[s - 1], lax.rem(z + s, 4))
    with mark('B_g2'):
        gain_add(2)
    gain_next(3)
    with mark("B_of"):
        wo_g.fourth()
    with mark("B_we"):
        wide_end(1, 0)
        wide_end(1, 1)
    with mark('B_g3'):
        gain_add(3)
    gain_next(4)
    with mark("B_ol"):
        wo_g.last()
    with mark("B_qf"):
        wq_g.fourth()
    with mark("B_k4"):
        for s in (1, 2, 3):
            wk_g.cps[s, 3].wait_recv()
    tot = TK[0, 0, 0, :, 0:128].astype(F32)
    for s in range(3):
        tot = tot + LZK[s].astype(F32)
    FK[...] = tot.astype(BF16)
    wk_g.cps["y"] = w.send(FK, YK, "y")
    with mark("B_out"):
        mid_cp.wait()
        for n in range(4):
            if n:
                out_cp[n - 1][0].wait_recv()
            local(OUT.at[0] if n == 0 else LOUT.at[n - 1], obuf).wait()
            add_into(gn_scr, gn_scr, obuf)

        def to_own(i, carry):
            at = pl.ds(pl.multiple_of(i * 32, 32), 32)
            for m, to in enumerate(places):
                bout_ref[at, pl.ds(to, 256)] = gn_scr[at, 256 * m : 256 * m + 256].astype(BF16)
            return carry

        lax.fori_loop(0, 8, to_own, 0)
    with mark('B_g4'):
        gain_add(4)
    with mark("B_last"):
        wq_g.last()
        wk_g.last()
    outs[-1].wait()
    w.finish()


def end_call(args):
    vmem = pl.BlockSpec(memory_space=pltpu.VMEM)
    hbm = pl.BlockSpec(memory_space=pl.ANY)
    outs = [
        ((256, 2048), BF16, vmem), ((2, 2048), F32, vmem),
        ((2, 256, 1408), F32, hbm), ((2, 256, 1408), F32, hbm),
        ((2, 256, 512), F32, vmem), ((512, 512), F32, vmem), ((2, 256, 128), F32, vmem), ((256, 2048), BF16, vmem),
        ((4, 2, 2, 256, 512), BF16, hbm), ((4, 2, 2, 256, 512), BF16, hbm), ((1, 2, 2, 256, 512), BF16, hbm),
        ((2, 2, 256, 1408), BF16, hbm), ((2, 2, 256, 1408), BF16, hbm), ((3, 256, 2048), BF16, hbm),
    ]
    scratch = [
        ((2, 2, 2, 256, 1408), BF16), ((4, 2, 2, 256, 512), BF16), ((4, 2, 2, 256, 512), BF16), ((1, 2, 2, 256, 512), BF16),
        ((2, 2, 2, 256, 512), BF16),
        ((4, 2, 256, 512), BF16), ((4, 2, 256, 512), BF16), ((1, 2, 256, 512), BF16),
        ((4, 256, 512), BF16), ((4, 256, 512), BF16), ((1, 256, 512), BF16),
        ((3, 256, 512), BF16), ((3, 256, 512), BF16), ((3, 256, 128), BF16),
        ((256, 512), BF16), ((256, 512), BF16), ((256, 128), BF16),
        ((256, 512), BF16), ((256, 512), BF16), ((256, 128), BF16),
        ((2, 2, 2, 2, 256, 512), BF16), ((2, 2, 2, 2, 256, 128), BF16), ((2048, 256), BF16), ((256, 512), F32),
        ((4, 256, 512), BF16), ((256, 512), F32), ((4, 256, 128), F32), ((3, 4, 256, 128), BF16), ((3, 4, 256, 128), BF16),
        ((1024, 512), BF16), ((1024, 512), BF16), ((1024, 128), F32), ((1024, 128), F32), ((256, 2048), F32),
        ((2, 2, 256, 1408), BF16), ((512, 256), F32), ((256, 1408), F32), ((2, 2048), F32), ((10, 2, 2048), F32), ((256, 2048), BF16),
        ((256, 2048), BF16), ((256, 2048), F32), ((256, 2048), BF16), ((4, 256, 512), BF16), ((4, 4, 256, 128), BF16),
        ((4, 256, 512), BF16), ((1024, 256), F32),
    ]
    return pl.pallas_call(
        end_kernel,
        out_shape=[jax.ShapeDtypeStruct(a, b) for a, b, _ in outs],
        in_specs=[hbm] * 16 + [vmem] * (len(args) - 16),
        out_specs=[o[2] for o in outs],
        scratch_shapes=[pltpu.VMEM(a, b) for a, b in scratch]
        + [pltpu.SemaphoreType.DMA((96,)), pltpu.SemaphoreType.DMA((96,)), pltpu.SemaphoreType.DMA((96,))],
        compiler_params=pltpu.CompilerParams(
            collective_id=1, has_side_effects=True, vmem_limit_bytes=67043328
        ),
        cost_estimate=pl.CostEstimate(flops=10**11, bytes_accessed=2 * 10**8, transcendentals=0),
    )(*args)


X_SWAP = [(0, 2), (1, 3), (2, 0), (3, 1)]
C_SWAP = [(0, 1), (1, 0), (2, 3), (3, 2)]
Y_SWAP = [(0, 1), (1, 0)]
PAIR = [(0, 1), (1, 0), (2, 3), (3, 2)]
MIDDLE = [(1, 2), (2, 1)]
OUTWARD = [(1, 0), (2, 3)]
INWARD = [(0, 1), (3, 2)]


def over_x(a):
    return lax.ppermute(a, "row", X_SWAP)


def over_c(a):
    return lax.ppermute(a, "row", C_SWAP)


def over_y(a):
    return lax.ppermute(a, "dp", Y_SWAP)


def over_z(a, pairs):
    return lax.ppermute(a, "col", pairs)


def from_slot(a, s):
    return over_z(a, [((i + s) % 4, i) for i in range(4)])


def to_slot(a, s):
    return over_z(a, [(i, (i + s) % 4) for i in range(4)])


def gather_col(own, inner):
    first = over_z(own, PAIR)
    mid = over_z(own, MIDDLE)
    third_in = over_z(first, MIDDLE)
    second = jnp.where(inner, mid, over_z(mid, OUTWARD))
    third = jnp.where(inner, third_in, over_z(third_in, OUTWARD))
    return own, first, second, third


def scatter_col(parts):
    own, first, second, third = parts
    t3 = (third + over_z(third.astype(BF16), INWARD)).astype(BF16)
    t2 = (second + over_z(second.astype(BF16), INWARD)).astype(BF16)
    t1 = (first + over_z(t3, MIDDLE)).astype(BF16)
    v = over_z(t2, MIDDLE)
    w = over_z(t1, PAIR)
    return own + v.astype(F32) + w.astype(F32)


def norm_forward(values, gain_vec):
    mean_sq = jnp.mean(values * values, axis=1, keepdims=True)
    inv_rms = lax.rsqrt(mean_sq + NORM_EPS)
    unit_rows = values * inv_rms
    return (unit_rows, inv_rms, (unit_rows * gain_vec).astype(BF16))


def norm_backward(grad_norm, unit_rows, inv_rms, gain_vec):
    scaled = grad_norm * gain_vec
    inner_sum = jnp.mean(scaled * unit_rows, axis=1, keepdims=True)
    return (inv_rms * (scaled - unit_rows * inner_sum), jnp.sum(grad_norm * unit_rows, axis=0))


def shards(
    tokens, gain_attn, w_query, w_keyval, w_output, gain_mlp, w_gate, w_up, w_down, out_grad,
    document_numbers, positions, *, rows,
):
    width = tokens.shape[1]
    fast = rows == 4
    z = lax.axis_index("col")
    r = lax.axis_index("row")
    y = lax.axis_index("dp")
    inner = (z == 1) | (z == 2)
    x, c = r // 2, r % 2
    blk = width // 8

    def permuted(a, abs_order):
        if not fast:
            return a
        axis = a.ndim - 1
        pieces = []
        for hi in range(2):
            for mid in range(2):
                for lo in range(2):
                    if abs_order:
                        at = 4 * (c ^ mid) + 2 * (x ^ hi) + (y ^ lo)
                    else:
                        at = 4 * (x ^ mid) + 2 * (c ^ hi) + (y ^ lo)
                    pieces.append(lax.dynamic_slice_in_dim(a, at * blk, blk, axis))
        return jnp.concatenate(pieces, axis=axis)

    to_rel = functools.partial(permuted, abs_order=False)
    to_abs = functools.partial(permuted, abs_order=True)

    def gather_rows(block):
        return lax.all_gather(block, "row", axis=0, tiled=True)

    def gather_slots(block):
        full = gather_rows(block)
        return [full] + [from_slot(full, s) for s in (1, 2, 3)]

    tok = to_rel(tokens)
    x_in = tok.astype(F32)
    gain_one = to_rel(gain_attn)
    gain_two = to_rel(gain_mlp)
    unit_one, inv_one, normed_one = norm_forward(x_in, gain_one)
    count = tokens.shape[0]
    my_pos = lax.dynamic_slice_in_dim(positions, z * count, count, 0)
    frequency = ROPE_BASE ** (-(jnp.arange(32, dtype=F32) * 2.0 / HEAD_SIZE))
    angles = my_pos.astype(F32)[:, None] * frequency[None, :]
    co, si = jnp.cos(angles), jnp.sin(angles)
    cos_q = jnp.concatenate([co, co, co, co], axis=1)
    sin_q = jnp.concatenate([-si, si, -si, si], axis=1)
    cos_k = jnp.concatenate([co, co, jnp.ones_like(co), jnp.ones_like(co)], axis=1)
    sin_k = jnp.concatenate([-si, si, jnp.zeros_like(si), jnp.zeros_like(si)], axis=1)
    my_seg = lax.dynamic_slice_in_dim(document_numbers, z * count, count, 0)
    key_seg = jnp.concatenate(
        [lax.dynamic_slice_in_dim(document_numbers, ((z + t) % 4) * count, count, 0) for t in range(4)]
    )
    lane = jnp.arange(count, dtype=jnp.int32)
    key_at = jnp.concatenate([((z + t) % 4) * count + lane for t in range(4)])
    allowed = (key_seg[:, None] == my_seg[None, :]) & (key_at[:, None] <= (z * count + lane)[None, :])
    bias = jnp.where(allowed, 0.0, MASK_FILL).astype(F32)

    def separate():
        full = lax.all_gather(w_keyval, "row", axis=0, tiled=True)
        wkv = jnp.concatenate([full] + [from_slot(full, s) for s in (1, 2, 3)], axis=1)
        wq = gather_slots(w_query)
        wo = gather_slots(w_output.T)
        wg, wu, wd = gather_rows(w_gate), gather_rows(w_up), gather_rows(w_down.T)
        kv = call(
            kv_kernel, [((4, count, 128), BF16)], (normed_one, wkv, cos_k, sin_k), 2 * count * width * 512
        )[0]
        kv_from = [kv]
        for t in (1, 2, 3):
            kv_from.append(over_z(kv, [((i + t) % 4, i) for i in range(4) if i + t >= 4]))
        kv_of = [[kv_from[t][(s - t) % 4] for t in range(4)] for s in range(4)]
        fwd = []
        for s in range(4):
            fwd.append(
                call(
                    fwd_kernel,
                    [((count, 512), BF16), ((count, 512), BF16), ((512, count), F32), ((8, count), F32)],
                    (normed_one, wq[s], *kv_of[s], bias, cos_q, sin_q),
                    2 * count * width * 512 + 8 * 4 * count * 1024 * 256,
                )
            )
        attn = [f[1] for f in fwd]
        mid = x_in + (nt(attn[0], wo[0]) + nt(attn[1], wo[1]) + nt(attn[2], wo[2]) + nt(attn[3], wo[3]))
        unit_two, inv_two, n2 = norm_forward(mid, gain_two)
        dys = gather_col(dy, inner)
        n2s = gather_col(n2, inner)
        outs, gns, acts, ggs, gus = [], [], [], [], []
        for s in range(4):
            gate_pre = nn(n2s[s], wg)
            up_pre = nn(n2s[s], wu)
            grad_act = nn(dys[s], wd)
            sig = jax.nn.sigmoid(gate_pre)
            silu = gate_pre * sig
            act = (silu * up_pre).astype(BF16)
            gg = (grad_act * up_pre * sig * (1.0 + gate_pre * (1.0 - sig))).astype(BF16)
            gu = (grad_act * silu).astype(BF16)
            outs.append(nt(act, wd))
            gns.append(nt(gg, wg) + nt(gu, wu))
            acts.append(act)
            ggs.append(gg)
            gus.append(gu)
        grad_norm_two = scatter_col(gns)
        flat = [jnp.concatenate(v, axis=0) for v in (n2s, dys, acts, ggs, gus)]
        mid_norm, gain2 = norm_backward(grad_norm_two, unit_two, inv_two, gain_two)
        gmid = dy.astype(F32) + mid_norm
        return wq, wo, wkv, kv_of, fwd, attn, mid, outs, flat, gmid, gmid.astype(BF16), gain2

    def together():
        def cut(block):
            return block.reshape(2, block.shape[0] // 2, block.shape[1])

        gain = jnp.stack([gain_attn, gain_mlp])
        WQ, WO, WKV, OUT, n1, q, ot, branch, _, LXM, _, TGU, gd, kv, o, lse, mid, gmid, gain2 = start_call(
            (
                gain, cut(w_query), cut(w_output.T), cut(w_keyval), bias, cos_q, sin_q, cos_k, sin_k, tokens, cut(w_gate),
                cut(w_up), cut(w_down.T), out_grad,
            )
        )
        gtok, gains, gg, gu, gq, go, gkv, bout = end_call(
            (
                WQ, WO, WKV, ot, TGU, LXM, OUT, mid, tokens, branch, gmid, n1, q, kv, o, bias, gain_one[None, :], gain2, lse,
                cos_q, sin_q, cos_k, sin_k,
            )
        )[:8]

        def joined(g):
            return g.reshape(2 * blk, g.shape[-1])

        return (
            bout, gtok, gains[0], joined(gq), joined(gkv), go, gains[1],
            joined(gg), joined(gu), joined(gd).T,
        )

    dy = to_rel(out_grad)
    if fast:
        return together()
    wq, wo, wkv, kv_of, fwd, attn, resid_mid, outs, flat, grad_mid, branch, gain_two_term = separate()
    n2_all, dy_all, act_all, gg_all, gu_all = flat
    block_out = (resid_mid + scatter_col([o.astype(F32) for o in outs])).astype(BF16)

    def ordered(lo, hi):
        return jnp.where(y == 0, jnp.concatenate([lo, hi], axis=0), jnp.concatenate([hi, lo], axis=0))

    def weight_grad(act_rel, g):
        half = width // 2
        if not fast:
            full = lax.psum_scatter(tn(act_rel, g).astype(BF16), "row", scatter_dimension=0, tiled=True)
            return lax.psum(full, "dp").astype(F32)
        got = over_c(tn(act_rel[:, half:], g).astype(BF16))
        t = tn(act_rel[:, :half], g) + got.astype(F32)
        q = half // 2
        got = over_x(t[q:].astype(BF16))
        t = (t[:q] + got.astype(F32)).astype(BF16)
        got = over_y(t).astype(F32)
        t = t.astype(F32)
        return ordered(t[: q // 2] + got[q // 2 :], t[q // 2 :] + got[: q // 2])

    def weight_grad_slots(act_rel, gs):
        half = width // 2
        if not fast:
            tot = 0.0
            for s in range(4):
                full = lax.psum_scatter(
                    tn(act_rel, gs[s]).astype(BF16), "row", scatter_dimension=0, tiled=True
                )
                tot = tot + (full if s == 0 else to_slot(full, s)).astype(F32)
            return lax.psum(tot.astype(BF16), "dp").astype(F32)
        tot = 0.0
        for s in range(4):
            got = over_c(tn(act_rel[:, half:], gs[s]).astype(BF16))
            t = tn(act_rel[:, :half], gs[s]) + got.astype(F32)
            b = blk
            t00, t01, t10, t11 = t[:b], t[b : 2 * b], t[2 * b : 3 * b], t[3 * b :]
            if s % 2:
                got = over_y(jnp.concatenate([t01, t11], axis=0).astype(BF16)).astype(F32)
                u0 = t00 + got[:b]
                u1 = t10 + got[b:]
                u = u0 + over_x(u1.astype(BF16)).astype(F32)
            else:
                got = over_x(jnp.concatenate([t10, t11], axis=0).astype(BF16)).astype(F32)
                u0 = t00 + got[:b]
                u1 = t01 + got[b:]
                u = u0 + over_y(u1.astype(BF16)).astype(F32)
            u = u.astype(BF16)
            tot = tot + (u if s == 0 else to_slot(u, s)).astype(F32)
        tot = tot.astype(BF16)
        return ordered(tot.astype(F32), over_y(tot).astype(F32))

    g_down = weight_grad(dy_all, act_all)
    g_gate = weight_grad(n2_all, gg_all)
    g_up = weight_grad(n2_all, gu_all)

    bwd = []
    for s in range(4):
        bwd.append(
            call(
                bwd_kernel,
                [((count, 512), BF16), ((count, 128), F32), ((3, count, 128), BF16)],
                (branch, wo[s], fwd[s][0], *kv_of[s], bias, cos_q, sin_q, fwd[s][2], fwd[s][3]),
                2 * count * width * 512 + 8 * 10 * count * 1024 * 256,
                scratch=(
                    pltpu.VMEM((1024, 512), BF16),
                    pltpu.VMEM((1024, 512), BF16),
                    pltpu.VMEM((1024, 128), F32),
                    pltpu.VMEM((1024, 128), F32),
                ),
            )
        )
    got = []
    for t in (1, 2, 3):
        out = jnp.stack([bwd[s][2][t - 1] for s in range(4)])
        got.append(over_z(out, [(i, (i + t) % 4) for i in range(4) if i + t >= 4]))
    dkv = call(
        dkv_kernel,
        [((4, count, 128), BF16)],
        (*[bwd[s][1] for s in range(4)], *got, cos_k, sin_k),
        count * 512 * 8,
    )[0]
    dkv = jnp.concatenate([dkv[s] for s in range(4)], axis=1)
    dq = [bwd[s][0] for s in range(4)]
    grad_norm_one = nt(dq[0], wq[0]) + nt(dq[1], wq[1]) + nt(dq[2], wq[2]) + nt(dq[3], wq[3])
    grad_norm_one = grad_norm_one + nt(dkv, wkv)
    in_norm, gain_one_term = norm_backward(grad_norm_one, unit_one, inv_one, gain_one)
    grad_tokens = (grad_mid + in_norm).astype(BF16)
    g_output = weight_grad_slots(branch, attn)
    g_query = weight_grad_slots(normed_one, dq)
    g_keyval = weight_grad_slots(normed_one, [dkv[:, 128 * s : 128 * s + 128] for s in range(4)])

    def total(v):
        if not fast:
            return lax.psum(v, ("dp", "row", "col"))
        v = v + over_c(v)
        v = v + over_x(v)
        v = v + over_y(v)
        v = v + over_z(v, PAIR)
        return v + over_z(v, [(0, 2), (1, 3), (2, 0), (3, 1)])

    return (
        to_abs(block_out),
        to_abs(grad_tokens),
        total(to_abs(gain_one_term)),
        g_query,
        g_keyval,
        g_output.T,
        total(to_abs(gain_two_term)),
        g_gate,
        g_up,
        g_down.T,
    )


def solution(mesh):
    spec = P(("dp", "row", "col"), None)
    down = P("row", "col")
    across = P("col", "row")
    seq = P(("dp", "row"))
    return jax.shard_map(
        functools.partial(shards, rows=mesh.shape["row"]),
        mesh=mesh,
        in_specs=(spec, P(), down, down, across, P(), down, down, across, spec, seq, seq),
        out_specs=(spec, spec, P(), down, down, across, P(), down, down, across),
        check_vma=False,
    )
```

```python
import functools
import math

import jax
import jax.numpy as jnp
from jax import lax
from jax.experimental import pallas as pl
from jax.experimental.pallas import tpu as pltpu
from jax.sharding import PartitionSpec as P

HEAD_SIZE = 64
SEQUENCE_LENGTH = 1024
NORM_EPS = 1e-05
ROPE_BASE = 10000.0
MASK_FILL = -1e30
BF16 = jnp.bfloat16
F32 = jnp.float32


def nn(a, b):
    return lax.dot_general(a, b, (((1,), (0,)), ((), ())), preferred_element_type=F32)


def nt(a, b):
    return lax.dot_general(a, b, (((1,), (1,)), ((), ())), preferred_element_type=F32)


def tn(a, b):
    return lax.dot_general(a, b, (((0,), (0,)), ((), ())), preferred_element_type=F32)


def swap_halves(v):
    lane = lax.broadcasted_iota(jnp.int32, v.shape, 1)
    return jnp.where((lane % 64) < 32, pltpu.roll(v, 96, 1), pltpu.roll(v, 32, 1))


def kv_kernel(n_ref, w_ref, c_ref, s_ref, o_ref):
    kv = nn(n_ref[...], w_ref[...])
    for s in range(4):
        v = kv[:, 128 * s : 128 * s + 128]
        o_ref[s] = (v * c_ref[...] + swap_halves(v) * s_ref[...]).astype(BF16)


def load_kv(kv_refs):
    return jnp.concatenate([r[...].astype(F32) for r in kv_refs], axis=0)


def fwd_kernel(n_ref, w_ref, k0, k1, k2, k3, bias_ref, c_ref, s_ref, q_ref, o_ref, ot_ref, lse_ref):
    q = nn(n_ref[...], w_ref[...])
    kv = load_kv((k0, k1, k2, k3))
    k_low = kv[:, :64].astype(BF16)
    v_t = kv.T[64:].astype(BF16)
    for p in range(4):
        cols = slice(128 * p, 128 * p + 128)
        v = q[:, cols]
        rot = (v * c_ref[...] + swap_halves(v) * s_ref[...]) * 0.125
        rot = rot.astype(BF16)
        q_ref[:, cols] = rot
        q_t = rot.astype(F32).T.astype(BF16)
        outs = []
        for e in range(2):
            s_t = nn(k_low, q_t[64 * e : 64 * e + 64]) + bias_ref[...]
            top = jnp.max(s_t, axis=0, keepdims=True)
            ex = jnp.exp(s_t - top)
            tot = jnp.sum(ex, axis=0, keepdims=True)
            outs.append(nn(v_t, ex.astype(BF16)) * (1.0 / tot))
            lse_ref[pl.ds(2 * p + e, 1), :] = top + jnp.log(tot)
        o_t = jnp.concatenate(outs, axis=0)
        ot_ref[cols, :] = o_t
        o_ref[:, cols] = o_t.T.astype(BF16)


def bwd_kernel(
    b_ref, w_ref, q_ref, k0, k1, k2, k3, bias_ref, c_ref, s_ref, ot_ref, lse_ref,
    dq_ref, d0_ref, dr_ref, ds_scr, p_scr, dk_scr, dv_scr,
):
    ga = nn(b_ref[...], w_ref[...]).astype(BF16).astype(F32)
    kv = load_kv((k0, k1, k2, k3))
    k_low = kv[:, :64].astype(BF16)
    v_low = pltpu.roll(kv, 64, 1)[:, :64].astype(BF16)
    k_t = kv.T[:64].astype(BF16)
    lane = lax.broadcasted_iota(jnp.int32, (256, 128), 1)
    for p in range(4):
        cols = slice(128 * p, 128 * p + 128)
        qp = q_ref[:, cols].astype(F32)
        gp = ga[:, cols]
        q_t = qp.T.astype(BF16)
        g_tf = gp.T
        g_t = g_tf.astype(BF16)
        prod = g_tf * ot_ref[cols, :]
        dq_t = []
        for e in range(2):
            half = slice(64 * e, 64 * e + 64)
            s_t = nn(k_low, q_t[half]) + bias_ref[...]
            pr = jnp.exp(s_t - lse_ref[pl.ds(2 * p + e, 1), :])
            dp = nn(v_low, g_t[half])
            inner = jnp.sum(prod[half], axis=0, keepdims=True)
            ds = (pr * (dp - inner)).astype(BF16)
            ds_scr[:, 256 * e : 256 * e + 256] = ds
            p_scr[:, 256 * e : 256 * e + 256] = pr.astype(BF16)
            dq_t.append(nn(k_t, ds))
        qbd = jnp.concatenate(
            [jnp.where(lane < 64, qp, 0.0), jnp.where(lane < 64, 0.0, qp)], axis=0
        ).astype(BF16)
        gbd = jnp.concatenate(
            [jnp.where(lane < 64, gp, 0.0), jnp.where(lane < 64, 0.0, gp)], axis=0
        ).astype(BF16)
        dk = nn(ds_scr[...], qbd)
        dv = nn(p_scr[...], gbd)
        if p == 0:
            dk_scr[...] = dk
            dv_scr[...] = dv
        else:
            dk_scr[...] += dk
            dv_scr[...] += dv
        dqp = jnp.concatenate(dq_t, axis=0).T * 0.125
        dq_ref[:, cols] = (dqp * c_ref[...] - swap_halves(dqp) * s_ref[...]).astype(BF16)
    dk = dk_scr[...]
    dv = dv_scr[...]
    lane = lax.broadcasted_iota(jnp.int32, dk.shape, 1)
    both = jnp.where(lane < 64, dk + pltpu.roll(dk, 64, 1), dv + pltpu.roll(dv, 64, 1))
    d0_ref[...] = both[:256]
    for t in range(3):
        dr_ref[t] = both[256 * (t + 1) : 256 * (t + 2)].astype(BF16)


def dkv_kernel(a0, a1, a2, a3, r1, r2, r3, c_ref, s_ref, o_ref):
    own = (a0, a1, a2, a3)
    got = (r1, r2, r3)
    for s in range(4):
        v = own[s][...]
        for t in range(1, 4):
            v = v + got[t - 1][(s + t) % 4].astype(F32)
        o_ref[s] = (v * c_ref[...] - swap_halves(v) * s_ref[...]).astype(BF16)


def call(body, outs, args, flops, scratch=(), vmem=48 << 20):
    spec = pl.BlockSpec(memory_space=pltpu.VMEM)
    shapes = [jax.ShapeDtypeStruct(s, d) for s, d in outs]
    nbytes = sum(a.size * a.dtype.itemsize for a in args) + sum(
        math.prod(s) * jnp.dtype(d).itemsize for s, d in outs
    )
    return pl.pallas_call(
        body,
        out_shape=shapes,
        in_specs=[spec] * len(args),
        out_specs=[spec] * len(outs),
        scratch_shapes=list(scratch),
        compiler_params=pltpu.CompilerParams(vmem_limit_bytes=vmem),
        cost_estimate=pl.CostEstimate(flops=flops, bytes_accessed=nbytes, transcendentals=0),
    )(*args)


MESH = pl.DeviceIdType.MESH


def mark(name):
    return jax.named_scope(name)


def relative(x, c, y):
    at = []
    for k in range(2):
        for i in range(2):
            for j in range(2):
                at.append(pl.multiple_of(256 * (4 * (x ^ i) + 2 * (c ^ k) + (y ^ j)), 256))
    return at


class Wire:
    def __init__(self, send_sem, recv_sem, z):
        self.send_sem, self.recv_sem, self.z = send_sem, recv_sem, z
        self.count = 0
        self.made = []

    def to(self, where):
        r = lax.axis_index("row")
        if where == "x":
            return {"row": lax.rem(r + 2, 4)}
        if where == "c":
            return {"row": r + 1 - 2 * lax.rem(r, 2)}
        if where == "y":
            return {"dp": 1 - lax.axis_index("dp")}
        return {"col": where}

    def copy(self, src, dst, where, only=None, recv=None):
        k = self.count
        self.count += 1
        cp = pltpu.make_async_remote_copy(
            src_ref=src, dst_ref=dst, send_sem=self.send_sem.at[k], recv_sem=self.recv_sem.at[k if recv is None else recv],
            device_id=self.to(where), device_id_type=MESH,
        )
        self.made.append((cp, only))
        return cp

    def sent(self, cp):
        self.made = [m for m in self.made if m[0] is not cp]
        cp.wait_send()

    def send(self, src, dst, where):
        cp = self.copy(src, dst, where)
        cp.start()
        return cp

    def finish(self):
        for cp, only in self.made:
            if only is None:
                cp.wait_send()
            else:
                pl.when(only)(cp.wait_send)


def greet(z):
    barrier = pltpu.get_barrier_semaphore()
    wire = Wire(None, None, z)
    for where in ("x", "c", "y"):
        pl.semaphore_signal(barrier, inc=1, device_id=wire.to(where), device_id_type=MESH)
    for d in (1, 2, 3):
        pl.semaphore_signal(barrier, inc=1, device_id={"col": lax.rem(z + d, 4)}, device_id_type=MESH)
    pl.semaphore_wait(barrier, 6)


def attend_slot(w_ref, n_ref, kv_scr, s, bias_ref, c_ref, s_ref, q_ref, o_ref, ot_ref, lse_ref, q_scr):
    q_scr[...] = nn(n_ref[...], w_ref[...])
    kv = jnp.concatenate([kv_scr[t, (s - t) % 4].astype(F32) for t in range(4)], axis=0)
    k_low = kv[:, :64].astype(BF16)
    v_t = kv.T[64:].astype(BF16)

    def pair(p, carry):
        at = pl.multiple_of(p * 128, 128)
        cols = pl.ds(at, 128)
        v = q_scr[:, cols]
        rot = ((v * c_ref[...] + swap_halves(v) * s_ref[...]) * 0.125).astype(BF16)
        q_ref[:, cols] = rot
        q_t = rot.astype(F32).T.astype(BF16)
        outs = []
        for e in range(2):
            s_t = nn(k_low, q_t[64 * e : 64 * e + 64]) + bias_ref[...]
            top = jnp.max(s_t, axis=0, keepdims=True)
            ex = jnp.exp(s_t - top)
            tot = jnp.sum(ex, axis=0, keepdims=True)
            outs.append(nn(v_t, ex.astype(BF16)) * (1.0 / tot))
            lse_ref[s, pl.ds(2 * p + e, 1), :] = top + jnp.log(tot)
        o_t = jnp.concatenate(outs, axis=0)
        ot_ref[cols, :] = o_t
        o_ref[s, :, cols] = o_t.T.astype(BF16)
        return carry

    lax.fori_loop(0, 4, pair, 0)


def start_kernel(
    gain1_ref, gain2_ref, wq_ref, wo_ref, wkv_ref, bias_ref, cq_ref, sq_ref, ck_ref, sk_ref, tok_ref, wg_ref, wu_ref, wd_ref, dy_ref,
    WQ, WO, WKV, OUT, NONE, QS, OT, BRANCH, LCM, LXM, LYM, TGU, GDOWN, kv_out, o_ref, lse_ref, mid_ref, gmid_ref, gain2_out,
    wm, gn_scr, N2, DY, wbuf, wkv_scr, q_scr, q_stage, ot_stage, gate_scr, up_scr, grad_scr, hid, out_stage, pre,
    gains, send_sem, recv_sem, loc_sem,
):
    own_scr = gmid_ref
    kv_scr = kv_out
    r = lax.axis_index("row")
    x, c = r // 2, lax.rem(r, 2)
    z = lax.axis_index("col")
    y = lax.axis_index("dp")
    inner = (z == 1) | (z == 2)
    outer = jnp.logical_not(inner)
    w = Wire(send_sem, recv_sem, z)
    locs = []

    def local(src, dst):
        cp = pltpu.make_async_copy(src, dst, loc_sem.at[len(locs)])
        cp.start()
        locs.append(cp)
        return cp

    greet(z)
    blocks = {"kv": (wkv_ref, WKV), "q": (wq_ref, WQ), "o": (wo_ref, WO)}
    ev = {}

    def start_z(name):
        ref, full = blocks[name]
        for s in (1, 2, 3):
            d = 4 - s
            ev[name, s, "z"] = w.send(ref.at[y], full.at[s, 0, 0, 0], lax.rem(z + d, 4))

    def start_own(name):
        ref, full = blocks[name]
        ev[name, 0, "x"] = w.send(ref.at[y], full.at[0, 0, 1, 0], "x")
        ev[name, 0, "own"] = [local(ref.at[y], full.at[0, 0, 0, 0]), local(ref.at[1 - y], full.at[0, 0, 0, 1])]
        ev[name, 0, "c0"] = [
            w.send(ref.at[y], full.at[0, 1, 0, 0], "c"), w.send(ref.at[1 - y], full.at[0, 1, 0, 1], "c")
        ]

    def own_second(name):
        full = blocks[name][1]
        ev[name, 0, "x"].wait_recv()
        ev[name, 0, "y"] = w.send(full.at[0, 0, 1, 0], full.at[0, 0, 1, 1], "y")

    def own_core(name):
        full = blocks[name][1]
        ev[name, 0, "y"].wait_recv()
        ev[name, 0, "c"] = w.send(full.at[0, 0, 1], full.at[0, 1, 1], "c")

    def first(name, s):
        full = blocks[name][1]
        ev[name, s, "z"].wait_recv()
        if (s % 2 == 1) != (name == "o"):
            ev[name, s, 1] = w.send(full.at[s, 0, 0, 0], full.at[s, 0, 0, 1], "y")
        else:
            ev[name, s, 1] = w.send(full.at[s, 0, 0, 0], full.at[s, 0, 1, 0], "x")

    def second(name, s):
        full = blocks[name][1]
        ev[name, s, 1].wait_recv()
        if (s % 2 == 1) != (name == "o"):
            ev[name, s, 2] = w.send(full.at[s, 0, 0], full.at[s, 0, 1], "x")
        else:
            ev[name, s, 2] = w.send(full.at[s, 0, :, 0], full.at[s, 0, :, 1], "y")

    def core(name, s):
        full = blocks[name][1]
        ev[name, s, 2].wait_recv()
        ev[name, s, "c"] = w.send(full.at[s, 0], full.at[s, 1], "c")

    def whole(name, s):
        ev[name, s, "c"].wait_recv()
        if s == 0:
            for cp in ev[name, 0, "c0"]:
                cp.wait_recv()
            for cp in ev[name, 0, "own"]:
                cp.wait()

    mats = {"g": (wg_ref, wm.at[0]), "u": (wu_ref, wm.at[1]), "d": (wd_ref, wm.at[2])}

    def mat_start(name):
        ref, full = mats[name]
        ev[name, "x"] = w.send(ref.at[y], full.at[0, 1, 0], "x")
        ev[name, "own"] = [local(ref.at[y], full.at[0, 0, 0]), local(ref.at[1 - y], full.at[0, 0, 1])]
        ev[name, "c0"] = [
            w.send(ref.at[y], full.at[1, 0, 0], "c"), w.send(ref.at[1 - y], full.at[1, 0, 1], "c")
        ]

    def mat_second(name):
        full = mats[name][1]
        ev[name, "x"].wait_recv()
        ev[name, "y"] = w.send(full.at[0, 1, 0], full.at[0, 1, 1], "y")

    def mat_core(name):
        full = mats[name][1]
        ev[name, "y"].wait_recv()
        ev[name, "c"] = w.send(full.at[0, 1], full.at[1, 1], "c")

    def mat_whole(name):
        ev[name, "c"].wait_recv()
        for cp in ev[name, "c0"]:
            cp.wait_recv()
        for cp in ev[name, "own"]:
            cp.wait()

    buddy = z + 1 - 2 * lax.rem(z, 2)
    middle = lax.rem(7 - z, 4)

    def some(cond, cp):
        pl.when(cond)(cp.start)
        return cp

    def rows_start(full):
        f = w.send(full.at[0], full.at[1], buddy)
        m = some(inner, w.copy(full.at[0], full.at[2], middle, only=inner))
        return [f, m]

    def rows_first(full, c):
        c[0].wait_recv()
        c.append(some(inner, w.copy(full.at[1], full.at[3], middle, only=inner)))

    def rows_second(full, c):
        pl.when(inner)(c[1].wait_recv)
        c.append(some(inner, w.copy(full.at[2], full.at[2], buddy, only=inner)))

    def rows_third(full, c):
        pl.when(inner)(c[2].wait_recv)
        c.append(some(inner, w.copy(full.at[3], full.at[3], buddy, only=inner)))

    def rows_have_second(c):
        pl.when(outer)(c[3].wait_recv)

    def rows_have_third(c):
        pl.when(outer)(c[4].wait_recv)

    tok_rel, n1_rel = gn_scr.at[0], gn_scr.at[1]
    moved = []
    for m, at in enumerate(relative(x, c, y)):
        to = pl.ds(256 * m, 256)
        moved.append(local(tok_ref.at[:, pl.ds(at, 256)], tok_rel.at[:, to]))
        moved.append(local(dy_ref.at[:, pl.ds(at, 256)], DY.at[0, :, to]))
        gains[0:1, to] = gain1_ref[:, pl.ds(at, 256)]
        gains[1:2, to] = gain2_ref[:, pl.ds(at, 256)]
    start_z("kv")
    start_own("kv")
    start_z("q")
    start_own("q")

    def norm_one(i, carry):
        at = pl.ds(pl.multiple_of(i * 32, 32), 32)
        x_in = tok_rel[at, :].astype(F32)
        inv = lax.rsqrt(jnp.mean(x_in * x_in, axis=1, keepdims=True) + NORM_EPS)
        n1_rel[at, :] = (x_in * inv * gains[0:1, :]).astype(BF16)
        mid_ref[at, :] = x_in
        return carry

    for cp in moved:
        cp.wait()
    with mark("A_norm1"):
        lax.fori_loop(0, 8, norm_one, 0)
    n1_out = local(n1_rel, NONE)
    for t in (1, 2, 3):

        @pl.when(z + t < 4)
        def _():
            kv_scr[t] = jnp.zeros_like(kv_scr[t])

    with mark("A_kv1"):
        own_second("kv")
        for s in (1, 2, 3):
            first("kv", s)
        own_second("q")
    with mark("A_kv2"):
        for s in (2, 1, 3):
            second("kv", s)
        own_core("kv")
    with mark("A_q1"):
        for s in (1, 2, 3):
            first("q", s)
    with mark("A_kv3"):
        for s in (2, 1, 3):
            core("kv", s)
    own_core("q")
    with mark("A_q2"):
        for s in (2, 1, 3):
            second("q", s)
    start_own("o")
    mat_start("g")
    got = []
    with mark("A_kvw"):
        for s in range(4):
            whole("kv", s)
            if s < 2:
                got.append(local(WKV.at[s], wkv_scr.at[s]))
        for s in range(4):
            got[s].wait()
            kv = nn(n1_rel[...], wkv_scr[s % 2].reshape(2048, 128))
            if s < 2:
                got.append(local(WKV.at[s + 2], wkv_scr.at[s]))
            kv_scr[0, s] = (kv * ck_ref[...] + swap_halves(kv) * sk_ref[...]).astype(BF16)
    kv_cp = {}
    for s in (0, 2, 1, 3):
        for d in (1, 2, 3):
            u = (s + d) % 4
            cp = w.copy(kv_scr.at[0, u], kv_scr.at[4 - d, u], lax.rem(z + d, 4), only=z + d < 4)
            kv_cp[4 - d, s] = cp
            pl.when(z + d < 4)(cp.start)
    cps, kept = {}, []
    with mark("A_q0w"):
        whole("q", 0)
    cps[0] = local(WQ.at[0], wbuf.at[0])
    start_z("o")
    dyc = rows_start(DY)
    def attend(s, b):
        cps[s].wait()
        for cp in kept:
            cp.wait()
        kept.clear()
        with mark("A_kvr"):
            for t in (1, 2, 3):
                pl.when(z + t >= 4)(kv_cp[t, s].wait_recv)
        with mark(f"A_att{s}"):
            attend_slot(
                wbuf.at[b].reshape(2048, 512), n1_rel, kv_scr, s, bias_ref, cq_ref, sq_ref, q_stage, o_ref, ot_stage,
                lse_ref, q_scr,
            )
        kept.append(local(q_stage, QS.at[s]))
        kept.append(local(ot_stage, OT.at[s]))

    attend(0, 0)
    with mark("A_q3"):
        core("q", 2)
        whole("q", 2)
    cps[2] = local(WQ.at[2], wbuf.at[1])
    attend(2, 1)
    with mark("A_o1"):
        own_second("o")
        for s in (1, 2, 3):
            first("o", s)
    mat_start("u")
    with mark("A_q4"):
        core("q", 1)
        core("q", 3)
        whole("q", 1)
    cps[1] = local(WQ.at[1], wbuf.at[0])
    whole("q", 3)
    cps[3] = local(WQ.at[3], wbuf.at[1])
    with mark("A_m1"):
        mat_second("g")
    with mark("A_dy1"):
        rows_first(DY, dyc)
    attend(1, 0)
    with mark("A_o2"):
        own_core("o")
        for s in (2, 1, 3):
            second("o", s)
    mat_start("d")
    with mark("A_dy2"):
        rows_second(DY, dyc)
    oc = {}
    attend(3, 1)
    with mark("A_m2"):
        mat_second("u")
    with mark("A_dy3"):
        rows_third(DY, dyc)
    with mark("A_o3"):
        for s in (2, 1, 3):
            core("o", s)
    for k, s in enumerate((0, 2, 1, 3)):
        with mark("A_oproj"):
            if s == 0:
                whole("o", 0)
                oc[0] = local(WO.at[0], wbuf.at[0])
            oc[s].wait()
            if k < 3:
                nxt = (2, 1, 3)[k]
                whole("o", nxt)
                oc[nxt] = local(WO.at[nxt], wbuf.at[(k + 1) % 2])

            def columns(i, carry):
                at = pl.ds(pl.multiple_of(i * 512, 512), 512)
                mid_ref[:, at] += nt(o_ref[s], wbuf[k % 2, i // 2, i % 2].reshape(512, 512))
                return carry

            lax.fori_loop(0, 4, columns, 0)

    def norm_two(i, carry):
        at = pl.ds(pl.multiple_of(i * 32, 32), 32)
        mid = mid_ref[at, :]
        inv = lax.rsqrt(jnp.mean(mid * mid, axis=1, keepdims=True) + NORM_EPS)
        N2[0, at, :] = (mid * inv * gains[1:2, :]).astype(BF16)
        return carry

    lax.fori_loop(0, 8, norm_two, 0)
    n2c = rows_start(N2)
    with mark("A_m2"):
        mat_core("g")
    with mark("A_m3"):
        mat_second("d")
        mat_core("u")
    with mark("A_n1"):
        rows_first(N2, n2c)
        rows_second(N2, n2c)
    with mark("A_m4"):
        mat_core("d")
        for name in mats:
            mat_whole(name)
    n1_out.wait()
    for cp in kept:
        cp.wait()
    def slot(a, stored):
        dy_a = DY[a]
        n2_a = N2[a]
        gate_scr[...] = nn(n2_a, wm[0].reshape(2048, 1408))
        up_scr[...] = nn(n2_a, wm[1].reshape(2048, 1408))
        grad_scr[...] = nn(dy_a, wm[2].reshape(2048, 1408))
        for cp in stored:
            cp.wait()

        def rows(i, carry):
            at = pl.ds(pl.multiple_of(i * 32, 32), 32)
            gate = gate_scr[at, :]
            up = up_scr[at, :]
            ga = grad_scr[at, :]
            sig = 1.0 / (1.0 + jnp.exp(-gate))
            silu = gate * sig
            hid[2, a, at, :] = (silu * up).astype(BF16)
            hid[0, a, at, :] = (ga * up * sig * (1.0 + gate * (1.0 - sig))).astype(BF16)
            hid[1, a, at, :] = (ga * silu).astype(BF16)
            return carry

        lax.fori_loop(0, 8, rows, 0)

        def columns(c, carry):
            at = pl.ds(pl.multiple_of(c * 512, 512), 512)
            k, i = c // 2, c % 2
            out_stage[:, at] = nt(hid[2, a], wm[2, k, i].reshape(512, 1408)).astype(BF16)
            gn = nt(hid[0, a], wm[0, k, i].reshape(512, 1408)) + nt(hid[1, a], wm[1, k, i].reshape(512, 1408))
            if a == 0:
                own_scr[:, at] = gn
            else:
                gn_scr[a - 1, :, at] = gn.astype(BF16)
            return carry

        lax.fori_loop(0, 4, columns, 0)
        return [local(out_stage, OUT.at[a])]

    def send_sum(a, n, where):
        for i in range(2):
            for j in range(2):
                piece = gn_scr.at[a - 1, :, pl.ds(1024 * i + 512 * j, 512)]
                w.copy(piece, wbuf.at[n // 2, n % 2, i, j], where, recv=112 + 4 * n + 2 * i + j).start()

    def sum_arrived(n):
        for i in range(2):
            for j in range(2):
                pltpu.make_async_remote_copy(
                    src_ref=gn_scr.at[0, :, pl.ds(0, 512)], dst_ref=wbuf.at[n // 2, n % 2, i, j],
                    send_sem=send_sem.at[0], recv_sem=recv_sem.at[112 + 4 * n + 2 * i + j],
                    device_id=w.to("c"), device_id_type=MESH,
                ).wait_recv()

    place = 1 + jnp.where(inner, 0, 1)
    second_at = jnp.where(z < 2, 2, 1)
    third_at = jnp.where(z < 2, 3, 0)
    with mark("A_slot0"):
        stored = slot(0, [])
    with mark("A_w1"):
        rows_have_second(dyc)
        rows_have_third(dyc)
        rows_third(N2, n2c)
    with mark("A_slot1"):
        stored = slot(1, stored)
    send_sum(1, 0, buddy)
    with mark("A_w2"):
        rows_have_second(n2c)
    with mark("A_slot2"):
        stored = slot(2, stored)
    send_sum(2, place, second_at)
    with mark("A_w3"):
        rows_have_third(n2c)
    with mark("A_slot3"):
        stored = slot(3, stored)
    send_sum(3, place, third_at)

    def add_rows(into, n):
        def body(i, carry):
            at = pl.ds(pl.multiple_of(i * 32, 32), 32)
            for h in range(2):
                for j in range(2):
                    cols = slice(1024 * h + 512 * j, 1024 * h + 512 * j + 512)
                    other = wbuf[n // 2, n % 2, h, j, at, :].astype(F32)
                    into[at, cols] = (into[at, cols].astype(F32) + other).astype(into.dtype)
            return carry

        lax.fori_loop(0, 8, body, 0)

    wide = {2: DY, 0: N2, 1: N2}
    mc, xs, ys = {}, {}, {}

    def wide_part(m, k):
        def tile(n, carry):
            cols = pl.ds(pl.multiple_of(1024 * k + 256 * n, 256), 256)
            src = jnp.concatenate([wide[m][a, :, cols] for a in range(4)], axis=0)
            wm[m, k, n // 2, n % 2] = tn(src, hid[m].reshape(1024, 1408)).astype(BF16)
            return carry

        with mark("A_dw"):
            lax.fori_loop(0, 4, tile, 0)
        if k:
            mc[m] = w.send(wm.at[m, 1], LCM.at[m], "c")

    turn = [0]

    def fetch(src):
        b = turn[0] % 2
        turn[0] += 1
        return pre.at[b], local(src, pre.at[b])

    def wide_core(m):
        with mark("A_wc"):
            mc[m].wait_recv()
            order = [(1, 0), (1, 1), (0, 0), (0, 1)]
            nxt = fetch(LCM.at[m, 1, 0])
            for n, (i, j) in enumerate(order):
                buf, cp = nxt
                if n < 3:
                    nxt = fetch(LCM.at[m, order[n + 1][0], order[n + 1][1]])
                cp.wait()
                add_into(wm.at[m, 0, i, j], wm.at[m, 0, i, j], buf)

    def wide_x(m, j):
        xs[m, j] = w.send(wm.at[m, 0, 1, j], LXM.at[m, j], "x")

    def wide_y(m, j):
        with mark("A_wy"):
            xs[m, j].wait_recv()
            buf, cp = fetch(LXM.at[m, j])
            cp.wait()
            add_into(wm.at[m, 0, 0, j], wm.at[m, 0, 0, j], buf)
            ys[m, j] = w.send(wm.at[m, 0, 0, j], LYM.at[m, 1 - j], "y")

    def wide_end(m, j):
        with mark("A_we"):
            ys[m, 1 - j].wait_recv()
            buf, cp = fetch(LYM.at[m, j])
            cp.wait()
            fin = (gate_scr, up_scr)[j]
            add_into(fin, wm.at[m, 0, 0, j], buf)
            return local(fin, GDOWN.at[lax.rem(y + j, 2)])

    for cp in stored:
        cp.wait()
    for name in mats:
        w.sent(ev[name, "y"])
        w.sent(ev[name, "c"])
    wide_part(2, 1)
    wide_part(2, 0)
    wide_core(2)
    wide_x(2, 0)
    wide_x(2, 1)
    wide_part(0, 1)
    wide_part(0, 0)
    wide_core(0)
    wide_x(0, 0)
    wide_y(2, 0)
    wide_part(1, 1)
    wide_part(1, 0)
    wide_y(2, 1)
    wide_core(1)
    saved = [local(wm.at[0, 0, 0], TGU.at[0, 0]), local(wm.at[0, 0, 1, 1], TGU.at[0, 1, 1])]
    saved.append(local(wm.at[1, 0], TGU.at[1]))
    with mark("A_r0"):
        sum_arrived(0)
    add_rows(own_scr, 0)
    with mark("A_r1"):
        sum_arrived(1)
        sum_arrived(2)
    add_rows(own_scr, 1)
    add_rows(own_scr, 2)
    gain2_out[...] = jnp.zeros_like(gain2_out)

    def norm_back(i, carry):
        at = pl.ds(pl.multiple_of(i * 32, 32), 32)
        gn = own_scr[at, :]
        mid = mid_ref[at, :]
        inv = lax.rsqrt(jnp.mean(mid * mid, axis=1, keepdims=True) + NORM_EPS)
        unit = mid * inv
        gain2_out[...] += jnp.sum(gn * unit, axis=0, keepdims=True)
        scaled = gn * gains[1:2, :]
        inside = jnp.mean(scaled * unit, axis=1, keepdims=True)
        gmid = DY[0, at, :].astype(F32) + inv * (scaled - unit * inside)
        gmid_ref[at, :] = gmid
        out_stage[at, :] = gmid.astype(BF16)
        return carry

    lax.fori_loop(0, 8, norm_back, 0)
    last = [local(out_stage, BRANCH)]
    last.append(wide_end(2, 0))
    last.append(wide_end(2, 1))
    with mark("A_end"):
        xs[0, 0].wait_recv()
    for cp in last + saved:
        cp.wait()
    assert w.count <= 112
    w.finish()


def start_call(args):
    vmem = pl.BlockSpec(memory_space=pltpu.VMEM)
    hbm = pl.BlockSpec(memory_space=pl.ANY)
    outs = [
        ((4, 2, 2, 2, 256, 512), BF16, hbm), ((4, 2, 2, 2, 256, 512), BF16, hbm),
        ((4, 2, 2, 2, 256, 128), BF16, hbm), ((4, 256, 2048), BF16, hbm),
        ((256, 2048), BF16, hbm), ((4, 256, 512), BF16, hbm), ((4, 512, 256), F32, hbm), ((256, 2048), BF16, hbm),
        ((3, 2, 2, 256, 1408), BF16, hbm), ((3, 2, 256, 1408), BF16, hbm), ((3, 2, 256, 1408), BF16, hbm),
        ((2, 2, 2, 256, 1408), BF16, hbm), ((2, 256, 1408), F32, hbm),
        ((4, 4, 256, 128), BF16, vmem), ((4, 256, 512), BF16, vmem), ((4, 8, 256), F32, vmem),
        ((256, 2048), F32, vmem), ((256, 2048), F32, vmem), ((1, 2048), F32, vmem),
    ]
    scratch = [
        ((3, 2, 2, 2, 256, 1408), BF16), ((3, 256, 2048), BF16), ((4, 256, 2048), BF16), ((4, 256, 2048), BF16),
        ((2, 2, 2, 2, 256, 512), BF16), ((2, 2, 2, 2, 256, 128), BF16), ((256, 512), F32),
        ((256, 512), BF16), ((512, 256), F32), ((256, 1408), F32), ((256, 1408), F32), ((256, 1408), F32),
        ((3, 4, 256, 1408), BF16), ((256, 2048), BF16), ((2, 256, 1408), BF16), ((2, 2048), F32),
    ]
    return pl.pallas_call(
        start_kernel,
        out_shape=[jax.ShapeDtypeStruct(a, b) for a, b, _ in outs],
        in_specs=[vmem] * 10 + [hbm] * (len(args) - 10),
        out_specs=[o[2] for o in outs],
        scratch_shapes=[pltpu.VMEM(a, b) for a, b in scratch]
        + [pltpu.SemaphoreType.DMA((128,)), pltpu.SemaphoreType.DMA((128,)), pltpu.SemaphoreType.DMA((128,))],
        compiler_params=pltpu.CompilerParams(
            collective_id=0, has_side_effects=True, vmem_limit_bytes=67043328
        ),
        cost_estimate=pl.CostEstimate(flops=10**10, bytes_accessed=10**8, transcendentals=0),
    )(*args)


def attend_back(s, kv_of, ga_scr, q_ref, bias_ref, c_ref, s_ref, ot_ref, lse_ref, dq_scr, d0, dr, ds_scr, p_scr, dk_scr, dv_scr):
    kv = jnp.concatenate([kv_of[t, (s - t) % 4].astype(F32) for t in range(4)], axis=0)
    k_low = kv[:, :64].astype(BF16)
    v_low = pltpu.roll(kv, 64, 1)[:, :64].astype(BF16)
    k_t = kv.T[:64].astype(BF16)
    dk_scr[...] = jnp.zeros_like(dk_scr)
    dv_scr[...] = jnp.zeros_like(dv_scr)

    def pair(p, carry):
        cols = pl.ds(pl.multiple_of(p * 128, 128), 128)
        lane = lax.broadcasted_iota(jnp.int32, (256, 128), 1)
        qp = q_ref[s, :, cols].astype(F32)
        gp = ga_scr[:, cols]
        q_t = qp.T.astype(BF16)
        g_tf = gp.T
        g_t = g_tf.astype(BF16)
        prod = g_tf * ot_ref[cols, :]
        dq_t = []
        for e in range(2):
            half = slice(64 * e, 64 * e + 64)
            s_t = nn(k_low, q_t[half]) + bias_ref[...]
            pr = jnp.exp(s_t - lse_ref[s, pl.ds(2 * p + e, 1), :])
            dp = nn(v_low, g_t[half])
            inner = jnp.sum(prod[half], axis=0, keepdims=True)
            ds = (pr * (dp - inner)).astype(BF16)
            ds_scr[:, 256 * e : 256 * e + 256] = ds
            p_scr[:, 256 * e : 256 * e + 256] = pr.astype(BF16)
            dq_t.append(nn(k_t, ds))
        qbd = jnp.concatenate(
            [jnp.where(lane < 64, qp, 0.0), jnp.where(lane < 64, 0.0, qp)], axis=0
        ).astype(BF16)
        gbd = jnp.concatenate(
            [jnp.where(lane < 64, gp, 0.0), jnp.where(lane < 64, 0.0, gp)], axis=0
        ).astype(BF16)
        dk_scr[...] += nn(ds_scr[...], qbd)
        dv_scr[...] += nn(p_scr[...], gbd)
        dqp = jnp.concatenate(dq_t, axis=0).T * 0.125
        dq_scr[s, :, cols] = (dqp * c_ref[...] - swap_halves(dqp) * s_ref[...]).astype(BF16)
        return carry

    lax.fori_loop(0, 4, pair, 0)
    dk = dk_scr[...]
    dv = dv_scr[...]
    lane = lax.broadcasted_iota(jnp.int32, dk.shape, 1)
    both = jnp.where(lane < 64, dk + pltpu.roll(dk, 64, 1), dv + pltpu.roll(dv, 64, 1))
    d0[s] = both[:256]
    for t in range(3):
        dr[t, s] = both[256 * (t + 1) : 256 * (t + 2)].astype(BF16)


def add_into(into, one, other, step=32):
    def body(i, carry):
        at = pl.ds(pl.multiple_of(i * step, step), step)
        into[at, :] = (one[at, :].astype(F32) + other[at, :].astype(F32)).astype(into.dtype)
        return carry

    lax.fori_loop(0, into.shape[0] // step, body, 0)


def end_kernel(
    WQ, WO, WKV, OT, TGU, LXM, OUT, MID, TOK, BRANCH, GMID, NONE, QS, KVS, OS, BIAS, gain1_ref, gain2t_ref,
    lse_ref, cq_ref, sq_ref, ck_ref, sk_ref,
    gtok_ref, gains_ref, GGT, GUP, GQ, GO, GKV, bout_ref, LCO, LCQ, LCK, LYM, LX, LOUT,
    TM, TO, TQ, TK, S, L1O, L1Q, L1K, L2O, L2Q, L2K, LZO, LZQ, LZK, FO, FQ, FK, YO, YQ, YK,
    wbuf, wk, act_t, ga_scr, dq_scr, dkv_scr, d0, dr, ld, ds_scr, p_scr, dk_scr, dv_scr, gn_scr, pre, ot_scr, fin, gsum, gland, obuf, branch_ref, gmid_ref, n1_ref, q_ref, kv_ref, o_ref, bias_ref, gain_rel,
    send_sem, recv_sem, loc_sem,
):
    z = lax.axis_index("col")
    y = lax.axis_index("dp")
    r = lax.axis_index("row")
    x, c = r // 2, lax.rem(r, 2)
    w = Wire(send_sem, recv_sem, z)
    locs = []

    def local(src, dst):
        cp = pltpu.make_async_copy(src, dst, loc_sem.at[len(locs)])
        cp.start()
        locs.append(cp)
        return cp

    brought = {
        "o": local(OS, o_ref), "b": local(BRANCH, branch_ref), "q": local(QS, q_ref), "kv": local(KVS, kv_ref),
        "bias": local(BIAS, bias_ref), "n": local(NONE, n1_ref), "g": local(GMID, gmid_ref),
    }
    greet(z)
    finals = (GGT, GUP)
    places = relative(x, c, y)
    for m, at in enumerate(places):
        gain_rel[:, 256 * m : 256 * m + 256] = gain1_ref[:, pl.ds(at, 256)]
    tok_cp = [local(TOK.at[:, pl.ds(at, 256)], obuf.at[:, pl.ds(256 * m, 256)]) for m, at in enumerate(places)]
    kept = [local(TGU.at[0, 0], TM.at[0, 0]), local(TGU.at[1], TM.at[1])]
    xs, ys = {}, {}
    xs[0, 1] = w.send(TGU.at[0, 1, 1], LX.at[0, 1], "x")
    buddy = z + 1 - 2 * lax.rem(z, 2)
    out_cp = []
    for s in (1, 2, 3):
        to = lax.rem(z + s, 4)
        second = jnp.where(z < 2, 2, 1)
        slot = jnp.where(to == buddy, 1, jnp.where(to == second, 2, 3))
        late = (slot == 3) & (z >= 2)
        out_cp.append((w.copy(OUT.at[slot], LOUT.at[s - 1], to), late))
        pl.when(jnp.logical_not(late))(out_cp[-1][0].start)
    wo_cp = {0: local(WO.at[0], wbuf.at[0])}
    wq_cp = {0: local(WQ.at[0], wbuf.at[1])}
    ot_cp = {0: local(OT.at[0], ot_scr)}

    def turned(src):
        for j in range(8):
            act_t[256 * j : 256 * j + 256, :] = src[:, 256 * j : 256 * j + 256].astype(F32).T.astype(BF16)

    def grad_part(g, keep, give, cols):
        for i in range(2):
            for j in range(2):
                at = 512 * i + 256 * j
                give[i, j, :, cols] = nn(act_t[1024 + at : 1024 + at + 256, :], g).astype(BF16)
        for i in range(2):
            for j in range(2):
                at = 512 * i + 256 * j
                keep[i, j, :, cols] = nn(act_t[at : at + 256, :], g).astype(BF16)

    every = slice(0, 512)
    brought["b"].wait()
    brought["o"].wait()
    with mark("B_turn"):
        turned(branch_ref)
    oc = []
    for s in range(4):
        if s > 1:
            w.sent(oc[s - 2])
        with mark("B_go"):
            grad_part(o_ref[s], TO.at[s], S.at[s % 2], every)
        oc.append(w.send(S.at[s % 2], LCO.at[s], "c"))

    slots = [0]

    def wide_x(m, j):
        xs[m, j] = w.send(TM.at[m, 1, j], LX.at[m, j], "x")

    def wide_y(m, j):
        if (m, j) != (0, 0):
            xs[m, j].wait_recv()
        b = slots[0] % 2
        slots[0] += 1
        local((LXM if (m, j) == (0, 0) else LX).at[m, j], pre.at[b, 0]).wait()
        add_into(TM.at[m, 0, j], TM.at[m, 0, j], pre.at[b, 0])
        ys[m, j] = w.send(TM.at[m, 0, j], LYM.at[m, 1 - j], "y")

    outs = []

    def wide_end(m, j):
        ys[m, 1 - j].wait_recv()
        b = slots[0] % 2
        slots[0] += 1
        local(LYM.at[m, j], pre.at[b, 0]).wait()
        if len(outs) >= 1:
            outs[-1].wait()
        add_into(fin, TM.at[m, 0, j], pre.at[b, 0])
        outs.append(local(fin, finals[m].at[lax.rem(y + j, 2)]))

    class Narrow:
        def __init__(self, T, LC, L1, L2, LZ, F, Y, out, y_first, turn=False):
            self.T, self.LC, self.L1, self.L2, self.LZ, self.F, self.Y, self.out = T, LC, L1, L2, LZ, F, Y, out
            self.cps = {}
            self.y_first, self.turn = y_first, turn

        def core(self, s, cp):
            cp.wait_recv()
            tiles = [(i, j, pre.at[i, j, :, pl.ds(0, 512)]) for i in range(2) for j in range(2)]
            loads = [local(self.LC.at[s, i, j], t) for i, j, t in tiles]
            for (i, j, t), cp in zip(tiles, loads):
                cp.wait()
                add_into(self.T.at[s, i, j], self.T.at[s, i, j], t)

        def first(self, s):
            if s in self.y_first:
                self.cps[s, 1] = w.send(self.T.at[s, :, 1], self.L1.at[s], "y")
            else:
                self.cps[s, 1] = w.send(self.T.at[s, 1], self.L1.at[s], "x")

        def second(self, s):
            self.cps[s, 1].wait_recv()
            for b in range(2):
                mine = self.T.at[s, b, 0] if s in self.y_first else self.T.at[s, 0, b]
                add_into(mine, mine, self.L1.at[s, b])
            if s in self.y_first:
                self.cps[s, 2] = w.send(self.T.at[s, 1, 0], self.L2.at[s], "x")
            else:
                self.cps[s, 2] = w.send(self.T.at[s, 0, 1], self.L2.at[s], "y")

        def third(self, s):
            self.cps[s, 2].wait_recv()
            mine = self.T.at[s, 0, 0]
            add_into(mine, mine, self.L2.at[s])
            if s:
                self.cps[s, 3] = w.send(mine, self.LZ.at[s - 1], lax.rem(z + s, 4))

        def fourth(self):
            for s in (1, 2, 3):
                self.cps[s, 3].wait_recv()

            def body(i, carry):
                at = pl.ds(pl.multiple_of(i * 32, 32), 32)
                tot = self.T[0, 0, 0, at, :].astype(F32)
                for s in range(3):
                    tot = tot + self.LZ[s, at, :].astype(F32)
                self.F[at, :] = tot.astype(BF16)
                return carry

            lax.fori_loop(0, 8, body, 0)
            self.cps["y"] = w.send(self.F, self.Y, "y")

        def last(self):
            self.cps["y"].wait_recv()
            if self.turn:
                for half, src in ((y, self.F), (1 - y, self.Y)):
                    self.out[:, pl.ds(pl.multiple_of(256 * half, 256), 256)] = src[...].astype(F32).T
            else:
                self.out[y] = self.F[...].astype(F32)
                self.out[1 - y] = self.Y[...].astype(F32)

    wo_g = Narrow(TO, LCO, L1O, L2O, LZO, FO, YO, GO, (1, 3), turn=True)
    wq_g = Narrow(TQ, LCQ, L1Q, L2Q, LZQ, FQ, YQ, GQ, (1,))
    qc = []
    dk_cp = {}

    def attend(s):
        wo_cp[s].wait()
        ga_scr[...] = nn(branch_ref[...], wbuf[0].reshape(2048, 512)).astype(BF16).astype(F32)
        if s < 3:
            wo_cp[s + 1] = local(WO.at[s + 1], wbuf.at[0])
        ot_cp[s].wait()
        attend_back(
            s, kv_ref, ga_scr, q_ref, bias_ref, cq_ref, sq_ref, ot_scr, lse_ref, dq_scr, d0, dr, ds_scr, p_scr,
            dk_scr, dv_scr,
        )
        if s < 3:
            ot_cp[s + 1] = local(OT.at[s + 1], ot_scr)
        for t in (1, 2, 3):
            cp = w.copy(dr.at[t - 1, s], ld.at[t - 1, s], lax.rem(z + t, 4), only=z + t >= 4)
            dk_cp[t, s] = cp
            pl.when(z + t >= 4)(cp.start)
        wq_cp[s].wait()

        def columns(i, carry):
            at = pl.ds(pl.multiple_of(i * 512, 512), 512)
            part = nt(dq_scr[s], wbuf[1, i // 2, i % 2].reshape(512, 512))
            if s:
                gn_scr[:, at] += part
            else:
                gn_scr[:, at] = part
            return carry

        lax.fori_loop(0, 4, columns, 0)
        if s < 3:
            wq_cp[s + 1] = local(WQ.at[s + 1], wbuf.at[1])
        w.sent(oc[s + 2] if s < 2 else qc[s - 2])
        grad_part(dq_scr[s], TQ.at[s], S.at[s % 2], every)
        qc.append(w.send(S.at[s % 2], LCQ.at[s], "c"))

    for cp in kept:
        cp.wait()
    wide_x(1, 0)
    wide_y(0, 0)
    wide_x(1, 1)
    for s in (1, 3, 0, 2):
        with mark("B_oc"):
            wo_g.core(s, oc[s])
        wo_g.first(s)
    for name in ("n", "q", "kv", "bias"):
        brought[name].wait()
    turned(n1_ref)
    with mark('B_att0'):
        attend(0)
    with mark("B_wy"):
        wide_y(0, 1)
    with mark('B_att1'):
        attend(1)
    with mark("B_qc"):
        wq_g.core(1, qc[1])
        wq_g.first(1)
    with mark('B_att2'):
        attend(2)
    with mark("B_o2"):
        for s in (1, 3):
            wo_g.second(s)
    with mark("B_wy"):
        wide_y(1, 0)
    with mark("B_qc"):
        wq_g.core(0, qc[0])
        wq_g.first(0)
    with mark('B_att3'):
        attend(3)
    wk_cp = {0: local(WKV.at[0], wk.at[0]), 1: local(WKV.at[1], wk.at[1])}
    with mark("B_qc"):
        for s in (3, 2):
            wq_g.core(s, qc[s])
            wq_g.first(s)
    with mark("B_o2"):
        for s in (0, 2):
            wo_g.second(s)
    with mark("B_o3"):
        for s in (1, 3):
            wo_g.third(s)
    for cp, late in out_cp:
        pl.when(late)(cp.start)
    with mark("B_wy"):
        wide_y(1, 1)
    with mark("B_q2"):
        wq_g.second(1)
    with mark("B_o3"):
        for s in (0, 2):
            wo_g.third(s)
    for s in range(4):
        dkv_scr[:, 128 * s : 128 * s + 128] = d0[s]
    for t in (1, 2, 3):

        with mark("B_dkr"):

            @pl.when(z < t)
            def _():
                for s in range(4):
                    dk_cp[t, (s + t) % 4].wait_recv()
                    dkv_scr[:, 128 * s : 128 * s + 128] += ld[t - 1, (s + t) % 4].astype(F32)

    for s in range(4):
        cols = slice(128 * s, 128 * s + 128)
        v = dkv_scr[:, cols]
        dkv = (v * ck_ref[...] - swap_halves(v) * sk_ref[...]).astype(BF16)
        wk_cp[s].wait()

        def columns(i, carry):
            at = pl.ds(pl.multiple_of(i * 512, 512), 512)
            gn_scr[:, at] += nt(dkv, wk[s % 2, i // 2, i % 2].reshape(512, 128))
            return carry

        lax.fori_loop(0, 4, columns, 0)
        if s < 2:
            wk_cp[s + 2] = local(WKV.at[s + 2], wk.at[s % 2])
        if s == 0:
            w.sent(qc[2])
        with mark("B_gk"):
            grad_part(dkv, TK.at[0], S.at[0], cols)
    kc = w.send(S.at[0], LCK.at[0], "c")

    gsum[0:1, :] = jnp.zeros((1, 2048), F32)
    for cp in tok_cp:
        cp.wait()

    def norm_back(i, carry):
        at = pl.ds(pl.multiple_of(i * 32, 32), 32)
        gn = gn_scr[at, :]
        x_in = obuf[at, :].astype(F32)
        inv = lax.rsqrt(jnp.mean(x_in * x_in, axis=1, keepdims=True) + NORM_EPS)
        unit = x_in * inv
        gsum[0:1, :] += jnp.sum(gn * unit, axis=0, keepdims=True)
        scaled = gn * gain_rel[...]
        inside = jnp.mean(scaled * unit, axis=1, keepdims=True)
        back = (gmid_ref[at, :] + inv * (scaled - unit * inside)).astype(BF16)
        for m, to in enumerate(places):
            gtok_ref[at, pl.ds(to, 256)] = back[:, 256 * m : 256 * m + 256]
        return carry

    brought["g"].wait()
    with mark("B_nb"):
        lax.fori_loop(0, 8, norm_back, 0)
    gsum[1:2, :] = gain2t_ref[...]
    for hi in range(2):
        for mid in range(2):
            for lo in range(2):
                at = 4 * (c ^ mid) + 2 * (x ^ hi) + (y ^ lo)
                gains_ref[:, 256 * (4 * hi + 2 * mid + lo) : 256 * (4 * hi + 2 * mid + lo) + 256] = gsum[
                    :, pl.ds(pl.multiple_of(at * 256, 256), 256)
                ]
    steps = ["c", "x", "y", z + 1 - 2 * lax.rem(z, 2), lax.rem(z + 2, 4)]
    gain_cp = []

    def gain_next(n):
        gland[5 + n] = gains_ref[...]
        gain_cp.append(w.send(gland.at[5 + n], gland.at[n], steps[n]))

    def gain_add(n):
        gain_cp[n].wait_recv()
        gains_ref[...] += gland[n]

    gain_next(0)
    mid_cp = local(MID, gn_scr)
    wk_g = Narrow(TK, LCK, L1K, L2K, LZK, FK, YK, GKV, ())
    with mark("B_kc"):
        wk_g.core(0, kc)
    with mark("B_kf"):
        wk_g.first(0)
    with mark('B_g0'):
        gain_add(0)
    gain_next(1)
    with mark("B_q2"):
        for s in (0, 3, 2):
            wq_g.second(s)
    with mark("B_we"):
        wide_end(0, 0)
    with mark("B_k2"):
        wk_g.second(0)
    with mark("B_q3"):
        for s in (1, 0, 3, 2):
            wq_g.third(s)
    with mark('B_g1'):
        gain_add(1)
    gain_next(2)
    with mark("B_we"):
        wide_end(0, 1)
    with mark("B_k3"):
        wk_g.cps[0, 2].wait_recv()
    add_into(TK.at[0, 0, 0], TK.at[0, 0, 0], L2K.at[0])
    for s in (1, 2, 3):
        wk_g.cps[s, 3] = w.send(TK.at[0, 0, 0, :, pl.ds(128 * s, 128)], LZK.at[s - 1], lax.rem(z + s, 4))
    with mark('B_g2'):
        gain_add(2)
    gain_next(3)
    with mark("B_of"):
        wo_g.fourth()
    with mark("B_we"):
        wide_end(1, 0)
        wide_end(1, 1)
    with mark('B_g3'):
        gain_add(3)
    gain_next(4)
    with mark("B_ol"):
        wo_g.last()
    with mark("B_qf"):
        wq_g.fourth()
    with mark("B_k4"):
        for s in (1, 2, 3):
            wk_g.cps[s, 3].wait_recv()
    tot = TK[0, 0, 0, :, 0:128].astype(F32)
    for s in range(3):
        tot = tot + LZK[s].astype(F32)
    FK[...] = tot.astype(BF16)
    wk_g.cps["y"] = w.send(FK, YK, "y")
    with mark("B_out"):
        mid_cp.wait()
        for n in range(4):
            if n:
                out_cp[n - 1][0].wait_recv()
            local(OUT.at[0] if n == 0 else LOUT.at[n - 1], obuf).wait()
            add_into(gn_scr, gn_scr, obuf)

        def to_own(i, carry):
            at = pl.ds(pl.multiple_of(i * 32, 32), 32)
            for m, to in enumerate(places):
                bout_ref[at, pl.ds(to, 256)] = gn_scr[at, 256 * m : 256 * m + 256].astype(BF16)
            return carry

        lax.fori_loop(0, 8, to_own, 0)
    with mark('B_g4'):
        gain_add(4)
    with mark("B_last"):
        wq_g.last()
        wk_g.last()
    outs[-1].wait()
    w.finish()


def end_call(args):
    vmem = pl.BlockSpec(memory_space=pltpu.VMEM)
    hbm = pl.BlockSpec(memory_space=pl.ANY)
    outs = [
        ((256, 2048), BF16, vmem), ((2, 2048), F32, vmem),
        ((2, 256, 1408), F32, hbm), ((2, 256, 1408), F32, hbm),
        ((2, 256, 512), F32, vmem), ((512, 512), F32, vmem), ((2, 256, 128), F32, vmem), ((256, 2048), BF16, vmem),
        ((4, 2, 2, 256, 512), BF16, hbm), ((4, 2, 2, 256, 512), BF16, hbm), ((1, 2, 2, 256, 512), BF16, hbm),
        ((2, 2, 256, 1408), BF16, hbm), ((2, 2, 256, 1408), BF16, hbm), ((3, 256, 2048), BF16, hbm),
    ]
    scratch = [
        ((2, 2, 2, 256, 1408), BF16), ((4, 2, 2, 256, 512), BF16), ((4, 2, 2, 256, 512), BF16), ((1, 2, 2, 256, 512), BF16),
        ((2, 2, 2, 256, 512), BF16),
        ((4, 2, 256, 512), BF16), ((4, 2, 256, 512), BF16), ((1, 2, 256, 512), BF16),
        ((4, 256, 512), BF16), ((4, 256, 512), BF16), ((1, 256, 512), BF16),
        ((3, 256, 512), BF16), ((3, 256, 512), BF16), ((3, 256, 128), BF16),
        ((256, 512), BF16), ((256, 512), BF16), ((256, 128), BF16),
        ((256, 512), BF16), ((256, 512), BF16), ((256, 128), BF16),
        ((2, 2, 2, 2, 256, 512), BF16), ((2, 2, 2, 2, 256, 128), BF16), ((2048, 256), BF16), ((256, 512), F32),
        ((4, 256, 512), BF16), ((256, 512), F32), ((4, 256, 128), F32), ((3, 4, 256, 128), BF16), ((3, 4, 256, 128), BF16),
        ((1024, 512), BF16), ((1024, 512), BF16), ((1024, 128), F32), ((1024, 128), F32), ((256, 2048), F32),
        ((2, 2, 256, 1408), BF16), ((512, 256), F32), ((256, 1408), F32), ((2, 2048), F32), ((10, 2, 2048), F32), ((256, 2048), BF16),
        ((256, 2048), BF16), ((256, 2048), F32), ((256, 2048), BF16), ((4, 256, 512), BF16), ((4, 4, 256, 128), BF16),
        ((4, 256, 512), BF16), ((1024, 256), F32), ((1, 2048), F32),
    ]
    return pl.pallas_call(
        end_kernel,
        out_shape=[jax.ShapeDtypeStruct(a, b) for a, b, _ in outs],
        in_specs=[hbm] * 16 + [vmem] * (len(args) - 16),
        out_specs=[o[2] for o in outs],
        scratch_shapes=[pltpu.VMEM(a, b) for a, b in scratch]
        + [pltpu.SemaphoreType.DMA((96,)), pltpu.SemaphoreType.DMA((96,)), pltpu.SemaphoreType.DMA((96,))],
        compiler_params=pltpu.CompilerParams(
            collective_id=1, has_side_effects=True, vmem_limit_bytes=67043328
        ),
        cost_estimate=pl.CostEstimate(flops=10**11, bytes_accessed=2 * 10**8, transcendentals=0),
    )(*args)


X_SWAP = [(0, 2), (1, 3), (2, 0), (3, 1)]
C_SWAP = [(0, 1), (1, 0), (2, 3), (3, 2)]
Y_SWAP = [(0, 1), (1, 0)]
PAIR = [(0, 1), (1, 0), (2, 3), (3, 2)]
MIDDLE = [(1, 2), (2, 1)]
OUTWARD = [(1, 0), (2, 3)]
INWARD = [(0, 1), (3, 2)]


def over_x(a):
    return lax.ppermute(a, "row", X_SWAP)


def over_c(a):
    return lax.ppermute(a, "row", C_SWAP)


def over_y(a):
    return lax.ppermute(a, "dp", Y_SWAP)


def over_z(a, pairs):
    return lax.ppermute(a, "col", pairs)


def from_slot(a, s):
    return over_z(a, [((i + s) % 4, i) for i in range(4)])


def to_slot(a, s):
    return over_z(a, [(i, (i + s) % 4) for i in range(4)])


def gather_col(own, inner):
    first = over_z(own, PAIR)
    mid = over_z(own, MIDDLE)
    third_in = over_z(first, MIDDLE)
    second = jnp.where(inner, mid, over_z(mid, OUTWARD))
    third = jnp.where(inner, third_in, over_z(third_in, OUTWARD))
    return own, first, second, third


def scatter_col(parts):
    own, first, second, third = parts
    t3 = (third + over_z(third.astype(BF16), INWARD)).astype(BF16)
    t2 = (second + over_z(second.astype(BF16), INWARD)).astype(BF16)
    t1 = (first + over_z(t3, MIDDLE)).astype(BF16)
    v = over_z(t2, MIDDLE)
    w = over_z(t1, PAIR)
    return own + v.astype(F32) + w.astype(F32)


def norm_forward(values, gain_vec):
    mean_sq = jnp.mean(values * values, axis=1, keepdims=True)
    inv_rms = lax.rsqrt(mean_sq + NORM_EPS)
    unit_rows = values * inv_rms
    return (unit_rows, inv_rms, (unit_rows * gain_vec).astype(BF16))


def norm_backward(grad_norm, unit_rows, inv_rms, gain_vec):
    scaled = grad_norm * gain_vec
    inner_sum = jnp.mean(scaled * unit_rows, axis=1, keepdims=True)
    return (inv_rms * (scaled - unit_rows * inner_sum), jnp.sum(grad_norm * unit_rows, axis=0))


def shards(
    tokens, gain_attn, w_query, w_keyval, w_output, gain_mlp, w_gate, w_up, w_down, out_grad,
    document_numbers, positions, *, rows,
):
    width = tokens.shape[1]
    fast = rows == 4
    z = lax.axis_index("col")
    r = lax.axis_index("row")
    y = lax.axis_index("dp")
    inner = (z == 1) | (z == 2)
    x, c = r // 2, r % 2
    blk = width // 8

    def permuted(a, abs_order):
        if not fast:
            return a
        axis = a.ndim - 1
        pieces = []
        for hi in range(2):
            for mid in range(2):
                for lo in range(2):
                    if abs_order:
                        at = 4 * (c ^ mid) + 2 * (x ^ hi) + (y ^ lo)
                    else:
                        at = 4 * (x ^ mid) + 2 * (c ^ hi) + (y ^ lo)
                    pieces.append(lax.dynamic_slice_in_dim(a, at * blk, blk, axis))
        return jnp.concatenate(pieces, axis=axis)

    to_rel = functools.partial(permuted, abs_order=False)
    to_abs = functools.partial(permuted, abs_order=True)

    def gather_rows(block):
        return lax.all_gather(block, "row", axis=0, tiled=True)

    def gather_slots(block):
        full = gather_rows(block)
        return [full] + [from_slot(full, s) for s in (1, 2, 3)]

    tok = to_rel(tokens)
    x_in = tok.astype(F32)
    gain_one = to_rel(gain_attn)
    gain_two = to_rel(gain_mlp)
    unit_one, inv_one, normed_one = norm_forward(x_in, gain_one)
    count = tokens.shape[0]
    my_pos = lax.dynamic_slice_in_dim(positions, z * count, count, 0)
    frequency = ROPE_BASE ** (-(jnp.arange(32, dtype=F32) * 2.0 / HEAD_SIZE))
    angles = my_pos.astype(F32)[:, None] * frequency[None, :]
    co, si = jnp.cos(angles), jnp.sin(angles)
    cos_q = jnp.concatenate([co, co, co, co], axis=1)
    sin_q = jnp.concatenate([-si, si, -si, si], axis=1)
    cos_k = jnp.concatenate([co, co, jnp.ones_like(co), jnp.ones_like(co)], axis=1)
    sin_k = jnp.concatenate([-si, si, jnp.zeros_like(si), jnp.zeros_like(si)], axis=1)
    my_seg = lax.dynamic_slice_in_dim(document_numbers, z * count, count, 0)
    key_seg = jnp.concatenate(
        [lax.dynamic_slice_in_dim(document_numbers, ((z + t) % 4) * count, count, 0) for t in range(4)]
    )
    lane = jnp.arange(count, dtype=jnp.int32)
    key_at = jnp.concatenate([((z + t) % 4) * count + lane for t in range(4)])
    allowed = (key_seg[:, None] == my_seg[None, :]) & (key_at[:, None] <= (z * count + lane)[None, :])
    bias = jnp.where(allowed, 0.0, MASK_FILL).astype(F32)

    def separate():
        full = lax.all_gather(w_keyval, "row", axis=0, tiled=True)
        wkv = jnp.concatenate([full] + [from_slot(full, s) for s in (1, 2, 3)], axis=1)
        wq = gather_slots(w_query)
        wo = gather_slots(w_output.T)
        wg, wu, wd = gather_rows(w_gate), gather_rows(w_up), gather_rows(w_down.T)
        kv = call(
            kv_kernel, [((4, count, 128), BF16)], (normed_one, wkv, cos_k, sin_k), 2 * count * width * 512
        )[0]
        kv_from = [kv]
        for t in (1, 2, 3):
            kv_from.append(over_z(kv, [((i + t) % 4, i) for i in range(4) if i + t >= 4]))
        kv_of = [[kv_from[t][(s - t) % 4] for t in range(4)] for s in range(4)]
        fwd = []
        for s in range(4):
            fwd.append(
                call(
                    fwd_kernel,
                    [((count, 512), BF16), ((count, 512), BF16), ((512, count), F32), ((8, count), F32)],
                    (normed_one, wq[s], *kv_of[s], bias, cos_q, sin_q),
                    2 * count * width * 512 + 8 * 4 * count * 1024 * 256,
                )
            )
        attn = [f[1] for f in fwd]
        mid = x_in + (nt(attn[0], wo[0]) + nt(attn[1], wo[1]) + nt(attn[2], wo[2]) + nt(attn[3], wo[3]))
        unit_two, inv_two, n2 = norm_forward(mid, gain_two)
        dys = gather_col(dy, inner)
        n2s = gather_col(n2, inner)
        outs, gns, acts, ggs, gus = [], [], [], [], []
        for s in range(4):
            gate_pre = nn(n2s[s], wg)
            up_pre = nn(n2s[s], wu)
            grad_act = nn(dys[s], wd)
            sig = jax.nn.sigmoid(gate_pre)
            silu = gate_pre * sig
            act = (silu * up_pre).astype(BF16)
            gg = (grad_act * up_pre * sig * (1.0 + gate_pre * (1.0 - sig))).astype(BF16)
            gu = (grad_act * silu).astype(BF16)
            outs.append(nt(act, wd))
            gns.append(nt(gg, wg) + nt(gu, wu))
            acts.append(act)
            ggs.append(gg)
            gus.append(gu)
        grad_norm_two = scatter_col(gns)
        flat = [jnp.concatenate(v, axis=0) for v in (n2s, dys, acts, ggs, gus)]
        mid_norm, gain2 = norm_backward(grad_norm_two, unit_two, inv_two, gain_two)
        gmid = dy.astype(F32) + mid_norm
        return wq, wo, wkv, kv_of, fwd, attn, mid, outs, flat, gmid, gmid.astype(BF16), gain2

    def together():
        def cut(block):
            return block.reshape(2, block.shape[0] // 2, block.shape[1])

        WQ, WO, WKV, OUT, n1, q, ot, branch, _, LXM, _, TGU, gd, kv, o, lse, mid, gmid, gain2 = start_call(
            (
                gain_attn[None, :], gain_mlp[None, :], cut(w_query), cut(w_output.T), cut(w_keyval), bias, cos_q, sin_q, cos_k, sin_k, tokens, cut(w_gate),
                cut(w_up), cut(w_down.T), out_grad,
            )
        )
        gtok, gains, gg, gu, gq, go, gkv, bout = end_call(
            (
                WQ, WO, WKV, ot, TGU, LXM, OUT, mid, tokens, branch, gmid, n1, q, kv, o, bias, gain_attn[None, :], gain2, lse,
                cos_q, sin_q, cos_k, sin_k,
            )
        )[:8]

        def joined(g):
            return g.reshape(2 * blk, g.shape[-1])

        return (
            bout, gtok, gains[0], joined(gq), joined(gkv), go, gains[1],
            joined(gg), joined(gu), joined(gd).T,
        )

    dy = to_rel(out_grad)
    if fast:
        return together()
    wq, wo, wkv, kv_of, fwd, attn, resid_mid, outs, flat, grad_mid, branch, gain_two_term = separate()
    n2_all, dy_all, act_all, gg_all, gu_all = flat
    block_out = (resid_mid + scatter_col([o.astype(F32) for o in outs])).astype(BF16)

    def ordered(lo, hi):
        return jnp.where(y == 0, jnp.concatenate([lo, hi], axis=0), jnp.concatenate([hi, lo], axis=0))

    def weight_grad(act_rel, g):
        half = width // 2
        if not fast:
            full = lax.psum_scatter(tn(act_rel, g).astype(BF16), "row", scatter_dimension=0, tiled=True)
            return lax.psum(full, "dp").astype(F32)
        got = over_c(tn(act_rel[:, half:], g).astype(BF16))
        t = tn(act_rel[:, :half], g) + got.astype(F32)
        q = half // 2
        got = over_x(t[q:].astype(BF16))
        t = (t[:q] + got.astype(F32)).astype(BF16)
        got = over_y(t).astype(F32)
        t = t.astype(F32)
        return ordered(t[: q // 2] + got[q // 2 :], t[q // 2 :] + got[: q // 2])

    def weight_grad_slots(act_rel, gs):
        half = width // 2
        if not fast:
            tot = 0.0
            for s in range(4):
                full = lax.psum_scatter(
                    tn(act_rel, gs[s]).astype(BF16), "row", scatter_dimension=0, tiled=True
                )
                tot = tot + (full if s == 0 else to_slot(full, s)).astype(F32)
            return lax.psum(tot.astype(BF16), "dp").astype(F32)
        tot = 0.0
        for s in range(4):
            got = over_c(tn(act_rel[:, half:], gs[s]).astype(BF16))
            t = tn(act_rel[:, :half], gs[s]) + got.astype(F32)
            b = blk
            t00, t01, t10, t11 = t[:b], t[b : 2 * b], t[2 * b : 3 * b], t[3 * b :]
            if s % 2:
                got = over_y(jnp.concatenate([t01, t11], axis=0).astype(BF16)).astype(F32)
                u0 = t00 + got[:b]
                u1 = t10 + got[b:]
                u = u0 + over_x(u1.astype(BF16)).astype(F32)
            else:
                got = over_x(jnp.concatenate([t10, t11], axis=0).astype(BF16)).astype(F32)
                u0 = t00 + got[:b]
                u1 = t01 + got[b:]
                u = u0 + over_y(u1.astype(BF16)).astype(F32)
            u = u.astype(BF16)
            tot = tot + (u if s == 0 else to_slot(u, s)).astype(F32)
        tot = tot.astype(BF16)
        return ordered(tot.astype(F32), over_y(tot).astype(F32))

    g_down = weight_grad(dy_all, act_all)
    g_gate = weight_grad(n2_all, gg_all)
    g_up = weight_grad(n2_all, gu_all)

    bwd = []
    for s in range(4):
        bwd.append(
            call(
                bwd_kernel,
                [((count, 512), BF16), ((count, 128), F32), ((3, count, 128), BF16)],
                (branch, wo[s], fwd[s][0], *kv_of[s], bias, cos_q, sin_q, fwd[s][2], fwd[s][3]),
                2 * count * width * 512 + 8 * 10 * count * 1024 * 256,
                scratch=(
                    pltpu.VMEM((1024, 512), BF16),
                    pltpu.VMEM((1024, 512), BF16),
                    pltpu.VMEM((1024, 128), F32),
                    pltpu.VMEM((1024, 128), F32),
                ),
            )
        )
    got = []
    for t in (1, 2, 3):
        out = jnp.stack([bwd[s][2][t - 1] for s in range(4)])
        got.append(over_z(out, [(i, (i + t) % 4) for i in range(4) if i + t >= 4]))
    dkv = call(
        dkv_kernel,
        [((4, count, 128), BF16)],
        (*[bwd[s][1] for s in range(4)], *got, cos_k, sin_k),
        count * 512 * 8,
    )[0]
    dkv = jnp.concatenate([dkv[s] for s in range(4)], axis=1)
    dq = [bwd[s][0] for s in range(4)]
    grad_norm_one = nt(dq[0], wq[0]) + nt(dq[1], wq[1]) + nt(dq[2], wq[2]) + nt(dq[3], wq[3])
    grad_norm_one = grad_norm_one + nt(dkv, wkv)
    in_norm, gain_one_term = norm_backward(grad_norm_one, unit_one, inv_one, gain_one)
    grad_tokens = (grad_mid + in_norm).astype(BF16)
    g_output = weight_grad_slots(branch, attn)
    g_query = weight_grad_slots(normed_one, dq)
    g_keyval = weight_grad_slots(normed_one, [dkv[:, 128 * s : 128 * s + 128] for s in range(4)])

    def total(v):
        if not fast:
            return lax.psum(v, ("dp", "row", "col"))
        v = v + over_c(v)
        v = v + over_x(v)
        v = v + over_y(v)
        v = v + over_z(v, PAIR)
        return v + over_z(v, [(0, 2), (1, 3), (2, 0), (3, 1)])

    return (
        to_abs(block_out),
        to_abs(grad_tokens),
        total(to_abs(gain_one_term)),
        g_query,
        g_keyval,
        g_output.T,
        total(to_abs(gain_two_term)),
        g_gate,
        g_up,
        g_down.T,
    )


def solution(mesh):
    spec = P(("dp", "row", "col"), None)
    down = P("row", "col")
    across = P("col", "row")
    seq = P(("dp", "row"))
    return jax.shard_map(
        functools.partial(shards, rows=mesh.shape["row"]),
        mesh=mesh,
        in_specs=(spec, P(), down, down, across, P(), down, down, across, spec, seq, seq),
        out_specs=(spec, spec, P(), down, down, across, P(), down, down, across),
        check_vma=False,
    )
```
